8 devices in a mesh: dp: 1 (over z), sh: 8 (over y, x, core).
Axes of the slice: x: 2, y: 2, z: 1, core: 2. Of those that a mesh axis runs over, the one named last changes fastest.
Arguments:
- k_prefill: bfloat16 [8, 4352, 8, 128], P('dp', None, 'sh')
- v_prefill: bfloat16 [8, 4352, 8, 128], P('dp', None, 'sh')
- lengths: int32 [8], P('dp')
- residual: bfloat16 [8, 4096], P(('dp', 'sh'))
- norm_gain: bfloat16 [4096], replicated
- w_query: bfloat16 [4096, 4096], replicated
- w_key: bfloat16 [4096, 1024], replicated
- w_value: bfloat16 [4096, 1024], replicated
- w_out: bfloat16 [4096, 4096], replicated
Outputs:
- output 1: bfloat16 [8, 4096], P(('dp', 'sh'))
- output 2: bfloat16 [8, 4096, 8, 128], P(('dp', 'sh'))
- output 3: bfloat16 [8, 4096, 8, 128], P(('dp', 'sh'))
All inputs are finite; a program needn't handle non-finite values.
Results may differ from the reference program's by a relative error of at most 0.00417.
Values are sent between devices in bfloat16 or wider.
A program may use at most 1 GiB of HBM per device.

```python
import jax
import jax.numpy as jnp
from jax import lax

MODEL_DIM = 4096
HEADS = 32
KV_HEADS = 8
HEAD_DIM = 128
WINDOW = 4096
SEQ_LEN = 4352
BATCH = 8
Q_GROUP = HEADS // KV_HEADS
Q_WIDTH = HEADS * HEAD_DIM
KV_WIDTH = KV_HEADS * HEAD_DIM
THETA = 10000.0
EPS = 1e-5


def setup_inputs(seed: int = 0, part: int = 0) -> dict:
    root_key = jax.random.key(seed)
    part_root, shared_root = jax.random.split(root_key)
    part_keys = jax.random.split(jax.random.fold_in(part_root, part), 4)
    shared_keys = jax.random.split(shared_root, 5)
    kv_shape = (BATCH, SEQ_LEN, KV_HEADS, HEAD_DIM)
    k_prefill = jax.random.normal(part_keys[0], kv_shape, jnp.float32).astype(jnp.bfloat16)
    v_prefill = jax.random.normal(part_keys[1], kv_shape, jnp.float32).astype(jnp.bfloat16)
    lengths = jax.random.randint(part_keys[2], (BATCH,), 1, SEQ_LEN + 1, dtype=jnp.int32)
    lengths = lengths.at[0].set(SEQ_LEN).at[1].set(1)
    residual = jax.random.normal(part_keys[3], (BATCH, MODEL_DIM), jnp.float32).astype(jnp.bfloat16)
    norm_gain = (1.0 + 0.3 * jax.random.normal(shared_keys[0], (MODEL_DIM,), jnp.float32)).astype(jnp.bfloat16)
    w_query = (jax.random.normal(shared_keys[1], (MODEL_DIM, Q_WIDTH), jnp.float32) * (2.0 / MODEL_DIM ** 0.5)).astype(jnp.bfloat16)
    w_key = (jax.random.normal(shared_keys[2], (MODEL_DIM, KV_WIDTH), jnp.float32) * (3.0 / MODEL_DIM ** 0.5)).astype(jnp.bfloat16)
    w_value = (jax.random.normal(shared_keys[3], (MODEL_DIM, KV_WIDTH), jnp.float32) * (3.0 / MODEL_DIM ** 0.5)).astype(jnp.bfloat16)
    w_out = (jax.random.normal(shared_keys[4], (Q_WIDTH, MODEL_DIM), jnp.float32) * (2.0 / Q_WIDTH ** 0.5)).astype(jnp.bfloat16)
    return {'k_prefill': k_prefill, 'v_prefill': v_prefill, 'lengths': lengths, 'residual': residual, 'norm_gain': norm_gain, 'w_query': w_query, 'w_key': w_key, 'w_value': w_value, 'w_out': w_out}


def rolling_cache(prefill, lengths):
    slot_ids = jnp.arange(WINDOW, dtype=jnp.int32)
    last_pos = lengths[:, None] - 1
    held_pos = last_pos - jnp.remainder(last_pos - slot_ids[None, :], WINDOW)
    held = jax.vmap(lambda row_vals, row_idx: jnp.take(row_vals, row_idx, axis=0))(prefill, jnp.maximum(held_pos, 0))
    return jnp.where((held_pos >= 0)[:, :, None, None], held, jnp.zeros((), prefill.dtype))


def rotate(heads, positions):
    half_dim = HEAD_DIM // 2
    inv_freq = THETA ** (-2.0 * jnp.arange(half_dim, dtype=jnp.float32) / HEAD_DIM)
    angles = positions.astype(jnp.float32).reshape(positions.shape + (1,) * (heads.ndim - 1)) * inv_freq
    cos_part = jnp.cos(angles)
    sin_part = jnp.sin(angles)
    first_half = heads[..., :half_dim].astype(jnp.float32)
    second_half = heads[..., half_dim:].astype(jnp.float32)
    return jnp.concatenate([first_half * cos_part - second_half * sin_part, second_half * cos_part + first_half * sin_part], axis=-1).astype(jnp.bfloat16)


def attend_row(row_args):
    q_row, k_row, v_row, live_row = row_args
    q_grouped = q_row.reshape(KV_HEADS, Q_GROUP, HEAD_DIM).astype(jnp.float32)
    scores = jnp.einsum('kgd,wkd->kgw', q_grouped, k_row.astype(jnp.float32)) / HEAD_DIM ** 0.5
    scores = jnp.where(live_row[None, None, :], scores, -jnp.inf)
    weights = jax.nn.softmax(scores, axis=-1).astype(jnp.bfloat16)
    mixed = jnp.einsum('kgw,wkd->kgd', weights.astype(jnp.float32), v_row.astype(jnp.float32))
    return mixed.astype(jnp.bfloat16).reshape(Q_WIDTH)


def reference(k_prefill, v_prefill, lengths, residual, norm_gain, w_query, w_key, w_value, w_out):
    k_cache = rolling_cache(k_prefill, lengths)
    v_cache = rolling_cache(v_prefill, lengths)
    resid_f32 = residual.astype(jnp.float32)
    inv_rms = lax.rsqrt(jnp.mean(resid_f32 * resid_f32, axis=-1, keepdims=True) + EPS)
    normed = (resid_f32 * inv_rms * norm_gain.astype(jnp.float32)).astype(jnp.bfloat16)
    q_heads = jnp.dot(normed, w_query, preferred_element_type=jnp.float32).astype(jnp.bfloat16).reshape(BATCH, HEADS, HEAD_DIM)
    k_new = jnp.dot(normed, w_key, preferred_element_type=jnp.float32).astype(jnp.bfloat16).reshape(BATCH, KV_HEADS, HEAD_DIM)
    v_new = jnp.dot(normed, w_value, preferred_element_type=jnp.float32).astype(jnp.bfloat16).reshape(BATCH, KV_HEADS, HEAD_DIM)
    q_heads = rotate(q_heads, lengths)
    k_new = rotate(k_new, lengths)
    slot_ids = jnp.arange(WINDOW, dtype=jnp.int32)
    new_slot = (slot_ids[None, :] == (lengths % WINDOW)[:, None])[:, :, None, None]
    k_cache = jnp.where(new_slot, k_new[:, None], k_cache)
    v_cache = jnp.where(new_slot, v_new[:, None], v_cache)
    live_slot = (lengths[:, None] - jnp.remainder(lengths[:, None] - slot_ids[None, :], WINDOW)) >= 0
    attn_out = lax.map(attend_row, (q_heads, k_cache, v_cache, live_slot))
    resid_out = (resid_f32 + jnp.dot(attn_out, w_out, preferred_element_type=jnp.float32)).astype(jnp.bfloat16)
    return (resid_out, k_cache, v_cache)
```

```python
import functools

import jax
import jax.numpy as jnp
from jax import lax
from jax.experimental import pallas as pl
from jax.experimental.pallas import tpu as pltpu
from jax.sharding import PartitionSpec as P

WINDOW = 4096
THETA = 10000.0
EPS = 1e-5
ALIGN = 16
HALF = 2304
BASE = 2 * HALF
QUANTUM = 256
STEP = 512
ANY = pl.BlockSpec(memory_space=pl.ANY)
VMEM = pl.BlockSpec(memory_space=pltpu.VMEM)
SMEM = pl.BlockSpec(memory_space=pltpu.SMEM)


def pack_kernel(scal, k_ref, v_ref, out_ref, lists, first_sem, second_sem, store_sem, *, seq_len):
    chip = scal[0]
    list_len = out_ref.shape[2]
    peers = [chip + 1 - 2 * (chip % 2), (chip + 2) % 4, 3 - chip]

    def first(t, k):
        src = (k_ref, v_ref)[t]
        return pltpu.make_async_copy(src.at[2 * peers[k]], lists.at[t, k, pl.ds(0, seq_len)], first_sem.at[t, k])

    def second(t, k):
        src = (k_ref, v_ref)[t]
        start = pl.multiple_of(scal[1 + 2 * peers[k]], ALIGN)
        return pltpu.make_async_copy(src.at[2 * peers[k] + 1], lists.at[t, k, pl.ds(start, seq_len)], second_sem.at[t, k])

    extra = (list_len - BASE) // 4

    def stores(t, k):
        total = scal[1 + 2 * peers[k]] + scal[2 + 2 * peers[k]]
        yield None, pltpu.make_async_copy(lists.at[t, k, pl.ds(0, BASE)], out_ref.at[t, k, pl.ds(0, BASE)], store_sem.at[t, k, 0])
        for i in range(4):
            rows = pl.ds(BASE + i * extra, extra)
            yield total > BASE + i * extra, pltpu.make_async_copy(lists.at[t, k, rows], out_ref.at[t, k, rows], store_sem.at[t, k, 1 + i])

    order = [(t, k) for k in range(3) for t in range(2)]
    for t, k in order:
        first(t, k).start()
    for t, k in order:
        first(t, k).wait()
        second(t, k).start()
    for t, k in order:
        second(t, k).wait()
        for live, copy in stores(t, k):
            if live is None:
                copy.start()
            else:
                pl.when(live)(copy.start)
    for t, k in order:
        for live, copy in stores(t, k):
            if live is None:
                copy.wait()
            else:
                pl.when(live)(copy.wait)


def pack(scal, k_rows, v_rows):
    seq_len, head_dim = k_rows.shape[1:]
    shape = (2, 3, 2 * seq_len, head_dim)
    return pl.pallas_call(
        functools.partial(pack_kernel, seq_len=seq_len),
        out_shape=jax.ShapeDtypeStruct(shape, k_rows.dtype),
        in_specs=[SMEM, ANY, ANY],
        out_specs=ANY,
        scratch_shapes=[pltpu.VMEM(shape, k_rows.dtype), pltpu.SemaphoreType.DMA((2, 3)), pltpu.SemaphoreType.DMA((2, 3)), pltpu.SemaphoreType.DMA((2, 3, 5))],
        compiler_params=pltpu.CompilerParams(vmem_limit_bytes=20 * 2**20),
        name='pack',
    )(scal, k_rows, v_rows)


def exchange_kernel(packed, k_ref, v_ref, land, swap, send_sem, recv_sem, esend_sem, erecv_sem, fsend_sem, frecv_sem, ssend_sem, srecv_sem, *, extra):
    me = lax.axis_index('sh')
    core = me % 2
    chip = me // 2
    partner = me + 1 - 2 * core
    peers = [chip + 1 - 2 * (chip % 2), (chip + 2) % 4, 3 - chip]

    def remote(src, dst, send, recv, device):
        return pltpu.make_async_remote_copy(src_ref=src, dst_ref=dst, send_sem=send, recv_sem=recv, device_id={'sh': device}, device_id_type=pl.DeviceIdType.MESH)

    def main(t, k, half):
        rows = pl.ds(half * HALF, HALF)
        return remote(packed.at[t, k, rows], land.at[t, k, core, rows], send_sem.at[t, k, half], recv_sem.at[t, k, core], 2 * peers[k] + half)

    def more(t, k):
        rows = pl.ds(BASE, extra)
        return remote(packed.at[t, k, rows], land.at[t, k, core, rows], esend_sem.at[t, k], erecv_sem.at[t, k, core], 2 * peers[k] + 1)

    def more_in(t, k, q):
        rows = land.at[t, k, q, pl.ds(BASE, extra)]
        return remote(rows, rows, esend_sem.at[t, k], erecv_sem.at[t, k, q], partner)

    def forward(t, k, q):
        rows = land.at[t, k, q, pl.ds(core * HALF, HALF)]
        return remote(rows, rows, fsend_sem.at[t, k, q], frecv_sem.at[t, k, q], partner)

    def main_in(t, k, q):
        rows = land.at[t, k, q, pl.ds(core * HALF, HALF)]
        return remote(rows, rows, fsend_sem.at[t, k, q], recv_sem.at[t, k, q], partner)

    def forward_in(t, k, q):
        rows = land.at[t, k, q, pl.ds((1 - core) * HALF, HALF)]
        return remote(rows, rows, fsend_sem.at[t, k, q], frecv_sem.at[t, k, q], partner)

    def across(t):
        return remote((k_ref, v_ref)[t].at[partner], swap.at[t], ssend_sem.at[t], srecv_sem.at[t], partner)

    order = [(t, k) for k in range(3) for t in range(2)]
    for t, k in order:
        for half in range(2):
            main(t, k, half).start()
        if extra:
            more(t, k).start()
    for t in range(2):
        across(t).start()
    for t, k in order:
        for q in range(2):
            main_in(t, k, q).wait_recv()
            forward(t, k, q).start()
    for t in range(2):
        across(t).wait()
    for t, k in order:
        for half in range(2):
            main(t, k, half).wait_send()
        if extra:
            more(t, k).wait_send()
    if extra:
        @pl.when(core == 1)
        def _():
            for t, k in order:
                for q in range(2):
                    more_in(t, k, q).wait_recv()
    for t, k in order:
        for q in range(2):
            forward(t, k, q).wait_send()
            forward_in(t, k, q).wait_recv()


def exchange(packed, k_rows, v_rows, *, extra):
    seq_len, head_dim = k_rows.shape[1:]
    dma = pltpu.SemaphoreType.DMA
    return pl.pallas_call(
        functools.partial(exchange_kernel, extra=extra),
        out_shape=(jax.ShapeDtypeStruct((2, 3, 2, 2 * seq_len, head_dim), k_rows.dtype), jax.ShapeDtypeStruct((2, seq_len, head_dim), k_rows.dtype)),
        in_specs=[ANY, ANY, ANY],
        out_specs=(ANY, ANY),
        scratch_shapes=[dma((2, 3, 2)), dma((2, 3, 2)), dma((2, 3)), dma((2, 3, 2)), dma((2, 3, 2)), dma((2, 3, 2)), dma((2,)), dma((2,))],
        compiler_params=pltpu.CompilerParams(has_side_effects=True),
        name=f'exchange_{extra}',
    )(packed, k_rows, v_rows)


def build_kernel(scal, q_ref, knew_ref, vnew_ref, res_ref, k_ref, v_ref, land, swap, wout_ref, kc_ref, vc_ref, xout_ref, ring, tail, wide, scores, probs, mixed, ovec, wbuf, ring_sem, tail_sem, w_sem, *, depth):
    step = pl.program_id(0)
    steps = WINDOW // STEP
    me, core, chip, n, offset = scal[0], scal[1], scal[2], scal[3], scal[4]
    chips = [chip, chip + 1 - 2 * (chip % 2), (chip + 2) % 4, 3 - chip]
    extra = tail.shape[2]
    heads = tail.shape[1]
    head_dim = tail.shape[3]

    def copies(t, start, size, dst, sem):
        own = 2 * chip + core
        other = 2 * chip + 1 - core
        rows = pl.ds(start, size)
        yield pltpu.make_async_copy((k_ref, v_ref)[t].at[me, rows], dst.at[own], sem.at[0])
        yield pltpu.make_async_copy(swap.at[t, rows], dst.at[other], sem.at[1])
        far = pl.ds(pl.multiple_of(offset + start, ALIGN), size)
        for k in range(3):
            for q in range(2):
                yield pltpu.make_async_copy(land.at[t, k, q, far], dst.at[2 * chips[k + 1] + q], sem.at[2 + 2 * k + q])

    def for_step(s, act):
        for t in range(2):
            local = s - t * steps
            @pl.when((local >= 0) & (local < steps) & (local * STEP < n))
            def _():
                for copy in copies(t, pl.multiple_of(local * STEP, STEP), STEP, ring.at[s % depth], ring_sem.at[s % depth]):
                    act(copy)

    def for_tail(t, act):
        @pl.when(n > WINDOW)
        def _():
            for copy in copies(t, WINDOW, extra, tail.at[t], tail_sem.at[t]):
                act(copy)

    w_rows = wbuf.shape[0] // (2 * steps)

    def w_copy(s):
        rows = pl.ds(pl.multiple_of(s * w_rows, w_rows), w_rows)
        return pltpu.make_async_copy(wout_ref.at[rows], wbuf.at[rows], w_sem.at[s])

    @pl.when(step == 0)
    def _():
        for_tail(0, lambda c: c.start())
        for s in range(depth - 1):
            for_step(jnp.int32(s), lambda c: c.start())
        for_tail(1, lambda c: c.start())
        mixed[...] = jnp.zeros_like(mixed)
    for_step(step + depth - 1, lambda c: c.start())
    w_copy(step).start()
    for_step(step, lambda c: c.wait())

    def assemble(t, local, new_ref, out_ref, use):
        @pl.when(local == 0)
        def _():
            for_tail(t, lambda c: c.wait())
        first = local * STEP
        pos = first + lax.broadcasted_iota(jnp.int32, (STEP, head_dim), 0)
        written = pos == lax.rem(n, WINDOW)
        held = pos < n
        again = pos[:extra] < n - WINDOW
        for h in range(heads):
            vals = ring[step % depth, h]
            low = jnp.where(again, tail[t, h], vals[:extra])
            vals = jnp.concatenate([low, vals[extra:]], axis=0)
            vals = jnp.where(held, vals, jnp.zeros_like(vals))
            vals = jnp.where(written, jnp.broadcast_to(new_ref[h:h + 1, :], vals.shape), vals)
            wide[pl.ds(h, STEP, stride=heads), :] = vals.astype(jnp.float32)
            use(h, vals)
        out_ref[...] = wide[...].reshape(STEP, heads, head_dim).astype(out_ref.dtype)

    @pl.when(step < steps)
    def _():
        slots = step * STEP + lax.broadcasted_iota(jnp.int32, (8, STEP), 1)
        live = (slots <= n) | (n >= WINDOW)

        def use(h, vals):
            s = lax.dot_general(q_ref[h], vals, (((1,), (1,)), ((), ())), preferred_element_type=jnp.float32) / head_dim ** 0.5
            scores[pl.ds(8 * h, 8), pl.ds(pl.multiple_of(step * STEP, STEP), STEP)] = jnp.where(live, s, -jnp.inf)
        assemble(0, step, knew_ref, kc_ref, use)

    @pl.when(step == steps)
    def _():
        for h in range(heads):
            s = scores[8 * h:8 * h + 8, :]
            e = jnp.exp(s - jnp.max(s, axis=-1, keepdims=True))
            probs[h] = (e / jnp.sum(e, axis=-1, keepdims=True)).astype(probs.dtype)

    @pl.when(step >= steps)
    def _():
        local = step - steps

        def use(h, vals):
            p = probs[h, :, pl.ds(pl.multiple_of(local * STEP, STEP), STEP)]
            mixed[h] += jnp.dot(p, vals, preferred_element_type=jnp.float32)
        assemble(1, local, vnew_ref, vc_ref, use)

    @pl.when(step == 2 * steps - 1)
    def _():
        group = wbuf.shape[0] // (heads * head_dim)
        for h in range(heads):
            o = mixed[h].astype(ovec.dtype)
            for g in range(group):
                cols = pl.ds((h * group + g) * head_dim, head_dim)
                ovec[:, cols] = jnp.broadcast_to(o[g:g + 1], (ovec.shape[0], head_dim))
        for s in range(2 * steps):
            w_copy(s).wait()
        width = 512

        def column(c, carry):
            cols = pl.ds(pl.multiple_of(c * width, width), width)
            acc = jnp.dot(ovec[...], wbuf[:, cols], preferred_element_type=jnp.float32)
            xout_ref[:, cols] = (res_ref[:, cols].astype(jnp.float32) + acc[:1]).astype(xout_ref.dtype)
            return carry
        lax.fori_loop(0, wbuf.shape[1] // width, column, 0)


def build(scal, q_heads, k_new, v_new, residual, k_rows, v_rows, land, swap, w_out):
    heads, head_dim = k_new.shape
    model_dim = residual.shape[1]
    seq_len = k_rows.shape[1]
    steps = WINDOW // STEP
    depth = 4
    dtype = k_rows.dtype
    cache = jax.ShapeDtypeStruct((WINDOW, heads, head_dim), dtype)
    block = (STEP, heads, head_dim)
    dma = pltpu.SemaphoreType.DMA
    return pl.pallas_call(
        functools.partial(build_kernel, depth=depth),
        grid=(2 * steps,),
        out_shape=(cache, cache, jax.ShapeDtypeStruct(residual.shape, dtype)),
        in_specs=[SMEM, VMEM, VMEM, VMEM, VMEM, ANY, ANY, ANY, ANY, ANY],
        out_specs=(pl.BlockSpec(block, lambda i: (jnp.minimum(i, steps - 1), 0, 0)), pl.BlockSpec(block, lambda i: (jnp.maximum(i - steps, 0), 0, 0)), VMEM),
        scratch_shapes=[
            pltpu.VMEM((depth, heads, STEP, head_dim), dtype),
            pltpu.VMEM((2, heads, seq_len - WINDOW, head_dim), dtype),
            pltpu.VMEM((STEP * heads, head_dim), jnp.float32),
            pltpu.VMEM((8 * heads, WINDOW), jnp.float32),
            pltpu.VMEM((heads, 8, WINDOW), dtype),
            pltpu.VMEM((heads, 8, head_dim), jnp.float32),
            pltpu.VMEM((16, w_out.shape[0]), dtype),
            pltpu.VMEM(w_out.shape, dtype),
            dma((depth, 8)), dma((2, 8)), dma((2 * steps,)),
        ],
        compiler_params=pltpu.CompilerParams(vmem_limit_bytes=60 * 2**20),
        name='build',
    )(scal, q_heads, k_new, v_new, residual, k_rows, v_rows, land, swap, w_out)


def rotate(heads, positions):
    head_dim = heads.shape[-1]
    half_dim = head_dim // 2
    inv_freq = THETA ** (-2.0 * jnp.arange(half_dim, dtype=jnp.float32) / head_dim)
    angles = positions.astype(jnp.float32).reshape(positions.shape + (1,) * (heads.ndim - 1)) * inv_freq
    cos_part = jnp.cos(angles)
    sin_part = jnp.sin(angles)
    first_half = heads[..., :half_dim].astype(jnp.float32)
    second_half = heads[..., half_dim:].astype(jnp.float32)
    return jnp.concatenate([first_half * cos_part - second_half * sin_part, second_half * cos_part + first_half * sin_part], axis=-1).astype(jnp.bfloat16)


def solution(mesh):
    head_spec = P('dp', None, 'sh', None)
    row_spec = P(('dp', 'sh'))
    full_spec = P(None, None)

    def per_device(k_prefill, v_prefill, lengths, residual, norm_gain, w_query, w_key, w_value, w_out):
        num_rows, seq_len, _, head_dim = k_prefill.shape
        kv_heads = w_key.shape[1] // head_dim
        q_group = w_query.shape[1] // w_key.shape[1]
        me = lax.axis_index('sh')
        core, chip = me % 2, me // 2
        my_length = lax.dynamic_slice_in_dim(lengths, me, 1)
        k_rows = k_prefill.reshape(num_rows, seq_len, head_dim)
        v_rows = v_prefill.reshape(num_rows, seq_len, head_dim)
        spans = (lengths + (ALIGN - 1)) // ALIGN * ALIGN
        packed = pack(jnp.concatenate([chip[None], spans]), k_rows, v_rows)
        longest = jnp.max(spans.reshape(-1, 2).sum(axis=1))
        sizes = (2 * seq_len - BASE) // QUANTUM
        which = jnp.clip((longest - BASE + QUANTUM - 1) // QUANTUM, 0, sizes)
        land, swap = lax.switch(which, [functools.partial(exchange, extra=i * QUANTUM) for i in range(sizes + 1)], packed, k_rows, v_rows)

        resid_f32 = residual.astype(jnp.float32)
        inv_rms = lax.rsqrt(jnp.mean(resid_f32 * resid_f32, axis=-1, keepdims=True) + EPS)
        normed = (resid_f32 * inv_rms * norm_gain.astype(jnp.float32)).astype(jnp.bfloat16)
        q_heads = jnp.dot(normed, w_query, preferred_element_type=jnp.float32).astype(jnp.bfloat16).reshape(1, kv_heads, q_group, head_dim)
        k_new = jnp.dot(normed, w_key, preferred_element_type=jnp.float32).astype(jnp.bfloat16).reshape(1, kv_heads, head_dim)
        v_new = jnp.dot(normed, w_value, preferred_element_type=jnp.float32).astype(jnp.bfloat16).reshape(kv_heads, head_dim)
        q_heads = jnp.pad(rotate(q_heads, my_length)[0], ((0, 0), (0, 8 - q_group), (0, 0)))
        k_new = rotate(k_new, my_length)[0]
        offset = jnp.where(core == 1, spans[2 * chip], 0)
        scal = jnp.stack([me, core, chip, my_length[0], offset])
        k_cache, v_cache, resid_out = build(scal, q_heads, k_new, v_new, residual, k_rows, v_rows, land, swap, w_out)
        return resid_out, k_cache[None], v_cache[None]
    return jax.shard_map(per_device, mesh=mesh, in_specs=(head_spec, head_spec, P('dp'), P(('dp', 'sh'), None), P(None), full_spec, full_spec, full_spec, full_spec), out_specs=(P(('dp', 'sh'), None), row_spec, row_spec), check_vma=False)
```

```python
import functools

import jax
import jax.numpy as jnp
from jax import lax
from jax.experimental import pallas as pl
from jax.experimental.pallas import tpu as pltpu
from jax.sharding import PartitionSpec as P

WINDOW = 4096
THETA = 10000.0
EPS = 1e-5
ALIGN = 16
HALF = 2192
BASE = 2 * HALF
QUANTUM = 128
STEP = 512
BUILD_VMEM = 60 * 2**20
LANES = 16
ANY = pl.BlockSpec(memory_space=pl.ANY)
VMEM = pl.BlockSpec(memory_space=pltpu.VMEM)
SMEM = pl.BlockSpec(memory_space=pltpu.SMEM)
HBM = pl.BlockSpec(memory_space=pltpu.HBM)


def list_length(seq_len):
    return BASE + -(-(2 * seq_len - BASE) // QUANTUM) * QUANTUM


def span(length):
    return (length + (ALIGN - 1)) // ALIGN * ALIGN


def pack_kernel(len_ref, k_ref, v_ref, out_ref, size_ref, lists, first_sem, second_sem, store_sem, *, seq_len):
    chip = lax.axis_index('sh') // 2
    list_len = lists.shape[2]
    peers = [chip + 1 - 2 * (chip % 2), (chip + 2) % 4, 3 - chip]

    def first(t, k):
        src = (k_ref, v_ref)[t]
        return pltpu.make_async_copy(src.at[2 * peers[k]], lists.at[t, k, pl.ds(0, seq_len)], first_sem.at[t, k])

    def second(t, k):
        src = (k_ref, v_ref)[t]
        start = pl.multiple_of(span(len_ref[2 * peers[k]]), ALIGN)
        return pltpu.make_async_copy(src.at[2 * peers[k] + 1], lists.at[t, k, pl.ds(start, seq_len)], second_sem.at[t, k])

    extra = (list_len - BASE) // 2

    def stores(t, k):
        total = span(len_ref[2 * peers[k]]) + span(len_ref[2 * peers[k] + 1])
        yield None, pltpu.make_async_copy(lists.at[t, k, pl.ds(0, BASE)], out_ref.at[t, k, pl.ds(0, BASE)], store_sem.at[t, k, 0])
        for i in range(2):
            rows = pl.ds(BASE + i * extra, extra)
            yield total > BASE + i * extra, pltpu.make_async_copy(lists.at[t, k, rows], out_ref.at[t, k, rows], store_sem.at[t, k, 1 + i])

    order = [(t, k) for k in range(3) for t in range(2)]
    for t, k in order:
        first(t, k).start()
    longest = span(len_ref[0]) + span(len_ref[1])
    for c in range(1, len_ref.shape[0] // 2):
        longest = jnp.maximum(longest, span(len_ref[2 * c]) + span(len_ref[2 * c + 1]))
    size_ref[0] = jnp.clip((longest - BASE + QUANTUM - 1) // QUANTUM, 0, (list_len - BASE) // QUANTUM)
    for t, k in order:
        first(t, k).wait()
        second(t, k).start()
    for t, k in order:
        second(t, k).wait()
        for live, copy in stores(t, k):
            if live is None:
                copy.start()
            else:
                pl.when(live)(copy.start)
    for t, k in order:
        for live, copy in stores(t, k):
            if live is None:
                copy.wait()
            else:
                pl.when(live)(copy.wait)


def pack(lengths, k_rows, v_rows):
    seq_len, head_dim = k_rows.shape[1:]
    shape = (2, 3, list_length(seq_len), head_dim)
    return pl.pallas_call(
        functools.partial(pack_kernel, seq_len=seq_len),
        out_shape=(jax.ShapeDtypeStruct(shape, k_rows.dtype), jax.ShapeDtypeStruct((1,), jnp.int32)),
        in_specs=[SMEM, HBM, HBM],
        out_specs=(HBM, SMEM),
        scratch_shapes=[pltpu.VMEM(shape, k_rows.dtype), pltpu.SemaphoreType.DMA((2, 3)), pltpu.SemaphoreType.DMA((2, 3)), pltpu.SemaphoreType.DMA((2, 3, 3))],
        compiler_params=pltpu.CompilerParams(vmem_limit_bytes=60 * 2**20),
        name='pack',
    )(lengths, k_rows, v_rows)


def project(res_ref, gain_ref, weights, proj_ref, normed, total, ring, ring_sem):
    depth, rows, width = ring.shape
    resid = res_ref[...].astype(jnp.float32)
    inv_rms = lax.rsqrt(jnp.sum(resid * resid, axis=-1, keepdims=True) / resid.shape[-1] + EPS)
    row = (resid * inv_rms * gain_ref[...].astype(jnp.float32)).astype(normed.dtype)
    normed[...] = jnp.broadcast_to(row, normed.shape)
    total[...] = jnp.zeros_like(total)
    steps = normed.shape[1] // rows
    at = 0
    for w_ref in weights:
        for left in range(0, w_ref.shape[1], width):
            def block(i, w_ref=w_ref, left=left):
                slot = lax.rem(i, depth)
                return pltpu.make_async_copy(w_ref.at[pl.ds(pl.multiple_of(i * rows, rows), rows), pl.ds(left, width)], ring.at[slot], ring_sem.at[slot])

            for i in range(depth - 1):
                block(i).start()

            def step(i, carry, block=block, at=at):
                @pl.when(i + depth - 1 < steps)
                def _():
                    block(i + depth - 1).start()
                block(i).wait()
                part = normed[:, pl.ds(pl.multiple_of(i * rows, rows), rows)]
                total[:, at:at + width] += jnp.dot(part, ring[lax.rem(i, depth)], preferred_element_type=jnp.float32)
                return carry
            lax.fori_loop(0, steps, step, 0)
            at += width
    proj_ref[...] = total[...].astype(proj_ref.dtype)


def remote(src, dst, send, recv, device):
    return pltpu.make_async_remote_copy(src_ref=src, dst_ref=dst, send_sem=send, recv_sem=recv, device_id={'sh': device}, device_id_type=pl.DeviceIdType.MESH)


ORDER = [(t, k) for k in range(3) for t in range(2)]


def more_kernel(packed, land, send_sem, recv_sem, *, extra):
    me = lax.axis_index('sh')
    core = me % 2
    chip = me // 2
    peers = [chip + 1 - 2 * (chip % 2), (chip + 2) % 4, 3 - chip]
    rows = pl.ds(BASE, extra)

    def out(t, k):
        return remote(packed.at[t, k, rows], land.at[t, k, core, rows], send_sem.at[t, k], recv_sem.at[t, k, core], 2 * peers[k] + 1)

    def into(t, k, q):
        here = land.at[t, k, q, rows]
        return remote(here, here, send_sem.at[t, k], recv_sem.at[t, k, q], me)

    for t, k in ORDER:
        out(t, k).start()
    for t, k in ORDER:
        out(t, k).wait_send()

    @pl.when(core == 1)
    def _():
        for t, k in ORDER:
            for q in range(2):
                into(t, k, q).wait_recv()


def nothing_kernel(packed, land):
    pass


def more(packed, *, extra):
    shape = jax.ShapeDtypeStruct(packed.shape[:2] + (2,) + packed.shape[2:], packed.dtype)
    if not extra:
        return pl.pallas_call(nothing_kernel, out_shape=shape, in_specs=[HBM], out_specs=HBM, compiler_params=pltpu.CompilerParams(vmem_limit_bytes=60 * 2**20), name='more_0')(packed)
    dma = pltpu.SemaphoreType.DMA
    return pl.pallas_call(
        functools.partial(more_kernel, extra=extra),
        out_shape=shape,
        in_specs=[HBM],
        out_specs=HBM,
        scratch_shapes=[dma((2, 3)), dma((2, 3, 2))],
        compiler_params=pltpu.CompilerParams(has_side_effects=True, vmem_limit_bytes=60 * 2**20),
        name=f'more_{extra}',
    )(packed)


def base_kernel(packed, k_ref, v_ref, res_ref, gain_ref, wq_ref, wk_ref, wv_ref, _, land, swap, proj_ref, normed, total, ring, ring_sem, send_sem, recv_sem, fsend_sem, frecv_sem, ssend_sem, srecv_sem):
    me = lax.axis_index('sh')
    core = me % 2
    chip = me // 2
    partner = me + 1 - 2 * core
    peers = [chip + 1 - 2 * (chip % 2), (chip + 2) % 4, 3 - chip]

    def main(t, k, half):
        rows = pl.ds(half * HALF, HALF)
        return remote(packed.at[t, k, rows], land.at[t, k, core, rows], send_sem.at[t, k, half], recv_sem.at[t, k, core], 2 * peers[k] + half)

    def forward(t, k, q):
        rows = land.at[t, k, q, pl.ds(core * HALF, HALF)]
        return remote(rows, rows, fsend_sem.at[t, k, q], frecv_sem.at[t, k, q], partner)

    def main_in(t, k, q):
        rows = land.at[t, k, q, pl.ds(core * HALF, HALF)]
        return remote(rows, rows, fsend_sem.at[t, k, q], recv_sem.at[t, k, q], partner)

    def forward_in(t, k, q):
        rows = land.at[t, k, q, pl.ds((1 - core) * HALF, HALF)]
        return remote(rows, rows, fsend_sem.at[t, k, q], frecv_sem.at[t, k, q], partner)

    def across(t):
        return remote((k_ref, v_ref)[t].at[partner], swap.at[t], ssend_sem.at[t], srecv_sem.at[t], partner)

    for t, k in ORDER:
        for half in range(2):
            main(t, k, half).start()
    for t in range(2):
        across(t).start()
    project(res_ref, gain_ref, (wq_ref, wk_ref, wv_ref), proj_ref, normed, total, ring, ring_sem)
    for t, k in ORDER:
        for q in range(2):
            main_in(t, k, q).wait_recv()
            forward(t, k, q).start()
    for t in range(2):
        across(t).wait()
    for t, k in ORDER:
        for half in range(2):
            main(t, k, half).wait_send()
    for t, k in ORDER:
        for q in range(2):
            forward(t, k, q).wait_send()
            forward_in(t, k, q).wait_recv()


def base(packed, k_rows, v_rows, residual, gain, w_query, w_key, w_value, land):
    seq_len, head_dim = k_rows.shape[1:]
    dtype = k_rows.dtype
    dma = pltpu.SemaphoreType.DMA
    model_dim = residual.shape[1]
    proj_dim = w_query.shape[1] + w_key.shape[1] + w_value.shape[1]
    return pl.pallas_call(
        base_kernel,
        out_shape=(jax.ShapeDtypeStruct(land.shape, dtype), jax.ShapeDtypeStruct((2, seq_len, head_dim), dtype), jax.ShapeDtypeStruct((LANES, proj_dim), dtype),),
        in_specs=[HBM, HBM, HBM, VMEM, VMEM, HBM, HBM, HBM, HBM],
        out_specs=(HBM, HBM, VMEM),
        scratch_shapes=[
            pltpu.VMEM((LANES, model_dim), dtype), pltpu.VMEM((LANES, proj_dim), jnp.float32), pltpu.VMEM((4, 1024, 512), dtype), dma((4,)),
            dma((2, 3, 2)), dma((2, 3, 2)), dma((2, 3, 2)), dma((2, 3, 2)), dma((2,)), dma((2,)),
        ],
        input_output_aliases={8: 0},
        compiler_params=pltpu.CompilerParams(has_side_effects=True, vmem_limit_bytes=60 * 2**20),
        name='base',
    )(packed, k_rows, v_rows, residual, gain, w_query, w_key, w_value, land)


def build_kernel(len_ref, proj_ref, cos_ref, sin_ref, res_ref, wout_ref, k_ref, v_ref, land, swap, kc_ref, vc_ref, xout_ref, wbuf, ring, tail, wide, scores, probs, mixed, ovec, q_ref, knew_ref, vnew_ref, ring_sem, tail_sem, w_sem, *, depth):
    step = pl.program_id(0)
    steps = WINDOW // STEP
    me = lax.axis_index('sh')
    core, chip, n = me % 2, me // 2, len_ref[me]
    offset = core * span(len_ref[2 * chip])
    chips = [chip, chip + 1 - 2 * (chip % 2), (chip + 2) % 4, 3 - chip]
    extra = tail.shape[2]
    heads = tail.shape[1]
    head_dim = tail.shape[3]

    def copies(t, start, size, dst, sem):
        own = 2 * chip + core
        other = 2 * chip + 1 - core
        rows = pl.ds(start, size)
        yield pltpu.make_async_copy((k_ref, v_ref)[t].at[me, rows], dst.at[own], sem.at[0])
        yield pltpu.make_async_copy(swap.at[t, rows], dst.at[other], sem.at[1])
        far = pl.ds(pl.multiple_of(offset + start, ALIGN), size)
        for k in range(3):
            for q in range(2):
                yield pltpu.make_async_copy(land.at[t, k, q, far], dst.at[2 * chips[k + 1] + q], sem.at[2 + 2 * k + q])

    def heads_of_row():
        q_width = wbuf.shape[0]
        group = q_width // (heads * head_dim)

        def part(at):
            return proj_ref[:1, at:at + head_dim]

        def turned(at):
            vals = part(at).astype(jnp.float32)
            return (vals * cos_ref[...] + pltpu.roll(vals, head_dim // 2, 1) * sin_ref[...]).astype(q_ref.dtype)

        for h in range(heads):
            q_ref[h] = jnp.concatenate([turned((h * group + g) * head_dim) for g in range(group)] + [jnp.zeros((q_ref.shape[1] - group, head_dim), q_ref.dtype)], axis=0)
        knew_ref[...] = jnp.concatenate([turned(q_width + h * head_dim) for h in range(heads)], axis=0)
        vnew_ref[...] = jnp.concatenate([part(q_width + (heads + h) * head_dim) for h in range(heads)], axis=0)

    def for_step(s, act):
        for t in range(2):
            local = s - t * steps
            @pl.when((local >= 0) & (local < steps) & (local * STEP < n))
            def _():
                for copy in copies(t, pl.multiple_of(local * STEP, STEP), STEP, ring.at[s % depth], ring_sem.at[s % depth]):
                    act(copy)

    def for_tail(t, act):
        @pl.when(n > WINDOW)
        def _():
            for copy in copies(t, WINDOW, extra, tail.at[t], tail_sem.at[t]):
                act(copy)

    w_rows = wbuf.shape[0] // (2 * steps)

    def w_copy(s):
        rows = pl.ds(pl.multiple_of(s * w_rows, w_rows), w_rows)
        return pltpu.make_async_copy(wout_ref.at[rows], wbuf.at[rows], w_sem.at[s])

    @pl.when(step == 0)
    def _():
        for_tail(0, lambda c: c.start())
        for s in range(depth - 1):
            for_step(jnp.int32(s), lambda c: c.start())
        for_tail(1, lambda c: c.start())
        mixed[...] = jnp.zeros_like(mixed)
        heads_of_row()
    for_step(step + depth - 1, lambda c: c.start())
    w_copy(step).start()
    for_step(step, lambda c: c.wait())

    def assemble(t, local, new_ref, out_ref, use):
        first = local * STEP
        newest = lax.rem(n, WINDOW)
        wraps = (local == 0) & (n > WINDOW)
        dead = first > n
        plain = (first + STEP <= n) & ~wraps & ((newest < first) | (newest >= first + STEP))

        @pl.when(wraps)
        def _():
            for_tail(t, lambda c: c.wait())

        def fill(vals_of):
            for h in range(heads):
                vals = vals_of(h)
                wide[pl.ds(h, STEP, stride=heads), :] = vals.astype(jnp.float32)
                use(h, vals)
            out_ref[...] = wide[...].reshape(STEP, heads, head_dim).astype(out_ref.dtype)

        @pl.when(plain)
        def _():
            fill(lambda h: ring[step % depth, h])

        @pl.when(dead)
        def _():
            out_ref[...] = jnp.zeros_like(out_ref)
            use(None, None)

        @pl.when(~plain & ~dead)
        def _():
            pos = first + lax.broadcasted_iota(jnp.int32, (STEP, head_dim), 0)

            def patched(h):
                vals = ring[step % depth, h]
                low = jnp.where(pos[:extra] < n - WINDOW, tail[t, h], vals[:extra])
                vals = jnp.concatenate([low, vals[extra:]], axis=0)
                vals = jnp.where(pos < n, vals, jnp.zeros_like(vals))
                return jnp.where(pos == newest, jnp.broadcast_to(new_ref[h:h + 1, :], vals.shape), vals)
            fill(patched)

    @pl.when(step < steps)
    def _():
        slots = step * STEP + lax.broadcasted_iota(jnp.int32, (8, STEP), 1)
        live = (slots <= n) | (n >= WINDOW)

        def use(h, vals):
            if h is None:
                scores[:, pl.ds(pl.multiple_of(step * STEP, STEP), STEP)] = jnp.full((scores.shape[0], STEP), -jnp.inf)
                return
            s = lax.dot_general(q_ref[h], vals, (((1,), (1,)), ((), ())), preferred_element_type=jnp.float32) / head_dim ** 0.5
            scores[pl.ds(8 * h, 8), pl.ds(pl.multiple_of(step * STEP, STEP), STEP)] = jnp.where(live, s, -jnp.inf)
        assemble(0, step, knew_ref, kc_ref, use)

    @pl.when(step == steps)
    def _():
        for h in range(heads):
            s = scores[8 * h:8 * h + 8, :]
            e = jnp.exp(s - jnp.max(s, axis=-1, keepdims=True))
            probs[h] = (e / jnp.sum(e, axis=-1, keepdims=True)).astype(probs.dtype)

    @pl.when(step >= steps)
    def _():
        local = step - steps

        def use(h, vals):
            if h is None:
                return
            p = probs[h, :, pl.ds(pl.multiple_of(local * STEP, STEP), STEP)]
            mixed[h] += jnp.dot(p, vals, preferred_element_type=jnp.float32)
        assemble(1, local, vnew_ref, vc_ref, use)

    @pl.when(step == 2 * steps - 1)
    def _():
        group = wbuf.shape[0] // (heads * head_dim)
        for h in range(heads):
            o = mixed[h].astype(ovec.dtype)
            for g in range(group):
                cols = pl.ds((h * group + g) * head_dim, head_dim)
                ovec[:, cols] = jnp.broadcast_to(o[g:g + 1], (ovec.shape[0], head_dim))
        for s in range(2 * steps):
            w_copy(s).wait()
        width = 512

        def column(c, carry):
            cols = pl.ds(pl.multiple_of(c * width, width), width)
            acc = jnp.dot(ovec[...], wbuf[:, cols], preferred_element_type=jnp.float32)
            xout_ref[:, cols] = (res_ref[:, cols].astype(jnp.float32) + acc[:1]).astype(xout_ref.dtype)
            return carry
        lax.fori_loop(0, wbuf.shape[1] // width, column, 0)


def build(lengths, proj, cos, sin, residual, w_out, k_rows, v_rows, land, swap, heads):
    seq_len, head_dim = k_rows.shape[1:]
    steps = WINDOW // STEP
    depth = 4
    dtype = k_rows.dtype
    cache = jax.ShapeDtypeStruct((WINDOW, heads, head_dim), dtype)
    block = (STEP, heads, head_dim)
    dma = pltpu.SemaphoreType.DMA
    return pl.pallas_call(
        functools.partial(build_kernel, depth=depth),
        grid=(2 * steps,),
        out_shape=(cache, cache, jax.ShapeDtypeStruct(residual.shape, dtype)),
        in_specs=[SMEM, VMEM, VMEM, VMEM, VMEM, HBM, HBM, HBM, HBM, HBM],
        out_specs=(pl.BlockSpec(block, lambda i: (jnp.minimum(i, steps - 1), 0, 0)), pl.BlockSpec(block, lambda i: (jnp.maximum(i - steps, 0), 0, 0)), VMEM),
        scratch_shapes=[
            pltpu.VMEM(w_out.shape, dtype),
            pltpu.VMEM((depth, heads, STEP, head_dim), dtype),
            pltpu.VMEM((2, heads, seq_len - WINDOW, head_dim), dtype),
            pltpu.VMEM((STEP * heads, head_dim), jnp.float32),
            pltpu.VMEM((8 * heads, WINDOW), jnp.float32),
            pltpu.VMEM((heads, 8, WINDOW), dtype),
            pltpu.VMEM((heads, 8, head_dim), jnp.float32),
            pltpu.VMEM((LANES, w_out.shape[0]), dtype),
            pltpu.VMEM((heads, 8, head_dim), dtype),
            pltpu.VMEM((heads, head_dim), dtype),
            pltpu.VMEM((heads, head_dim), dtype),
            dma((depth, 8)), dma((2, 8)), dma((2 * steps,)),
        ],
        compiler_params=pltpu.CompilerParams(vmem_limit_bytes=BUILD_VMEM),
        name='build',
    )(lengths, proj, cos, sin, residual, w_out, k_rows, v_rows, land, swap)


def turn(length, head_dim):
    half_dim = head_dim // 2
    inv_freq = THETA ** (-2.0 * jnp.arange(half_dim, dtype=jnp.float32) / head_dim)
    angles = length.astype(jnp.float32) * inv_freq
    cos, sin = jnp.cos(angles), jnp.sin(angles)
    return jnp.concatenate([cos, cos])[None], jnp.concatenate([-sin, sin])[None]


def solution(mesh):
    head_spec = P('dp', None, 'sh', None)
    row_spec = P(('dp', 'sh'))
    full_spec = P(None, None)

    def per_device(k_prefill, v_prefill, lengths, residual, norm_gain, w_query, w_key, w_value, w_out):
        num_rows, seq_len, _, head_dim = k_prefill.shape
        kv_heads = w_key.shape[1] // head_dim
        k_rows = k_prefill.reshape(num_rows, seq_len, head_dim)
        v_rows = v_prefill.reshape(num_rows, seq_len, head_dim)
        cos, sin = turn(lengths[lax.axis_index('sh')], head_dim)
        gain = norm_gain[None]
        lengths, cos, sin, gain = lax.optimization_barrier((lengths, cos, sin, gain))
        packed, size = pack(lengths, k_rows, v_rows)
        sizes = (list_length(seq_len) - BASE) // QUANTUM
        land = lax.switch(size[0], [functools.partial(more, extra=i * QUANTUM) for i in range(sizes + 1)], packed)
        land, swap, proj = base(packed, k_rows, v_rows, residual, gain, w_query, w_key, w_value, land)
        k_cache, v_cache, resid_out = build(lengths, proj, cos, sin, residual, w_out, k_rows, v_rows, land, swap, kv_heads)
        return resid_out, k_cache[None], v_cache[None]
    return jax.shard_map(per_device, mesh=mesh, in_specs=(head_spec, head_spec, P('dp'), P(('dp', 'sh'), None), P(None), full_spec, full_spec, full_spec, full_spec), out_specs=(P(('dp', 'sh'), None), row_spec, row_spec), check_vma=False)
```

```python
import functools

import jax
import jax.numpy as jnp
import numpy as np
from jax import lax
from jax.experimental import pallas as pl
from jax.experimental.pallas import tpu as pltpu
from jax.sharding import PartitionSpec as P

WINDOW = 4096
THETA = 10000.0
EPS = 1e-5
ALIGN = 16
HALF = 2192
BASE = 2 * HALF
QUANTUM = 128
STEP = 512
PARTS = 4
BASE_VMEM = 14 * 2**20
BUILD_VMEM = 18 * 2**20
LANES = 16
ANY = pl.BlockSpec(memory_space=pl.ANY)
VMEM = pl.BlockSpec(memory_space=pltpu.VMEM)
SMEM = pl.BlockSpec(memory_space=pltpu.SMEM)
HBM = pl.BlockSpec(memory_space=pltpu.HBM)


def list_length(seq_len):
    return BASE + -(-(2 * seq_len - BASE) // QUANTUM) * QUANTUM


def span(length):
    return (length + (ALIGN - 1)) // ALIGN * ALIGN


def pack_kernel(len_ref, k_ref, v_ref, out_ref, size_ref, lists, first_sem, second_sem, store_sem, *, seq_len):
    chip = lax.axis_index('sh') // 2
    list_len = lists.shape[2]
    peers = [chip + 1 - 2 * (chip % 2), (chip + 2) % 4, 3 - chip]

    def first(t, k):
        src = (k_ref, v_ref)[t]
        return pltpu.make_async_copy(src.at[2 * peers[k]], lists.at[t, k, pl.ds(0, seq_len)], first_sem.at[t, k])

    def second(t, k):
        src = (k_ref, v_ref)[t]
        start = pl.multiple_of(span(len_ref[2 * peers[k]]), ALIGN)
        return pltpu.make_async_copy(src.at[2 * peers[k] + 1], lists.at[t, k, pl.ds(start, seq_len)], second_sem.at[t, k])

    extra = (list_len - BASE) // 2

    def stores(t, k):
        total = span(len_ref[2 * peers[k]]) + span(len_ref[2 * peers[k] + 1])
        yield None, pltpu.make_async_copy(lists.at[t, k, pl.ds(0, BASE)], out_ref.at[t, k, pl.ds(0, BASE)], store_sem.at[t, k, 0])
        for i in range(2):
            rows = pl.ds(BASE + i * extra, extra)
            yield total > BASE + i * extra, pltpu.make_async_copy(lists.at[t, k, rows], out_ref.at[t, k, rows], store_sem.at[t, k, 1 + i])

    order = [(t, k) for k in range(3) for t in range(2)]
    for t, k in order:
        first(t, k).start()
    longest = span(len_ref[0]) + span(len_ref[1])
    for c in range(1, len_ref.shape[0] // 2):
        longest = jnp.maximum(longest, span(len_ref[2 * c]) + span(len_ref[2 * c + 1]))
    size_ref[0] = jnp.clip((longest - BASE + QUANTUM - 1) // QUANTUM, 0, (list_len - BASE) // QUANTUM)
    for t, k in order:
        first(t, k).wait()
        second(t, k).start()
    for t, k in order:
        second(t, k).wait()
        for live, copy in stores(t, k):
            if live is None:
                copy.start()
            else:
                pl.when(live)(copy.start)
    for t, k in order:
        for live, copy in stores(t, k):
            if live is None:
                copy.wait()
            else:
                pl.when(live)(copy.wait)


def pack(lengths, k_rows, v_rows):
    seq_len, head_dim = k_rows.shape[1:]
    shape = (2, 3, list_length(seq_len), head_dim)
    return pl.pallas_call(
        functools.partial(pack_kernel, seq_len=seq_len),
        out_shape=(jax.ShapeDtypeStruct(shape, k_rows.dtype), jax.ShapeDtypeStruct((1,), jnp.int32)),
        in_specs=[SMEM, HBM, HBM],
        out_specs=(HBM, SMEM),
        scratch_shapes=[pltpu.VMEM(shape, k_rows.dtype), pltpu.SemaphoreType.DMA((2, 3)), pltpu.SemaphoreType.DMA((2, 3)), pltpu.SemaphoreType.DMA((2, 3, 3))],
        compiler_params=pltpu.CompilerParams(vmem_limit_bytes=60 * 2**20),
        name='pack',
    )(lengths, k_rows, v_rows)


def project(res_ref, gain_ref, weights, proj_ref, normed, total, ring, ring_sem):
    depth, side, _ = ring.shape
    resid = res_ref[...].astype(jnp.float32)
    inv_rms = lax.rsqrt(jnp.sum(resid * resid, axis=-1, keepdims=True) / resid.shape[-1] + EPS)
    lanes = gain_ref.shape[1]
    for r in range(gain_ref.shape[0]):
        cols = slice(r * lanes, (r + 1) * lanes)
        row = (resid[:, cols] * inv_rms * gain_ref[r:r + 1, :].astype(jnp.float32)).astype(normed.dtype)
        normed[:, cols] = jnp.broadcast_to(row, (normed.shape[0], lanes))
    total[...] = jnp.zeros_like(total)
    deep = normed.shape[1] // side

    def at(i):
        return pl.multiple_of(i // deep * side, side), pl.multiple_of(i % deep * side, side)

    def fetch(i):
        left, top = at(i)
        first = 0
        for w_ref in weights:
            width = w_ref.shape[1]

            @pl.when((left >= first) & (left < first + width))
            def _(w_ref=w_ref, first=first):
                here = pl.multiple_of(left - first, side)
                pltpu.make_async_copy(w_ref.at[pl.ds(top, side), pl.ds(here, side)], ring.at[i % depth], ring_sem.at[i % depth]).start()
            first += width

    blocks = total.shape[1] // side * deep

    def prime(i, carry):
        fetch(i)
        return carry
    lax.fori_loop(0, depth - 1, prime, 0)

    def step(i, carry):
        @pl.when(i + depth - 1 < blocks)
        def _():
            fetch(i + depth - 1)
        pltpu.make_async_copy(weights[0].at[pl.ds(0, side), pl.ds(0, side)], ring.at[i % depth], ring_sem.at[i % depth]).wait()
        left, top = at(i)
        total[:, pl.ds(left, side)] += jnp.dot(normed[:, pl.ds(top, side)], ring[i % depth], preferred_element_type=jnp.float32)
        return carry
    lax.fori_loop(0, blocks, step, 0)
    proj_ref[...] = total[...].astype(proj_ref.dtype)


def remote(src, dst, send, recv, device):
    return pltpu.make_async_remote_copy(src_ref=src, dst_ref=dst, send_sem=send, recv_sem=recv, device_id={'sh': device}, device_id_type=pl.DeviceIdType.MESH)


ORDER = [(t, k) for k in range(3) for t in range(2)]


def more_kernel(packed, land, send_sem, recv_sem, *, extra):
    me = lax.axis_index('sh')
    core = me % 2
    chip = me // 2
    peers = [chip + 1 - 2 * (chip % 2), (chip + 2) % 4, 3 - chip]
    rows = pl.ds(BASE, extra)

    def out(t, k):
        return remote(packed.at[t, k, rows], land.at[t, k, core, rows], send_sem.at[t, k], recv_sem.at[t, k, core], 2 * peers[k] + 1)

    def into(t, k, q):
        here = land.at[t, k, q, rows]
        return remote(here, here, send_sem.at[t, k], recv_sem.at[t, k, q], me)

    for t, k in ORDER:
        out(t, k).start()
    for t, k in ORDER:
        out(t, k).wait_send()

    @pl.when(core == 1)
    def _():
        for t, k in ORDER:
            for q in range(2):
                into(t, k, q).wait_recv()


def nothing_kernel(packed, land):
    pass


def more(packed, *, extra):
    shape = jax.ShapeDtypeStruct(packed.shape[:2] + (2,) + packed.shape[2:], packed.dtype)
    if not extra:
        return pl.pallas_call(nothing_kernel, out_shape=shape, in_specs=[HBM], out_specs=HBM, compiler_params=pltpu.CompilerParams(vmem_limit_bytes=60 * 2**20), name='more_0')(packed)
    dma = pltpu.SemaphoreType.DMA
    return pl.pallas_call(
        functools.partial(more_kernel, extra=extra),
        out_shape=shape,
        in_specs=[HBM],
        out_specs=HBM,
        scratch_shapes=[dma((2, 3)), dma((2, 3, 2))],
        compiler_params=pltpu.CompilerParams(has_side_effects=True, vmem_limit_bytes=60 * 2**20),
        name=f'more_{extra}',
    )(packed)


def base_kernel(packed, k_ref, v_ref, res_ref, gain_ref, wq_ref, wk_ref, wv_ref, wout_ref, _, land, swap, proj_ref, *rest):
    held_refs, (normed, total, ring, ring_sem, held_sem, send_sem, recv_sem, fsend_sem, frecv_sem, ssend_sem, srecv_sem) = rest[:PARTS], rest[PARTS:]
    me = lax.axis_index('sh')
    core = me % 2
    chip = me // 2
    partner = me + 1 - 2 * core
    peers = [chip + 1 - 2 * (chip % 2), (chip + 2) % 4, 3 - chip]

    def main(t, k, half):
        rows = pl.ds(half * HALF, HALF)
        return remote(packed.at[t, k, rows], land.at[t, k, core, rows], send_sem.at[t, k, half], recv_sem.at[t, k, core], 2 * peers[k] + half)

    def forward(t, k, q):
        rows = land.at[t, k, q, pl.ds(core * HALF, HALF)]
        return remote(rows, rows, fsend_sem.at[t, k, q], frecv_sem.at[t, k, q], partner)

    def main_in(t, k, q):
        rows = land.at[t, k, q, pl.ds(core * HALF, HALF)]
        return remote(rows, rows, fsend_sem.at[t, k, q], recv_sem.at[t, k, q], partner)

    def forward_in(t, k, q):
        rows = land.at[t, k, q, pl.ds((1 - core) * HALF, HALF)]
        return remote(rows, rows, fsend_sem.at[t, k, q], frecv_sem.at[t, k, q], partner)

    def across(t):
        return remote((k_ref, v_ref)[t].at[partner], swap.at[t], ssend_sem.at[t], srecv_sem.at[t], partner)

    for t, k in ORDER:
        for half in range(2):
            main(t, k, half).start()
    for t in range(2):
        across(t).start()
    project(res_ref, gain_ref, (wq_ref, wk_ref, wv_ref), proj_ref, normed, total, ring, ring_sem)
    part = wout_ref.shape[0] // PARTS
    held = [pltpu.make_async_copy(wout_ref.at[pl.ds(i * part, part)], held_refs[i], held_sem.at[i]) for i in range(PARTS)]
    for copy in held:
        copy.start()
    for t, k in ORDER:
        for q in range(2):
            main_in(t, k, q).wait_recv()
            forward(t, k, q).start()
    for t in range(2):
        across(t).wait()
    for t, k in ORDER:
        for half in range(2):
            main(t, k, half).wait_send()
    for t, k in ORDER:
        for q in range(2):
            forward(t, k, q).wait_send()
            forward_in(t, k, q).wait_recv()
    for copy in held:
        copy.wait()


def base(packed, k_rows, v_rows, residual, gain, w_query, w_key, w_value, w_out, land):
    seq_len, head_dim = k_rows.shape[1:]
    dtype = k_rows.dtype
    dma = pltpu.SemaphoreType.DMA
    model_dim = residual.shape[1]
    proj_dim = w_query.shape[1] + w_key.shape[1] + w_value.shape[1]
    return pl.pallas_call(
        base_kernel,
        out_shape=(jax.ShapeDtypeStruct(land.shape, dtype), jax.ShapeDtypeStruct((2, seq_len, head_dim), dtype), jax.ShapeDtypeStruct((LANES, proj_dim), dtype), )+ PARTS * (jax.ShapeDtypeStruct((w_out.shape[0] // PARTS, w_out.shape[1]), dtype),),
        in_specs=[HBM, HBM, HBM, VMEM, VMEM, HBM, HBM, HBM, HBM, HBM],
        out_specs=(HBM, HBM, VMEM) + PARTS * (ANY,),
        scratch_shapes=[
            pltpu.VMEM((LANES, model_dim), dtype), pltpu.VMEM((LANES, proj_dim), jnp.float32), pltpu.VMEM((8, 512, 512), dtype), dma((8,)), dma((PARTS,)),
            dma((2, 3, 2)), dma((2, 3, 2)), dma((2, 3, 2)), dma((2, 3, 2)), dma((2,)), dma((2,)),
        ],
        input_output_aliases={9: 0},
        compiler_params=pltpu.CompilerParams(has_side_effects=True, vmem_limit_bytes=BASE_VMEM),
        name='base',
    )(packed, k_rows, v_rows, residual, gain, w_query, w_key, w_value, w_out, land)


def build_kernel(len_ref, proj_ref, freq_ref, res_ref, *rest, depth):
    w_refs, (k_ref, v_ref, land, swap, kc_ref, vc_ref, xout_ref, ring, tail, wide, scores, probs, mixed, ovec, q_ref, knew_ref, vnew_ref, ring_sem, tail_sem) = rest[:PARTS], rest[PARTS:]
    step = pl.program_id(0)
    steps = WINDOW // STEP
    me = lax.axis_index('sh')
    core, chip, n = me % 2, me // 2, len_ref[me]
    offset = core * span(len_ref[2 * chip])
    chips = [chip, chip + 1 - 2 * (chip % 2), (chip + 2) % 4, 3 - chip]
    extra = tail.shape[2]
    heads = tail.shape[1]
    head_dim = tail.shape[3]

    def copies(t, start, size, dst, sem):
        own = 2 * chip + core
        other = 2 * chip + 1 - core
        rows = pl.ds(start, size)
        yield pltpu.make_async_copy((k_ref, v_ref)[t].at[me, rows], dst.at[own], sem.at[0])
        yield pltpu.make_async_copy(swap.at[t, rows], dst.at[other], sem.at[1])
        far = pl.ds(pl.multiple_of(offset + start, ALIGN), size)
        for k in range(3):
            for q in range(2):
                yield pltpu.make_async_copy(land.at[t, k, q, far], dst.at[2 * chips[k + 1] + q], sem.at[2 + 2 * k + q])

    def heads_of_row():
        q_width = ovec.shape[1]
        group = q_width // (heads * head_dim)

        def part(at):
            return proj_ref[:1, at:at + head_dim]

        angles = n.astype(jnp.float32) * freq_ref[...]
        lane = lax.broadcasted_iota(jnp.int32, angles.shape, 1)
        cos, sin = jnp.cos(angles), jnp.sin(angles)
        sin = jnp.where(lane < head_dim // 2, -sin, sin)

        def turned(at):
            vals = part(at).astype(jnp.float32)
            return (vals * cos + pltpu.roll(vals, head_dim // 2, 1) * sin).astype(q_ref.dtype)

        for h in range(heads):
            q_ref[h] = jnp.concatenate([turned((h * group + g) * head_dim) for g in range(group)] + [jnp.zeros((q_ref.shape[1] - group, head_dim), q_ref.dtype)], axis=0)
        knew_ref[...] = jnp.concatenate([turned(q_width + h * head_dim) for h in range(heads)], axis=0)
        vnew_ref[...] = jnp.concatenate([part(q_width + (heads + h) * head_dim) for h in range(heads)], axis=0)

    def for_step(s, act):
        for t in range(2):
            local = s - t * steps
            @pl.when((local >= 0) & (local < steps) & (local * STEP < n))
            def _():
                for copy in copies(t, pl.multiple_of(local * STEP, STEP), STEP, ring.at[s % depth], ring_sem.at[s % depth]):
                    act(copy)

    def for_tail(t, act):
        @pl.when(n > WINDOW)
        def _():
            for copy in copies(t, WINDOW, extra, tail.at[t], tail_sem.at[t]):
                act(copy)

    @pl.when(step == 0)
    def _():
        for_tail(0, lambda c: c.start())
        for s in range(depth - 1):
            for_step(jnp.int32(s), lambda c: c.start())
        for_tail(1, lambda c: c.start())
        mixed[...] = jnp.zeros_like(mixed)
        heads_of_row()
    for_step(step + depth - 1, lambda c: c.start())
    for_step(step, lambda c: c.wait())

    def assemble(t, local, new_ref, out_ref, use):
        first = local * STEP
        newest = lax.rem(n, WINDOW)
        wraps = (local == 0) & (n > WINDOW)
        dead = first > n
        plain = (first + STEP <= n) & ~wraps & ((newest < first) | (newest >= first + STEP))

        @pl.when(wraps)
        def _():
            for_tail(t, lambda c: c.wait())

        def fill(vals_of):
            for h in range(heads):
                vals = vals_of(h)
                wide[pl.ds(h, STEP, stride=heads), :] = vals.astype(jnp.float32)
                use(h, vals)
            out_ref[...] = wide[...].reshape(STEP, heads, head_dim).astype(out_ref.dtype)

        @pl.when(plain)
        def _():
            fill(lambda h: ring[step % depth, h])

        @pl.when(dead)
        def _():
            out_ref[...] = jnp.zeros_like(out_ref)
            use(None, None)

        @pl.when(~plain & ~dead)
        def _():
            pos = first + lax.broadcasted_iota(jnp.int32, (STEP, head_dim), 0)

            def patched(h):
                vals = ring[step % depth, h]
                low = jnp.where(pos[:extra] < n - WINDOW, tail[t, h], vals[:extra])
                vals = jnp.concatenate([low, vals[extra:]], axis=0)
                vals = jnp.where(pos < n, vals, jnp.zeros_like(vals))
                return jnp.where(pos == newest, jnp.broadcast_to(new_ref[h:h + 1, :], vals.shape), vals)
            fill(patched)

    @pl.when(step < steps)
    def _():
        slots = step * STEP + lax.broadcasted_iota(jnp.int32, (8, STEP), 1)
        live = (slots <= n) | (n >= WINDOW)

        def use(h, vals):
            if h is None:
                scores[:, pl.ds(pl.multiple_of(step * STEP, STEP), STEP)] = jnp.full((scores.shape[0], STEP), -jnp.inf)
                return
            s = lax.dot_general(q_ref[h], vals, (((1,), (1,)), ((), ())), preferred_element_type=jnp.float32) / head_dim ** 0.5
            scores[pl.ds(8 * h, 8), pl.ds(pl.multiple_of(step * STEP, STEP), STEP)] = jnp.where(live, s, -jnp.inf)
        assemble(0, step, knew_ref, kc_ref, use)

    @pl.when(step == steps)
    def _():
        for h in range(heads):
            s = scores[8 * h:8 * h + 8, :]
            e = jnp.exp(s - jnp.max(s, axis=-1, keepdims=True))
            probs[h] = (e / jnp.sum(e, axis=-1, keepdims=True)).astype(probs.dtype)

    @pl.when(step >= steps)
    def _():
        local = step - steps

        def use(h, vals):
            if h is None:
                return
            p = probs[h, :, pl.ds(pl.multiple_of(local * STEP, STEP), STEP)]
            mixed[h] += jnp.dot(p, vals, preferred_element_type=jnp.float32)
        assemble(1, local, vnew_ref, vc_ref, use)

    @pl.when(step == 2 * steps - 1)
    def _():
        group = ovec.shape[1] // (heads * head_dim)
        for h in range(heads):
            o = mixed[h].astype(ovec.dtype)
            for g in range(group):
                cols = pl.ds((h * group + g) * head_dim, head_dim)
                ovec[:, cols] = jnp.broadcast_to(o[g:g + 1], (ovec.shape[0], head_dim))
        width = 512

        def column(c, carry):
            cols = pl.ds(pl.multiple_of(c * width, width), width)
            acc = jnp.zeros((ovec.shape[0], width), jnp.float32)
            for i, w_ref in enumerate(w_refs):
                acc += jnp.dot(ovec[:, i * w_ref.shape[0]:(i + 1) * w_ref.shape[0]], w_ref[:, cols], preferred_element_type=jnp.float32)
            xout_ref[:, cols] = (res_ref[:, cols].astype(jnp.float32) + acc[:1]).astype(xout_ref.dtype)
            return carry
        lax.fori_loop(0, xout_ref.shape[1] // width, column, 0)


def build(lengths, proj, freq, residual, w_out, k_rows, v_rows, land, swap, heads):
    seq_len, head_dim = k_rows.shape[1:]
    steps = WINDOW // STEP
    depth = 4
    dtype = k_rows.dtype
    cache = jax.ShapeDtypeStruct((WINDOW, heads, head_dim), dtype)
    block = (STEP, heads, head_dim)
    dma = pltpu.SemaphoreType.DMA
    return pl.pallas_call(
        functools.partial(build_kernel, depth=depth),
        grid=(2 * steps,),
        out_shape=(cache, cache, jax.ShapeDtypeStruct(residual.shape, dtype)),
        in_specs=[SMEM, VMEM, VMEM, VMEM] + PARTS * [VMEM] + [HBM, HBM, HBM, HBM],
        out_specs=(pl.BlockSpec(block, lambda i: (jnp.minimum(i, steps - 1), 0, 0)), pl.BlockSpec(block, lambda i: (jnp.maximum(i - steps, 0), 0, 0)), VMEM),
        scratch_shapes=[
            pltpu.VMEM((depth, heads, STEP, head_dim), dtype),
            pltpu.VMEM((2, heads, seq_len - WINDOW, head_dim), dtype),
            pltpu.VMEM((STEP * heads, head_dim), jnp.float32),
            pltpu.VMEM((8 * heads, WINDOW), jnp.float32),
            pltpu.VMEM((heads, 8, WINDOW), dtype),
            pltpu.VMEM((heads, 8, head_dim), jnp.float32),
            pltpu.VMEM((LANES, PARTS * w_out[0].shape[0]), dtype),
            pltpu.VMEM((heads, 8, head_dim), dtype),
            pltpu.VMEM((heads, head_dim), dtype),
            pltpu.VMEM((heads, head_dim), dtype),
            dma((depth, 8)), dma((2, 8)),
        ],
        compiler_params=pltpu.CompilerParams(vmem_limit_bytes=BUILD_VMEM),
        name='build',
    )(lengths, proj, freq, residual, *w_out, k_rows, v_rows, land, swap)


def frequencies(head_dim):
    half = THETA ** (-2.0 * np.arange(head_dim // 2, dtype=np.float64) / head_dim)
    return np.concatenate([half, half])[None].astype(np.float32)


def solution(mesh):
    head_spec = P('dp', None, 'sh', None)
    row_spec = P(('dp', 'sh'))
    full_spec = P(None, None)

    def per_device(k_prefill, v_prefill, lengths, residual, norm_gain, w_query, w_key, w_value, w_out):
        num_rows, seq_len, _, head_dim = k_prefill.shape
        kv_heads = w_key.shape[1] // head_dim
        k_rows = k_prefill.reshape(num_rows, seq_len, head_dim)
        v_rows = v_prefill.reshape(num_rows, seq_len, head_dim)
        packed, size = pack(lengths, k_rows, v_rows)
        sizes = (list_length(seq_len) - BASE) // QUANTUM
        land = lax.switch(size[0], [functools.partial(more, extra=i * QUANTUM) for i in range(sizes + 1)], packed)
        land, swap, proj, *held = base(packed, k_rows, v_rows, residual, norm_gain.reshape(-1, head_dim), w_query, w_key, w_value, w_out, land)
        k_cache, v_cache, resid_out = build(lengths, proj, jnp.asarray(frequencies(head_dim)), residual, held, k_rows, v_rows, land, swap, kv_heads)
        return resid_out, k_cache[None], v_cache[None]
    return jax.shard_map(per_device, mesh=mesh, in_specs=(head_spec, head_spec, P('dp'), P(('dp', 'sh'), None), P(None), full_spec, full_spec, full_spec, full_spec), out_specs=(P(('dp', 'sh'), None), row_spec, row_spec), check_vma=False)
```

```python
import functools

import jax
import jax.numpy as jnp
import numpy as np
from jax import lax
from jax.experimental import pallas as pl
from jax.experimental.pallas import tpu as pltpu
from jax.sharding import PartitionSpec as P

WINDOW = 4096
THETA = 10000.0
EPS = 1e-5
ALIGN = 16
HALF = 2208
BASE = 2 * HALF
CUTS = 4
PIECES = 2
QUANTUM = 128
STEP = 512
PARTS = 4
BASE_VMEM = 14 * 2**20
BUILD_VMEM = 20 * 2**20
LANES = 16
ORDER = [(t, k) for k in range(3) for t in range(2)]
ANY = pl.BlockSpec(memory_space=pl.ANY)
VMEM = pl.BlockSpec(memory_space=pltpu.VMEM)
SMEM = pl.BlockSpec(memory_space=pltpu.SMEM)
HBM = pl.BlockSpec(memory_space=pltpu.HBM)


def list_length(seq_len):
    return BASE + -(-(2 * seq_len - BASE) // QUANTUM) * QUANTUM


def span(length):
    return (length + (ALIGN - 1)) // ALIGN * ALIGN


def pack_kernel(len_ref, k_ref, v_ref, out_ref, size_ref, lists, first_sem, second_sem, store_sem, *, seq_len):
    chip = lax.axis_index('sh') // 2
    list_len = lists.shape[2]
    peers = [chip + 1 - 2 * (chip % 2), (chip + 2) % 4, 3 - chip]

    part = seq_len // CUTS

    def spans_of(k):
        return span(len_ref[2 * peers[k]]), span(len_ref[2 * peers[k] + 1])

    def loads(t, k, second):
        src = (k_ref, v_ref)[t]
        spans = spans_of(k)
        for i in range(CUTS):
            start = pl.multiple_of(second * spans[0] + i * part, ALIGN)
            yield spans[second] > i * part, pltpu.make_async_copy(src.at[2 * peers[k] + second, pl.ds(i * part, part)], lists.at[t, k, pl.ds(start, part)], (first_sem, second_sem)[second].at[t, k, i])

    def stores(t, k):
        size = list_len // (2 * CUTS)
        for i in range(2 * CUTS):
            rows = pl.ds(i * size, size)
            yield sum(spans_of(k)) > i * size, pltpu.make_async_copy(lists.at[t, k, rows], out_ref.at[t, k, rows], store_sem.at[t, k, i])

    def start(copies):
        for live, copy in copies:
            pl.when(live)(copy.start)

    def wait(copies):
        for live, copy in copies:
            pl.when(live)(copy.wait)

    for t, k in ORDER:
        start(loads(t, k, 0))
    longest = span(len_ref[0]) + span(len_ref[1])
    for c in range(1, len_ref.shape[0] // 2):
        longest = jnp.maximum(longest, span(len_ref[2 * c]) + span(len_ref[2 * c + 1]))
    size_ref[0] = jnp.clip((longest - BASE + QUANTUM - 1) // QUANTUM, 0, (list_len - BASE) // QUANTUM)
    for t, k in ORDER:
        wait(loads(t, k, 0))
        start(loads(t, k, 1))
    for t, k in ORDER:
        wait(loads(t, k, 1))
        start(stores(t, k))
    for t, k in ORDER:
        wait(stores(t, k))


def pack(lengths, k_rows, v_rows):
    seq_len, head_dim = k_rows.shape[1:]
    shape = (2, 3, list_length(seq_len), head_dim)
    return pl.pallas_call(
        functools.partial(pack_kernel, seq_len=seq_len),
        out_shape=(jax.ShapeDtypeStruct(shape, k_rows.dtype), jax.ShapeDtypeStruct((1,), jnp.int32)),
        in_specs=[SMEM, HBM, HBM],
        out_specs=(HBM, SMEM),
        scratch_shapes=[pltpu.VMEM(shape, k_rows.dtype), pltpu.SemaphoreType.DMA((2, 3, CUTS)), pltpu.SemaphoreType.DMA((2, 3, CUTS)), pltpu.SemaphoreType.DMA((2, 3, 2 * CUTS))],
        compiler_params=pltpu.CompilerParams(vmem_limit_bytes=60 * 2**20),
        name='pack',
    )(lengths, k_rows, v_rows)


def project(res_ref, gain_ref, weights, proj_ref, normed, total, ring, ring_sem):
    depth, side, _ = ring.shape
    resid = res_ref[...].astype(jnp.float32)
    inv_rms = lax.rsqrt(jnp.sum(resid * resid, axis=-1, keepdims=True) / resid.shape[-1] + EPS)
    lanes = gain_ref.shape[1]
    for r in range(gain_ref.shape[0]):
        cols = slice(r * lanes, (r + 1) * lanes)
        row = (resid[:, cols] * inv_rms * gain_ref[r:r + 1, :].astype(jnp.float32)).astype(normed.dtype)
        normed[:, cols] = jnp.broadcast_to(row, (normed.shape[0], lanes))
    total[...] = jnp.zeros_like(total)
    deep = normed.shape[1] // side

    def at(i):
        return pl.multiple_of(i // deep * side, side), pl.multiple_of(i % deep * side, side)

    def fetch(i):
        left, top = at(i)
        first = 0
        for w_ref in weights:
            width = w_ref.shape[1]

            @pl.when((left >= first) & (left < first + width))
            def _(w_ref=w_ref, first=first):
                here = pl.multiple_of(left - first, side)
                pltpu.make_async_copy(w_ref.at[pl.ds(top, side), pl.ds(here, side)], ring.at[i % depth], ring_sem.at[i % depth]).start()
            first += width

    blocks = total.shape[1] // side * deep

    def prime(i, carry):
        fetch(i)
        return carry
    lax.fori_loop(0, depth - 1, prime, 0)

    def step(i, carry):
        @pl.when(i + depth - 1 < blocks)
        def _():
            fetch(i + depth - 1)
        pltpu.make_async_copy(weights[0].at[pl.ds(0, side), pl.ds(0, side)], ring.at[i % depth], ring_sem.at[i % depth]).wait()
        left, top = at(i)
        total[:, pl.ds(left, side)] += jnp.dot(normed[:, pl.ds(top, side)], ring[i % depth], preferred_element_type=jnp.float32)
        return carry
    lax.fori_loop(0, blocks, step, 0)
    proj_ref[...] = total[...].astype(proj_ref.dtype)


def remote(src, dst, send, recv, device):
    return pltpu.make_async_remote_copy(src_ref=src, dst_ref=dst, send_sem=send, recv_sem=recv, device_id={'sh': device}, device_id_type=pl.DeviceIdType.MESH)


def more_kernel(packed, land, send_sem, recv_sem, *, extra):
    me = lax.axis_index('sh')
    core = me % 2
    chip = me // 2
    peers = [chip + 1 - 2 * (chip % 2), (chip + 2) % 4, 3 - chip]
    rows = pl.ds(BASE, extra)

    def out(t, k):
        return remote(packed.at[t, k, rows], land.at[t, k, core, rows], send_sem.at[t, k], recv_sem.at[t, k, core], 2 * peers[k] + 1)

    def into(t, k, q):
        here = land.at[t, k, q, rows]
        return remote(here, here, send_sem.at[t, k], recv_sem.at[t, k, q], me)

    for t, k in ORDER:
        out(t, k).start()
    for t, k in ORDER:
        out(t, k).wait_send()

    @pl.when(core == 1)
    def _():
        for t, k in ORDER:
            for q in range(2):
                into(t, k, q).wait_recv()


def nothing_kernel(packed, land):
    pass


def more(packed, *, extra):
    shape = jax.ShapeDtypeStruct((2, 4, 2) + packed.shape[2:], packed.dtype)
    if not extra:
        return pl.pallas_call(nothing_kernel, out_shape=shape, in_specs=[HBM], out_specs=HBM, compiler_params=pltpu.CompilerParams(vmem_limit_bytes=60 * 2**20), name='more_0')(packed)
    dma = pltpu.SemaphoreType.DMA
    return pl.pallas_call(
        functools.partial(more_kernel, extra=extra),
        out_shape=shape,
        in_specs=[HBM],
        out_specs=HBM,
        scratch_shapes=[dma((2, 3)), dma((2, 3, 2))],
        compiler_params=pltpu.CompilerParams(has_side_effects=True, vmem_limit_bytes=60 * 2**20),
        name=f'more_{extra}',
    )(packed)


def base_kernel(packed, k_ref, v_ref, res_ref, gain_ref, wq_ref, wk_ref, wv_ref, wout_ref, _, land, proj_ref, *rest):
    held_refs, (normed, total, ring, ring_sem, held_sem, send_sem, recv_sem, fsend_sem, frecv_sem, ssend_sem, srecv_sem) = rest[:PARTS], rest[PARTS:]
    me = lax.axis_index('sh')
    core = me % 2
    chip = me // 2
    partner = me + 1 - 2 * core
    peers = [chip + 1 - 2 * (chip % 2), (chip + 2) % 4, 3 - chip]

    size = HALF // PIECES

    def main(t, k, half, p):
        rows = pl.ds(half * HALF + p * size, size)
        return remote(packed.at[t, k, rows], land.at[t, k, core, rows], send_sem.at[t, k, half, p], recv_sem.at[t, k, core, p], 2 * peers[k] + half)

    def forward(t, k, q, p):
        rows = land.at[t, k, q, pl.ds(core * HALF + p * size, size)]
        return remote(rows, rows, fsend_sem.at[t, k, q, p], frecv_sem.at[t, k, q, p], partner)

    def main_in(t, k, q, p):
        rows = land.at[t, k, q, pl.ds(core * HALF + p * size, size)]
        return remote(rows, rows, fsend_sem.at[t, k, q, p], recv_sem.at[t, k, q, p], partner)

    def forward_in(t, k, q, p):
        rows = land.at[t, k, q, pl.ds((1 - core) * HALF + p * size, size)]
        return remote(rows, rows, fsend_sem.at[t, k, q, p], frecv_sem.at[t, k, q, p], partner)

    def across(t):
        return remote((k_ref, v_ref)[t].at[partner], land.at[t, 3, core, pl.ds(0, k_ref.shape[1])], ssend_sem.at[t], srecv_sem.at[t], partner)

    def across_in(t):
        rows = land.at[t, 3, 1 - core, pl.ds(0, k_ref.shape[1])]
        return remote(rows, rows, ssend_sem.at[t], srecv_sem.at[t], partner)

    for t, k in ORDER:
        for half in range(2):
            for p in range(PIECES):
                main(t, k, half, p).start()
    for t in range(2):
        across(t).start()
    project(res_ref, gain_ref, (wq_ref, wk_ref, wv_ref), proj_ref, normed, total, ring, ring_sem)
    part = wout_ref.shape[0] // PARTS
    held = [pltpu.make_async_copy(wout_ref.at[pl.ds(i * part, part)], held_refs[i], held_sem.at[i]) for i in range(PARTS)]
    for copy in held:
        copy.start()
    for t, k in ORDER:
        for p in range(PIECES):
            for q in range(2):
                main_in(t, k, q, p).wait_recv()
                forward(t, k, q, p).start()
    for t in range(2):
        across(t).wait_send()
        across_in(t).wait_recv()
    for t, k in ORDER:
        for half in range(2):
            for p in range(PIECES):
                main(t, k, half, p).wait_send()
    for t, k in ORDER:
        for q in range(2):
            for p in range(PIECES):
                forward(t, k, q, p).wait_send()
                forward_in(t, k, q, p).wait_recv()
    for copy in held:
        copy.wait()


def base(packed, k_rows, v_rows, residual, gain, w_query, w_key, w_value, w_out, land):
    dtype = k_rows.dtype
    dma = pltpu.SemaphoreType.DMA
    model_dim = residual.shape[1]
    proj_dim = w_query.shape[1] + w_key.shape[1] + w_value.shape[1]
    return pl.pallas_call(
        base_kernel,
        out_shape=(jax.ShapeDtypeStruct(land.shape, dtype), jax.ShapeDtypeStruct((LANES, proj_dim), dtype), )+ PARTS * (jax.ShapeDtypeStruct((w_out.shape[0] // PARTS, w_out.shape[1]), dtype),),
        in_specs=[HBM, HBM, HBM, VMEM, VMEM, HBM, HBM, HBM, HBM, HBM],
        out_specs=(HBM, VMEM) + PARTS * (ANY,),
        scratch_shapes=[
            pltpu.VMEM((LANES, model_dim), dtype), pltpu.VMEM((LANES, proj_dim), jnp.float32), pltpu.VMEM((8, 512, 512), dtype), dma((8,)), dma((PARTS,)),
            dma((2, 3, 2, PIECES)), dma((2, 3, 2, PIECES)), dma((2, 3, 2, PIECES)), dma((2, 3, 2, PIECES)), dma((2,)), dma((2,)),
        ],
        input_output_aliases={9: 0},
        compiler_params=pltpu.CompilerParams(has_side_effects=True, vmem_limit_bytes=BASE_VMEM),
        name='base',
    )(packed, k_rows, v_rows, residual, gain, w_query, w_key, w_value, w_out, land)


def build_kernel(len_ref, proj_ref, freq_ref, res_ref, *rest, depth):
    w_refs, (k_ref, v_ref, land, kc_ref, vc_ref, xout_ref, ring, tail, wide, scores, probs, mixed, ovec, q_ref, knew_ref, vnew_ref, ring_sem, tail_sem) = rest[:PARTS], rest[PARTS:]
    step = pl.program_id(0)
    steps = WINDOW // STEP
    me = lax.axis_index('sh')
    core, chip, n = me % 2, me // 2, len_ref[me]
    offset = core * span(len_ref[2 * chip])
    chips = [chip, chip + 1 - 2 * (chip % 2), (chip + 2) % 4, 3 - chip]
    extra = tail.shape[2]
    heads = tail.shape[1]
    head_dim = tail.shape[3]

    def copies(t, start, size, dst, sem):
        own = 2 * chip + core
        other = 2 * chip + 1 - core
        rows = pl.ds(start, size)
        yield pltpu.make_async_copy((k_ref, v_ref)[t].at[me, rows], dst.at[own], sem.at[0])
        yield pltpu.make_async_copy(land.at[t, 3, 1 - core, rows], dst.at[other], sem.at[1])
        far = pl.ds(pl.multiple_of(offset + start, ALIGN), size)
        for k in range(3):
            for q in range(2):
                yield pltpu.make_async_copy(land.at[t, k, q, far], dst.at[2 * chips[k + 1] + q], sem.at[2 + 2 * k + q])

    def heads_of_row():
        q_width = ovec.shape[1]
        group = q_width // (heads * head_dim)

        def part(at):
            return proj_ref[:1, at:at + head_dim]

        angles = n.astype(jnp.float32) * freq_ref[...]
        lane = lax.broadcasted_iota(jnp.int32, angles.shape, 1)
        cos, sin = jnp.cos(angles), jnp.sin(angles)
        sin = jnp.where(lane < head_dim // 2, -sin, sin)

        def turned(at):
            vals = part(at).astype(jnp.float32)
            return (vals * cos + pltpu.roll(vals, head_dim // 2, 1) * sin).astype(q_ref.dtype)

        for h in range(heads):
            q_ref[h] = jnp.concatenate([turned((h * group + g) * head_dim) for g in range(group)] + [jnp.zeros((q_ref.shape[1] - group, head_dim), q_ref.dtype)], axis=0)
        knew_ref[...] = jnp.concatenate([turned(q_width + h * head_dim) for h in range(heads)], axis=0)
        vnew_ref[...] = jnp.concatenate([part(q_width + (heads + h) * head_dim) for h in range(heads)], axis=0)

    def for_step(s, act):
        for t in range(2):
            local = s - t * steps
            @pl.when((local >= 0) & (local < steps) & (local * STEP < n))
            def _():
                for copy in copies(t, pl.multiple_of(local * STEP, STEP), STEP, ring.at[s % depth], ring_sem.at[s % depth]):
                    act(copy)

    def for_tail(t, act):
        @pl.when(n > WINDOW)
        def _():
            for copy in copies(t, WINDOW, extra, tail.at[t], tail_sem.at[t]):
                act(copy)

    @pl.when(step == 0)
    def _():
        for_tail(0, lambda c: c.start())
        for s in range(depth - 1):
            for_step(jnp.int32(s), lambda c: c.start())
        for_tail(1, lambda c: c.start())
        mixed[...] = jnp.zeros_like(mixed)
        heads_of_row()
    for_step(step + depth - 1, lambda c: c.start())
    for_step(step, lambda c: c.wait())

    def assemble(t, local, new_ref, out_ref, use):
        first = local * STEP
        newest = lax.rem(n, WINDOW)
        wraps = (local == 0) & (n > WINDOW)
        dead = first > n
        plain = (first + STEP <= n) & ~wraps & ((newest < first) | (newest >= first + STEP))

        @pl.when(wraps)
        def _():
            for_tail(t, lambda c: c.wait())

        def fill(vals_of):
            for h in range(heads):
                vals = vals_of(h)
                wide[pl.ds(h, STEP, stride=heads), :] = vals.astype(jnp.float32)
                use(h, vals)
            out_ref[...] = wide[...].reshape(STEP, heads, head_dim).astype(out_ref.dtype)

        @pl.when(plain)
        def _():
            fill(lambda h: ring[step % depth, h])

        @pl.when(dead)
        def _():
            out_ref[...] = jnp.zeros_like(out_ref)
            use(None, None)

        @pl.when(~plain & ~dead)
        def _():
            pos = first + lax.broadcasted_iota(jnp.int32, (STEP, head_dim), 0)

            def patched(h):
                vals = ring[step % depth, h]
                low = jnp.where(pos[:extra] < n - WINDOW, tail[t, h], vals[:extra])
                vals = jnp.concatenate([low, vals[extra:]], axis=0)
                vals = jnp.where(pos < n, vals, jnp.zeros_like(vals))
                return jnp.where(pos == newest, jnp.broadcast_to(new_ref[h:h + 1, :], vals.shape), vals)
            fill(patched)

    @pl.when(step < steps)
    def _():
        slots = step * STEP + lax.broadcasted_iota(jnp.int32, (8, STEP), 1)
        live = (slots <= n) | (n >= WINDOW)

        def use(h, vals):
            if h is None:
                scores[:, pl.ds(pl.multiple_of(step * STEP, STEP), STEP)] = jnp.full((scores.shape[0], STEP), -jnp.inf)
                return
            s = lax.dot_general(q_ref[h], vals, (((1,), (1,)), ((), ())), preferred_element_type=jnp.float32) / head_dim ** 0.5
            scores[pl.ds(8 * h, 8), pl.ds(pl.multiple_of(step * STEP, STEP), STEP)] = jnp.where(live, s, -jnp.inf)
        assemble(0, step, knew_ref, kc_ref, use)

    @pl.when(step == steps)
    def _():
        for h in range(heads):
            s = scores[8 * h:8 * h + 8, :]
            e = jnp.exp(s - jnp.max(s, axis=-1, keepdims=True))
            probs[h] = (e / jnp.sum(e, axis=-1, keepdims=True)).astype(probs.dtype)

    @pl.when(step >= steps)
    def _():
        local = step - steps

        def use(h, vals):
            if h is None:
                return
            p = probs[h, :, pl.ds(pl.multiple_of(local * STEP, STEP), STEP)]
            mixed[h] += jnp.dot(p, vals, preferred_element_type=jnp.float32)
        assemble(1, local, vnew_ref, vc_ref, use)

    @pl.when(step == 2 * steps - 1)
    def _():
        group = ovec.shape[1] // (heads * head_dim)
        for h in range(heads):
            o = mixed[h].astype(ovec.dtype)
            for g in range(group):
                cols = pl.ds((h * group + g) * head_dim, head_dim)
                ovec[:, cols] = jnp.broadcast_to(o[g:g + 1], (ovec.shape[0], head_dim))
        width = 512

        def column(c, carry):
            cols = pl.ds(pl.multiple_of(c * width, width), width)
            acc = jnp.zeros((ovec.shape[0], width), jnp.float32)
            for i, w_ref in enumerate(w_refs):
                acc += jnp.dot(ovec[:, i * w_ref.shape[0]:(i + 1) * w_ref.shape[0]], w_ref[:, cols], preferred_element_type=jnp.float32)
            xout_ref[:, cols] = (res_ref[:, cols].astype(jnp.float32) + acc[:1]).astype(xout_ref.dtype)
            return carry
        lax.fori_loop(0, xout_ref.shape[1] // width, column, 0)


def build(lengths, proj, freq, residual, w_out, k_rows, v_rows, land, heads):
    seq_len, head_dim = k_rows.shape[1:]
    steps = WINDOW // STEP
    depth = 6
    dtype = k_rows.dtype
    cache = jax.ShapeDtypeStruct((WINDOW, heads, head_dim), dtype)
    block = (STEP, heads, head_dim)
    dma = pltpu.SemaphoreType.DMA
    return pl.pallas_call(
        functools.partial(build_kernel, depth=depth),
        grid=(2 * steps,),
        out_shape=(cache, cache, jax.ShapeDtypeStruct(residual.shape, dtype)),
        in_specs=[SMEM, VMEM, VMEM, VMEM] + PARTS * [VMEM] + [HBM, HBM, HBM],
        out_specs=(pl.BlockSpec(block, lambda i: (jnp.minimum(i, steps - 1), 0, 0)), pl.BlockSpec(block, lambda i: (jnp.maximum(i - steps, 0), 0, 0)), VMEM),
        scratch_shapes=[
            pltpu.VMEM((depth, heads, STEP, head_dim), dtype),
            pltpu.VMEM((2, heads, seq_len - WINDOW, head_dim), dtype),
            pltpu.VMEM((STEP * heads, head_dim), jnp.float32),
            pltpu.VMEM((8 * heads, WINDOW), jnp.float32),
            pltpu.VMEM((heads, 8, WINDOW), dtype),
            pltpu.VMEM((heads, 8, head_dim), jnp.float32),
            pltpu.VMEM((LANES, PARTS * w_out[0].shape[0]), dtype),
            pltpu.VMEM((heads, 8, head_dim), dtype),
            pltpu.VMEM((heads, head_dim), dtype),
            pltpu.VMEM((heads, head_dim), dtype),
            dma((depth, 8)), dma((2, 8)),
        ],
        compiler_params=pltpu.CompilerParams(vmem_limit_bytes=BUILD_VMEM),
        name='build',
    )(lengths, proj, freq, residual, *w_out, k_rows, v_rows, land)


def frequencies(head_dim):
    half = THETA ** (-2.0 * np.arange(head_dim // 2, dtype=np.float64) / head_dim)
    return np.concatenate([half, half])[None].astype(np.float32)


def solution(mesh):
    head_spec = P('dp', None, 'sh', None)
    row_spec = P(('dp', 'sh'))
    full_spec = P(None, None)

    def per_device(k_prefill, v_prefill, lengths, residual, norm_gain, w_query, w_key, w_value, w_out):
        num_rows, seq_len, _, head_dim = k_prefill.shape
        kv_heads = w_key.shape[1] // head_dim
        k_rows = k_prefill.reshape(num_rows, seq_len, head_dim)
        v_rows = v_prefill.reshape(num_rows, seq_len, head_dim)
        packed, size = pack(lengths, k_rows, v_rows)
        sizes = (list_length(seq_len) - BASE) // QUANTUM
        land = lax.switch(size[0], [functools.partial(more, extra=i * QUANTUM) for i in range(sizes + 1)], packed)
        land, proj, *held = base(packed, k_rows, v_rows, residual, norm_gain.reshape(-1, head_dim), w_query, w_key, w_value, w_out, land)
        k_cache, v_cache, resid_out = build(lengths, proj, jnp.asarray(frequencies(head_dim)), residual, held, k_rows, v_rows, land, kv_heads)
        return resid_out, k_cache[None], v_cache[None]
    return jax.shard_map(per_device, mesh=mesh, in_specs=(head_spec, head_spec, P('dp'), P(('dp', 'sh'), None), P(None), full_spec, full_spec, full_spec, full_spec), out_specs=(P(('dp', 'sh'), None), row_spec, row_spec), check_vma=False)
```

```python
import functools

import jax
import jax.numpy as jnp
import numpy as np
from jax import lax
from jax.experimental import pallas as pl
from jax.experimental.pallas import tpu as pltpu
from jax.sharding import PartitionSpec as P

WINDOW = 4096
THETA = 10000.0
EPS = 1e-5
ALIGN = 16
HALF = 2208
BASE = 2 * HALF
CUTS = 4
PIECES = 2
QUANTUM = 128
STEP = 512
SLAB = 128
GROUP = 4
BLOCK = 128
PITCH = 12
PARTS = 4
BASE_VMEM = 14 * 2**20
BUILD_VMEM = 20 * 2**20
LANES = 16
ORDER = [(t, k) for k in range(3) for t in range(2)]
ANY = pl.BlockSpec(memory_space=pl.ANY)
VMEM = pl.BlockSpec(memory_space=pltpu.VMEM)
SMEM = pl.BlockSpec(memory_space=pltpu.SMEM)
HBM = pl.BlockSpec(memory_space=pltpu.HBM)


def list_length(seq_len):
    return BASE + -(-(2 * seq_len - BASE) // QUANTUM) * QUANTUM


def span(length):
    return (length + (ALIGN - 1)) // ALIGN * ALIGN


def pack_kernel(len_ref, k_ref, v_ref, out_ref, size_ref, lists, first_sem, second_sem, store_sem, *, seq_len):
    chip = lax.axis_index('sh') // 2
    list_len = lists.shape[2]
    peers = [chip + 1 - 2 * (chip % 2), (chip + 2) % 4, 3 - chip]

    part = seq_len // CUTS

    def spans_of(k):
        return span(len_ref[2 * peers[k]]), span(len_ref[2 * peers[k] + 1])

    def loads(t, k, second):
        src = (k_ref, v_ref)[t]
        spans = spans_of(k)
        for i in range(CUTS):
            start = pl.multiple_of(second * spans[0] + i * part, ALIGN)
            yield spans[second] > i * part, pltpu.make_async_copy(src.at[2 * peers[k] + second, pl.ds(i * part, part)], lists.at[t, k, pl.ds(start, part)], (first_sem, second_sem)[second].at[t, k, i])

    def stores(t, k):
        size = list_len // (2 * CUTS)
        for i in range(2 * CUTS):
            rows = pl.ds(i * size, size)
            yield sum(spans_of(k)) > i * size, pltpu.make_async_copy(lists.at[t, k, rows], out_ref.at[t, k, rows], store_sem.at[t, k, i])

    def start(copies):
        for live, copy in copies:
            pl.when(live)(copy.start)

    def wait(copies):
        for live, copy in copies:
            pl.when(live)(copy.wait)

    for t, k in ORDER:
        start(loads(t, k, 0))
    longest = span(len_ref[0]) + span(len_ref[1])
    for c in range(1, len_ref.shape[0] // 2):
        longest = jnp.maximum(longest, span(len_ref[2 * c]) + span(len_ref[2 * c + 1]))
    size_ref[0] = jnp.clip((longest - BASE + QUANTUM - 1) // QUANTUM, 0, (list_len - BASE) // QUANTUM)
    for t, k in ORDER:
        wait(loads(t, k, 0))
        start(loads(t, k, 1))
    for t, k in ORDER:
        wait(loads(t, k, 1))
        start(stores(t, k))
    for t, k in ORDER:
        wait(stores(t, k))


def pack(lengths, k_rows, v_rows):
    seq_len, head_dim = k_rows.shape[1:]
    shape = (2, 3, list_length(seq_len), head_dim)
    return pl.pallas_call(
        functools.partial(pack_kernel, seq_len=seq_len),
        out_shape=(jax.ShapeDtypeStruct(shape, k_rows.dtype), jax.ShapeDtypeStruct((1,), jnp.int32)),
        in_specs=[SMEM, HBM, HBM],
        out_specs=(HBM, SMEM),
        scratch_shapes=[pltpu.VMEM(shape, k_rows.dtype), pltpu.SemaphoreType.DMA((2, 3, CUTS)), pltpu.SemaphoreType.DMA((2, 3, CUTS)), pltpu.SemaphoreType.DMA((2, 3, 2 * CUTS))],
        compiler_params=pltpu.CompilerParams(vmem_limit_bytes=60 * 2**20),
        name='pack',
    )(lengths, k_rows, v_rows)


def project(res_ref, gain_ref, weights, proj_ref, normed, total, ring, ring_sem):
    depth, side, _ = ring.shape
    resid = res_ref[...].astype(jnp.float32)
    inv_rms = lax.rsqrt(jnp.sum(resid * resid, axis=-1, keepdims=True) / resid.shape[-1] + EPS)
    lanes = gain_ref.shape[1]
    for r in range(gain_ref.shape[0]):
        cols = slice(r * lanes, (r + 1) * lanes)
        row = (resid[:, cols] * inv_rms * gain_ref[r:r + 1, :].astype(jnp.float32)).astype(normed.dtype)
        normed[:, cols] = jnp.broadcast_to(row, (normed.shape[0], lanes))
    total[...] = jnp.zeros_like(total)
    deep = normed.shape[1] // side

    def at(i):
        return pl.multiple_of(i // deep * side, side), pl.multiple_of(i % deep * side, side)

    def fetch(i):
        left, top = at(i)
        first = 0
        for w_ref in weights:
            width = w_ref.shape[1]

            @pl.when((left >= first) & (left < first + width))
            def _(w_ref=w_ref, first=first):
                here = pl.multiple_of(left - first, side)
                pltpu.make_async_copy(w_ref.at[pl.ds(top, side), pl.ds(here, side)], ring.at[i % depth], ring_sem.at[i % depth]).start()
            first += width

    blocks = total.shape[1] // side * deep

    def prime(i, carry):
        fetch(i)
        return carry
    lax.fori_loop(0, depth - 1, prime, 0)

    def step(i, carry):
        @pl.when(i + depth - 1 < blocks)
        def _():
            fetch(i + depth - 1)
        pltpu.make_async_copy(weights[0].at[pl.ds(0, side), pl.ds(0, side)], ring.at[i % depth], ring_sem.at[i % depth]).wait()
        left, top = at(i)
        total[:, pl.ds(left, side)] += jnp.dot(normed[:, pl.ds(top, side)], ring[i % depth], preferred_element_type=jnp.float32)
        return carry
    lax.fori_loop(0, blocks, step, 0)
    proj_ref[...] = total[...].astype(proj_ref.dtype)


def remote(src, dst, send, recv, device):
    return pltpu.make_async_remote_copy(src_ref=src, dst_ref=dst, send_sem=send, recv_sem=recv, device_id={'sh': device}, device_id_type=pl.DeviceIdType.MESH)


def more_kernel(packed, land, send_sem, recv_sem, *, extra):
    me = lax.axis_index('sh')
    core = me % 2
    chip = me // 2
    peers = [chip + 1 - 2 * (chip % 2), (chip + 2) % 4, 3 - chip]
    rows = pl.ds(BASE, extra)

    def out(t, k):
        return remote(packed.at[t, k, rows], land.at[t, k, core, rows], send_sem.at[t, k], recv_sem.at[t, k, core], 2 * peers[k] + 1)

    def into(t, k, q):
        here = land.at[t, k, q, rows]
        return remote(here, here, send_sem.at[t, k], recv_sem.at[t, k, q], me)

    for t, k in ORDER:
        out(t, k).start()
    for t, k in ORDER:
        out(t, k).wait_send()

    @pl.when(core == 1)
    def _():
        for t, k in ORDER:
            for q in range(2):
                into(t, k, q).wait_recv()


def nothing_kernel(packed, land):
    pass


def more(packed, *, extra):
    shape = jax.ShapeDtypeStruct((2, 4, 2) + packed.shape[2:], packed.dtype)
    if not extra:
        return pl.pallas_call(nothing_kernel, out_shape=shape, in_specs=[HBM], out_specs=HBM, compiler_params=pltpu.CompilerParams(vmem_limit_bytes=60 * 2**20), name='more_0')(packed)
    dma = pltpu.SemaphoreType.DMA
    return pl.pallas_call(
        functools.partial(more_kernel, extra=extra),
        out_shape=shape,
        in_specs=[HBM],
        out_specs=HBM,
        scratch_shapes=[dma((2, 3)), dma((2, 3, 2))],
        compiler_params=pltpu.CompilerParams(has_side_effects=True, vmem_limit_bytes=60 * 2**20),
        name=f'more_{extra}',
    )(packed)


def base_kernel(packed, k_ref, v_ref, res_ref, gain_ref, wq_ref, wk_ref, wv_ref, wout_ref, _, land, proj_ref, *rest):
    held_refs, (normed, total, ring, ring_sem, held_sem, send_sem, recv_sem, fsend_sem, frecv_sem, ssend_sem, srecv_sem) = rest[:PARTS], rest[PARTS:]
    me = lax.axis_index('sh')
    core = me % 2
    chip = me // 2
    partner = me + 1 - 2 * core
    peers = [chip + 1 - 2 * (chip % 2), (chip + 2) % 4, 3 - chip]

    size = HALF // PIECES

    def main(t, k, half, p):
        rows = pl.ds(half * HALF + p * size, size)
        return remote(packed.at[t, k, rows], land.at[t, k, core, rows], send_sem.at[t, k, half, p], recv_sem.at[t, k, core, p], 2 * peers[k] + half)

    def forward(t, k, q, p):
        rows = land.at[t, k, q, pl.ds(core * HALF + p * size, size)]
        return remote(rows, rows, fsend_sem.at[t, k, q, p], frecv_sem.at[t, k, q, p], partner)

    def main_in(t, k, q, p):
        rows = land.at[t, k, q, pl.ds(core * HALF + p * size, size)]
        return remote(rows, rows, fsend_sem.at[t, k, q, p], recv_sem.at[t, k, q, p], partner)

    def forward_in(t, k, q, p):
        rows = land.at[t, k, q, pl.ds((1 - core) * HALF + p * size, size)]
        return remote(rows, rows, fsend_sem.at[t, k, q, p], frecv_sem.at[t, k, q, p], partner)

    def across(t):
        return remote((k_ref, v_ref)[t].at[partner], land.at[t, 3, core, pl.ds(0, k_ref.shape[1])], ssend_sem.at[t], srecv_sem.at[t], partner)

    def across_in(t):
        rows = land.at[t, 3, 1 - core, pl.ds(0, k_ref.shape[1])]
        return remote(rows, rows, ssend_sem.at[t], srecv_sem.at[t], partner)

    for t, k in ORDER:
        for half in range(2):
            for p in range(PIECES):
                main(t, k, half, p).start()
    for t in range(2):
        across(t).start()
    project(res_ref, gain_ref, (wq_ref, wk_ref, wv_ref), proj_ref, normed, total, ring, ring_sem)
    slabs, part, slab = held_refs[0].shape

    def hold(c, carry):
        for i in range(PARTS):
            pltpu.make_async_copy(wout_ref.at[pl.ds(i * part, part), pl.ds(pl.multiple_of(c * slab, slab), slab)], held_refs[i].at[c], held_sem.at[i]).start()
        return carry
    lax.fori_loop(0, slabs, hold, 0)
    for t, k in ORDER:
        for p in range(PIECES):
            for q in range(2):
                main_in(t, k, q, p).wait_recv()
                forward(t, k, q, p).start()
    for t in range(2):
        across(t).wait_send()
        across_in(t).wait_recv()
    for t, k in ORDER:
        for half in range(2):
            for p in range(PIECES):
                main(t, k, half, p).wait_send()
    for t, k in ORDER:
        for q in range(2):
            for p in range(PIECES):
                forward(t, k, q, p).wait_send()
                forward_in(t, k, q, p).wait_recv()
    for i in range(PARTS):
        pltpu.make_async_copy(held_refs[i], held_refs[i], held_sem.at[i]).wait()


def base(packed, k_rows, v_rows, residual, gain, w_query, w_key, w_value, w_out, land):
    dtype = k_rows.dtype
    dma = pltpu.SemaphoreType.DMA
    model_dim = residual.shape[1]
    proj_dim = w_query.shape[1] + w_key.shape[1] + w_value.shape[1]
    return pl.pallas_call(
        base_kernel,
        out_shape=(jax.ShapeDtypeStruct(land.shape, dtype), jax.ShapeDtypeStruct((LANES, proj_dim), dtype), )+ PARTS * (jax.ShapeDtypeStruct((w_out.shape[1] // SLAB, w_out.shape[0] // PARTS, SLAB), dtype),),
        in_specs=[HBM, HBM, HBM, VMEM, VMEM, HBM, HBM, HBM, HBM, HBM],
        out_specs=(HBM, VMEM) + PARTS * (ANY,),
        scratch_shapes=[
            pltpu.VMEM((LANES, model_dim), dtype), pltpu.VMEM((LANES, proj_dim), jnp.float32), pltpu.VMEM((8, 512, 512), dtype), dma((8,)), dma((PARTS,)),
            dma((2, 3, 2, PIECES)), dma((2, 3, 2, PIECES)), dma((2, 3, 2, PIECES)), dma((2, 3, 2, PIECES)), dma((2,)), dma((2,)),
        ],
        input_output_aliases={9: 0},
        compiler_params=pltpu.CompilerParams(has_side_effects=True, vmem_limit_bytes=BASE_VMEM),
        name='base',
    )(packed, k_rows, v_rows, residual, gain, w_query, w_key, w_value, w_out, land)


def build_kernel(len_ref, proj_ref, freq_ref, res_ref, *rest, depth):
    w_refs, (k_ref, v_ref, land, kc_ref, vc_ref, xout_ref, ring, tail, wide, made, scores, probs, mixed, ovec, q_ref, knew_ref, vnew_ref, ring_sem, tail_sem, made_sem) = rest[:PARTS], rest[PARTS:]
    step = pl.program_id(0)
    steps = WINDOW // STEP
    me = lax.axis_index('sh')
    core, chip, n = me % 2, me // 2, len_ref[me]
    offset = core * span(len_ref[2 * chip])
    chips = [chip, chip + 1 - 2 * (chip % 2), (chip + 2) % 4, 3 - chip]
    extra = tail.shape[2]
    heads = tail.shape[1]
    head_dim = tail.shape[3]

    def copies(t, start, size, dst, sem):
        own = 2 * chip + core
        other = 2 * chip + 1 - core
        rows = pl.ds(start, size)
        yield pltpu.make_async_copy((k_ref, v_ref)[t].at[me, rows], dst.at[own], sem)
        yield pltpu.make_async_copy(land.at[t, 3, 1 - core, rows], dst.at[other], sem)
        far = pl.ds(pl.multiple_of(offset + start, ALIGN), size)
        for k in range(3):
            for q in range(2):
                yield pltpu.make_async_copy(land.at[t, k, q, far], dst.at[2 * chips[k + 1] + q], sem)

    def heads_of_row():
        q_width = ovec.shape[1]
        group = q_width // (heads * head_dim)

        def part(at):
            return proj_ref[:1, at:at + head_dim]

        angles = n.astype(jnp.float32) * freq_ref[...]
        lane = lax.broadcasted_iota(jnp.int32, angles.shape, 1)
        cos, sin = jnp.cos(angles), jnp.sin(angles)
        sin = jnp.where(lane < head_dim // 2, -sin, sin)

        def turned(at):
            vals = part(at).astype(jnp.float32)
            return (vals * cos + pltpu.roll(vals, head_dim // 2, 1) * sin).astype(q_ref.dtype)

        for h in range(heads):
            q_ref[h] = jnp.concatenate([turned((h * group + g) * head_dim) for g in range(group)] + [jnp.zeros((q_ref.shape[1] - group, head_dim), q_ref.dtype)], axis=0)
        knew_ref[...] = jnp.concatenate([turned(q_width + h * head_dim) for h in range(heads)], axis=0)
        vnew_ref[...] = jnp.concatenate([part(q_width + (heads + h) * head_dim) for h in range(heads)], axis=0)

    def chunk(s, then):
        for t in range(2):
            local = s - t * steps
            pl.when((local >= 0) & (local < steps) & (local * STEP < n))(functools.partial(then, t, local))

    def fetch(s):
        def then(t, local):
            for copy in copies(t, pl.multiple_of(local * STEP, STEP), STEP, ring.at[s % depth], ring_sem.at[s % depth]):
                copy.start()
        chunk(s, then)

    def arrived(s):
        def then(t, local):
            whole = ring.at[s % depth]
            pltpu.make_async_copy(whole, whole, ring_sem.at[s % depth]).wait()
        chunk(s, then)

    def fetch_tail(t):
        @pl.when(n > WINDOW)
        def _():
            for copy in copies(t, WINDOW, extra, tail.at[t], tail_sem.at[t]):
                copy.start()

    def save(s, out_ref, local):
        rows = pl.ds(pl.multiple_of(local * STEP * heads, STEP * heads), STEP * heads)
        return pltpu.make_async_copy(made.at[s % 2], out_ref.at[rows], made_sem.at[s % 2])

    @pl.when(step == 0)
    def _():
        fetch_tail(0)
        for s in range(depth - 1):
            fetch(jnp.int32(s))
        fetch_tail(1)
        mixed[...] = jnp.zeros_like(mixed)
        heads_of_row()
    fetch(step + depth - 1)
    arrived(step)

    @pl.when(step >= 2)
    def _():
        save(step, kc_ref, 0).wait()

    def assemble(t, local, new_ref, out_ref, use):
        first = local * STEP
        newest = lax.rem(n, WINDOW)
        wraps = (local == 0) & (n > WINDOW)
        dead = first > n
        plain = (first + STEP <= n) & ~wraps & ((newest < first) | (newest >= first + STEP))
        slot = step % depth
        out = step % 2

        @pl.when(wraps)
        def _():
            whole = tail.at[t]
            pltpu.make_async_copy(whole, whole, tail_sem.at[t]).wait()

        @pl.when(~plain & ~dead)
        def _():
            pos = first + lax.broadcasted_iota(jnp.int32, (STEP, head_dim), 0)
            for h in range(heads):
                vals = ring[slot, h]
                low = jnp.where(pos[:extra] < n - WINDOW, tail[t, h], vals[:extra])
                vals = jnp.concatenate([low, vals[extra:]], axis=0)
                vals = jnp.where(pos < n, vals, jnp.zeros_like(vals))
                ring[slot, h] = jnp.where(pos == newest, jnp.broadcast_to(new_ref[h:h + 1, :], vals.shape), vals)

        @pl.when(dead)
        def _():
            made[out] = jnp.zeros(made.shape[1:], made.dtype)
            use(None, None, None)

        @pl.when(~dead)
        def _():
            def mix(b, carry):
                for h in range(heads):
                    vals = ring[slot, h, pl.ds(pl.multiple_of(b * BLOCK, BLOCK), BLOCK), :]
                    wide[pl.ds(h, BLOCK, stride=PITCH), :] = vals.astype(jnp.float32)
                    use(h, b, vals)
                rows = jnp.concatenate([wide[PITCH * p:PITCH * p + heads, :] for p in range(BLOCK)], axis=0)
                made[out, pl.ds(pl.multiple_of(b * BLOCK * heads, BLOCK * heads), BLOCK * heads), :] = rows.astype(made.dtype)
                return carry
            lax.fori_loop(0, STEP // BLOCK, mix, 0)
        save(step, out_ref, local).start()

    def slots_of(local, b, size):
        return pl.ds(pl.multiple_of(local * STEP + b * BLOCK, BLOCK), size)

    @pl.when(step < steps)
    def _():
        def use(h, b, vals):
            if h is None:
                scores[:, slots_of(step, 0, STEP)] = jnp.full((scores.shape[0], STEP), -jnp.inf)
                return
            slots = step * STEP + b * BLOCK + lax.broadcasted_iota(jnp.int32, (8, BLOCK), 1)
            live = (slots <= n) | (n >= WINDOW)
            s = lax.dot_general(q_ref[h], vals, (((1,), (1,)), ((), ())), preferred_element_type=jnp.float32) / head_dim ** 0.5
            scores[pl.ds(8 * h, 8), slots_of(step, b, BLOCK)] = jnp.where(live, s, -jnp.inf)
        assemble(0, step, knew_ref, kc_ref, use)

    @pl.when(step == steps)
    def _():
        for h in range(heads):
            s = scores[8 * h:8 * h + 8, :]
            e = jnp.exp(s - jnp.max(s, axis=-1, keepdims=True))
            probs[h] = (e / jnp.sum(e, axis=-1, keepdims=True)).astype(probs.dtype)

    @pl.when(step >= steps)
    def _():
        local = step - steps

        def use(h, b, vals):
            if h is None:
                return
            p = probs[h, :, slots_of(local, b, BLOCK)]
            mixed[h] += jnp.dot(p, vals, preferred_element_type=jnp.float32)
        assemble(1, local, vnew_ref, vc_ref, use)

    @pl.when(step == 2 * steps - 1)
    def _():
        group = ovec.shape[1] // (heads * head_dim)
        for h in range(heads):
            o = mixed[h].astype(ovec.dtype)
            for g in range(group):
                cols = pl.ds((h * group + g) * head_dim, head_dim)
                ovec[:, cols] = jnp.broadcast_to(o[g:g + 1], (ovec.shape[0], head_dim))
        slabs, part, slab = w_refs[0].shape
        width = GROUP * slab

        def column(c, carry):
            acc = jnp.zeros((ovec.shape[0], width), jnp.float32)
            for i, w_ref in enumerate(w_refs):
                block = jnp.concatenate([w_ref[c * GROUP + j] for j in range(GROUP)], axis=1)
                acc += jnp.dot(ovec[:, i * part:(i + 1) * part], block, preferred_element_type=jnp.float32)
            cols = pl.ds(pl.multiple_of(c * width, width), width)
            xout_ref[:, cols] = (res_ref[:, cols].astype(jnp.float32) + acc[:1]).astype(xout_ref.dtype)
            return carry
        lax.fori_loop(0, slabs // GROUP, column, 0)
        for s in range(2 * steps - 2, 2 * steps):
            save(s, vc_ref, 0).wait()


def build(lengths, proj, freq, residual, w_out, k_rows, v_rows, land, heads):
    seq_len, head_dim = k_rows.shape[1:]
    steps = WINDOW // STEP
    depth = 6
    dtype = k_rows.dtype
    cache = jax.ShapeDtypeStruct((WINDOW * heads, head_dim), dtype)
    dma = pltpu.SemaphoreType.DMA
    return pl.pallas_call(
        functools.partial(build_kernel, depth=depth),
        grid=(2 * steps,),
        out_shape=(cache, cache, jax.ShapeDtypeStruct(residual.shape, dtype)),
        in_specs=[SMEM, VMEM, VMEM, VMEM] + PARTS * [VMEM] + [HBM, HBM, HBM],
        out_specs=(HBM, HBM, VMEM),
        scratch_shapes=[
            pltpu.VMEM((depth, heads, STEP, head_dim), dtype),
            pltpu.VMEM((2, heads, seq_len - WINDOW, head_dim), dtype),
            pltpu.VMEM((BLOCK * PITCH, head_dim), jnp.float32),
            pltpu.VMEM((2, STEP * heads, head_dim), dtype),
            pltpu.VMEM((8 * heads, WINDOW), jnp.float32),
            pltpu.VMEM((heads, 8, WINDOW), dtype),
            pltpu.VMEM((heads, 8, head_dim), jnp.float32),
            pltpu.VMEM((LANES, PARTS * w_out[0].shape[1]), dtype),
            pltpu.VMEM((heads, 8, head_dim), dtype),
            pltpu.VMEM((heads, head_dim), dtype),
            pltpu.VMEM((heads, head_dim), dtype),
            dma((depth,)), dma((2,)), dma((2,)),
        ],
        compiler_params=pltpu.CompilerParams(vmem_limit_bytes=BUILD_VMEM),
        name='build',
    )(lengths, proj, freq, residual, *w_out, k_rows, v_rows, land)


def frequencies(head_dim):
    half = THETA ** (-2.0 * np.arange(head_dim // 2, dtype=np.float64) / head_dim)
    return np.concatenate([half, half])[None].astype(np.float32)


def solution(mesh):
    head_spec = P('dp', None, 'sh', None)
    row_spec = P(('dp', 'sh'))
    full_spec = P(None, None)

    def per_device(k_prefill, v_prefill, lengths, residual, norm_gain, w_query, w_key, w_value, w_out):
        num_rows, seq_len, _, head_dim = k_prefill.shape
        kv_heads = w_key.shape[1] // head_dim
        k_rows = k_prefill.reshape(num_rows, seq_len, head_dim)
        v_rows = v_prefill.reshape(num_rows, seq_len, head_dim)
        packed, size = pack(lengths, k_rows, v_rows)
        sizes = (list_length(seq_len) - BASE) // QUANTUM
        land = lax.switch(size[0], [functools.partial(more, extra=i * QUANTUM) for i in range(sizes + 1)], packed)
        land, proj, *held = base(packed, k_rows, v_rows, residual, norm_gain.reshape(-1, head_dim), w_query, w_key, w_value, w_out, land)
        k_cache, v_cache, resid_out = build(lengths, proj, jnp.asarray(frequencies(head_dim)), residual, held, k_rows, v_rows, land, kv_heads)
        shape = (1, WINDOW, kv_heads, head_dim)
        return resid_out, k_cache.reshape(shape), v_cache.reshape(shape)
    return jax.shard_map(per_device, mesh=mesh, in_specs=(head_spec, head_spec, P('dp'), P(('dp', 'sh'), None), P(None), full_spec, full_spec, full_spec, full_spec), out_specs=(P(('dp', 'sh'), None), row_spec, row_spec), check_vma=False)
```

```python
import functools

import jax
import jax.numpy as jnp
import numpy as np
from jax import lax
from jax.experimental import pallas as pl
from jax.experimental.pallas import tpu as pltpu
from jax.sharding import PartitionSpec as P

WINDOW = 4096
THETA = 10000.0
EPS = 1e-5
ALIGN = 16
HALF = 2208
BASE = 2 * HALF
CUTS = 4
PIECES = 2
QUANTUM = 128
STEP = 512
SLAB = 128
GROUP = 4
MADE = 4
SAVES = 2
BLOCK = 128
PITCH = 12
PARTS = 4
BASE_VMEM = 14 * 2**20
BUILD_VMEM = 18 * 2**20
LANES = 16
ORDER = [(t, k) for k in range(3) for t in range(2)]
ANY = pl.BlockSpec(memory_space=pl.ANY)
VMEM = pl.BlockSpec(memory_space=pltpu.VMEM)
SMEM = pl.BlockSpec(memory_space=pltpu.SMEM)
HBM = pl.BlockSpec(memory_space=pltpu.HBM)


def list_length(seq_len):
    return BASE + -(-(2 * seq_len - BASE) // QUANTUM) * QUANTUM


def span(length):
    return (length + (ALIGN - 1)) // ALIGN * ALIGN


def pack_kernel(len_ref, k_ref, v_ref, out_ref, size_ref, lists, first_sem, second_sem, store_sem, *, seq_len):
    chip = lax.axis_index('sh') // 2
    list_len = lists.shape[2]
    peers = [chip + 1 - 2 * (chip % 2), (chip + 2) % 4, 3 - chip]

    part = seq_len // CUTS

    def spans_of(k):
        return span(len_ref[2 * peers[k]]), span(len_ref[2 * peers[k] + 1])

    def loads(t, k, second):
        src = (k_ref, v_ref)[t]
        spans = spans_of(k)
        for i in range(CUTS):
            start = pl.multiple_of(second * spans[0] + i * part, ALIGN)
            yield spans[second] > i * part, pltpu.make_async_copy(src.at[2 * peers[k] + second, pl.ds(i * part, part)], lists.at[t, k, pl.ds(start, part)], (first_sem, second_sem)[second].at[t, k, i])

    def stores(t, k):
        size = list_len // (2 * CUTS)
        for i in range(2 * CUTS):
            rows = pl.ds(i * size, size)
            yield sum(spans_of(k)) > i * size, pltpu.make_async_copy(lists.at[t, k, rows], out_ref.at[t, k, rows], store_sem.at[t, k, i])

    def start(copies):
        for live, copy in copies:
            pl.when(live)(copy.start)

    def wait(copies):
        for live, copy in copies:
            pl.when(live)(copy.wait)

    for t, k in ORDER:
        start(loads(t, k, 0))
    longest = span(len_ref[0]) + span(len_ref[1])
    for c in range(1, len_ref.shape[0] // 2):
        longest = jnp.maximum(longest, span(len_ref[2 * c]) + span(len_ref[2 * c + 1]))
    size_ref[0] = jnp.clip((longest - BASE + QUANTUM - 1) // QUANTUM, 0, (list_len - BASE) // QUANTUM)
    for t, k in ORDER:
        wait(loads(t, k, 0))
        start(loads(t, k, 1))
    for t, k in ORDER:
        wait(loads(t, k, 1))
        start(stores(t, k))
    for t, k in ORDER:
        wait(stores(t, k))


def pack(lengths, k_rows, v_rows):
    seq_len, head_dim = k_rows.shape[1:]
    shape = (2, 3, list_length(seq_len), head_dim)
    return pl.pallas_call(
        functools.partial(pack_kernel, seq_len=seq_len),
        out_shape=(jax.ShapeDtypeStruct(shape, k_rows.dtype), jax.ShapeDtypeStruct((1,), jnp.int32)),
        in_specs=[SMEM, HBM, HBM],
        out_specs=(HBM, SMEM),
        scratch_shapes=[pltpu.VMEM(shape, k_rows.dtype), pltpu.SemaphoreType.DMA((2, 3, CUTS)), pltpu.SemaphoreType.DMA((2, 3, CUTS)), pltpu.SemaphoreType.DMA((2, 3, 2 * CUTS))],
        compiler_params=pltpu.CompilerParams(vmem_limit_bytes=60 * 2**20),
        name='pack',
    )(lengths, k_rows, v_rows)


def project(res_ref, gain_ref, weights, proj_ref, normed, total, ring, ring_sem):
    depth, side, _ = ring.shape
    resid = res_ref[...].astype(jnp.float32)
    inv_rms = lax.rsqrt(jnp.sum(resid * resid, axis=-1, keepdims=True) / resid.shape[-1] + EPS)
    lanes = gain_ref.shape[1]
    for r in range(gain_ref.shape[0]):
        cols = slice(r * lanes, (r + 1) * lanes)
        row = (resid[:, cols] * inv_rms * gain_ref[r:r + 1, :].astype(jnp.float32)).astype(normed.dtype)
        normed[:, cols] = jnp.broadcast_to(row, (normed.shape[0], lanes))
    total[...] = jnp.zeros_like(total)
    deep = normed.shape[1] // side

    def at(i):
        return pl.multiple_of(i // deep * side, side), pl.multiple_of(i % deep * side, side)

    def fetch(i):
        left, top = at(i)
        first = 0
        for w_ref in weights:
            width = w_ref.shape[1]

            @pl.when((left >= first) & (left < first + width))
            def _(w_ref=w_ref, first=first):
                here = pl.multiple_of(left - first, side)
                pltpu.make_async_copy(w_ref.at[pl.ds(top, side), pl.ds(here, side)], ring.at[i % depth], ring_sem.at[i % depth]).start()
            first += width

    blocks = total.shape[1] // side * deep

    def prime(i, carry):
        fetch(i)
        return carry
    lax.fori_loop(0, depth - 1, prime, 0)

    def step(i, carry):
        @pl.when(i + depth - 1 < blocks)
        def _():
            fetch(i + depth - 1)
        pltpu.make_async_copy(weights[0].at[pl.ds(0, side), pl.ds(0, side)], ring.at[i % depth], ring_sem.at[i % depth]).wait()
        left, top = at(i)
        total[:, pl.ds(left, side)] += jnp.dot(normed[:, pl.ds(top, side)], ring[i % depth], preferred_element_type=jnp.float32)
        return carry
    lax.fori_loop(0, blocks, step, 0)
    proj_ref[...] = total[...].astype(proj_ref.dtype)


def remote(src, dst, send, recv, device):
    return pltpu.make_async_remote_copy(src_ref=src, dst_ref=dst, send_sem=send, recv_sem=recv, device_id={'sh': device}, device_id_type=pl.DeviceIdType.MESH)


def more_kernel(packed, land, send_sem, recv_sem, *, extra):
    me = lax.axis_index('sh')
    core = me % 2
    chip = me // 2
    peers = [chip + 1 - 2 * (chip % 2), (chip + 2) % 4, 3 - chip]
    rows = pl.ds(BASE, extra)

    def out(t, k):
        return remote(packed.at[t, k, rows], land.at[t, k, core, rows], send_sem.at[t, k], recv_sem.at[t, k, core], 2 * peers[k] + 1)

    def into(t, k, q):
        here = land.at[t, k, q, rows]
        return remote(here, here, send_sem.at[t, k], recv_sem.at[t, k, q], me)

    for t, k in ORDER:
        out(t, k).start()
    for t, k in ORDER:
        out(t, k).wait_send()

    @pl.when(core == 1)
    def _():
        for t, k in ORDER:
            for q in range(2):
                into(t, k, q).wait_recv()


def nothing_kernel(packed, land):
    pass


def more(packed, *, extra):
    shape = jax.ShapeDtypeStruct((2, 4, 2) + packed.shape[2:], packed.dtype)
    if not extra:
        return pl.pallas_call(nothing_kernel, out_shape=shape, in_specs=[HBM], out_specs=HBM, compiler_params=pltpu.CompilerParams(vmem_limit_bytes=60 * 2**20), name='more_0')(packed)
    dma = pltpu.SemaphoreType.DMA
    return pl.pallas_call(
        functools.partial(more_kernel, extra=extra),
        out_shape=shape,
        in_specs=[HBM],
        out_specs=HBM,
        scratch_shapes=[dma((2, 3)), dma((2, 3, 2))],
        compiler_params=pltpu.CompilerParams(has_side_effects=True, vmem_limit_bytes=60 * 2**20),
        name=f'more_{extra}',
    )(packed)


def base_kernel(packed, k_ref, v_ref, res_ref, gain_ref, wq_ref, wk_ref, wv_ref, wout_ref, _, land, proj_ref, *rest):
    held_refs, (normed, total, ring, ring_sem, held_sem, send_sem, recv_sem, fsend_sem, frecv_sem, ssend_sem, srecv_sem) = rest[:PARTS], rest[PARTS:]
    me = lax.axis_index('sh')
    core = me % 2
    chip = me // 2
    partner = me + 1 - 2 * core
    peers = [chip + 1 - 2 * (chip % 2), (chip + 2) % 4, 3 - chip]

    size = HALF // PIECES

    def main(t, k, half, p):
        rows = pl.ds(half * HALF + p * size, size)
        return remote(packed.at[t, k, rows], land.at[t, k, core, rows], send_sem.at[t, k, half, p], recv_sem.at[t, k, core, p], 2 * peers[k] + half)

    def forward(t, k, q, p):
        rows = land.at[t, k, q, pl.ds(core * HALF + p * size, size)]
        return remote(rows, rows, fsend_sem.at[t, k, q, p], frecv_sem.at[t, k, q, p], partner)

    def main_in(t, k, q, p):
        rows = land.at[t, k, q, pl.ds(core * HALF + p * size, size)]
        return remote(rows, rows, fsend_sem.at[t, k, q, p], recv_sem.at[t, k, q, p], partner)

    def forward_in(t, k, q, p):
        rows = land.at[t, k, q, pl.ds((1 - core) * HALF + p * size, size)]
        return remote(rows, rows, fsend_sem.at[t, k, q, p], frecv_sem.at[t, k, q, p], partner)

    def across(t):
        return remote((k_ref, v_ref)[t].at[partner], land.at[t, 3, core, pl.ds(0, k_ref.shape[1])], ssend_sem.at[t], srecv_sem.at[t], partner)

    def across_in(t):
        rows = land.at[t, 3, 1 - core, pl.ds(0, k_ref.shape[1])]
        return remote(rows, rows, ssend_sem.at[t], srecv_sem.at[t], partner)

    for t, k in ORDER:
        for half in range(2):
            for p in range(PIECES):
                main(t, k, half, p).start()
    for t in range(2):
        across(t).start()
    project(res_ref, gain_ref, (wq_ref, wk_ref, wv_ref), proj_ref, normed, total, ring, ring_sem)
    slabs, part, slab = held_refs[0].shape

    def hold(c, carry):
        for i in range(PARTS):
            pltpu.make_async_copy(wout_ref.at[pl.ds(i * part, part), pl.ds(pl.multiple_of(c * slab, slab), slab)], held_refs[i].at[c], held_sem.at[i]).start()
        return carry
    lax.fori_loop(0, slabs, hold, 0)
    for t, k in ORDER:
        for p in range(PIECES):
            for q in range(2):
                main_in(t, k, q, p).wait_recv()
                forward(t, k, q, p).start()
    for t in range(2):
        across(t).wait_send()
        across_in(t).wait_recv()
    for t, k in ORDER:
        for half in range(2):
            for p in range(PIECES):
                main(t, k, half, p).wait_send()
    for t, k in ORDER:
        for q in range(2):
            for p in range(PIECES):
                forward(t, k, q, p).wait_send()
                forward_in(t, k, q, p).wait_recv()
    for i in range(PARTS):
        pltpu.make_async_copy(held_refs[i], held_refs[i], held_sem.at[i]).wait()


def base(packed, k_rows, v_rows, residual, gain, w_query, w_key, w_value, w_out, land):
    dtype = k_rows.dtype
    dma = pltpu.SemaphoreType.DMA
    model_dim = residual.shape[1]
    proj_dim = w_query.shape[1] + w_key.shape[1] + w_value.shape[1]
    return pl.pallas_call(
        base_kernel,
        out_shape=(jax.ShapeDtypeStruct(land.shape, dtype), jax.ShapeDtypeStruct((LANES, proj_dim), dtype), )+ PARTS * (jax.ShapeDtypeStruct((w_out.shape[1] // SLAB, w_out.shape[0] // PARTS, SLAB), dtype),),
        in_specs=[HBM, HBM, HBM, VMEM, VMEM, HBM, HBM, HBM, HBM, HBM],
        out_specs=(HBM, VMEM) + PARTS * (ANY,),
        scratch_shapes=[
            pltpu.VMEM((LANES, model_dim), dtype), pltpu.VMEM((LANES, proj_dim), jnp.float32), pltpu.VMEM((8, 512, 512), dtype), dma((8,)), dma((PARTS,)),
            dma((2, 3, 2, PIECES)), dma((2, 3, 2, PIECES)), dma((2, 3, 2, PIECES)), dma((2, 3, 2, PIECES)), dma((2,)), dma((2,)),
        ],
        input_output_aliases={9: 0},
        compiler_params=pltpu.CompilerParams(has_side_effects=True, vmem_limit_bytes=BASE_VMEM),
        name='base',
    )(packed, k_rows, v_rows, residual, gain, w_query, w_key, w_value, w_out, land)


def build_kernel(len_ref, proj_ref, freq_ref, res_ref, *rest, depth):
    w_refs, (k_ref, v_ref, land, kc_ref, vc_ref, xout_ref, ring, tail, wide, made, scores, probs, mixed, ovec, q_ref, knew_ref, vnew_ref, ring_sem, tail_sem, made_sem) = rest[:PARTS], rest[PARTS:]
    step = pl.program_id(0)
    steps = WINDOW // STEP
    me = lax.axis_index('sh')
    core, chip, n = me % 2, me // 2, len_ref[me]
    offset = core * span(len_ref[2 * chip])
    chips = [chip, chip + 1 - 2 * (chip % 2), (chip + 2) % 4, 3 - chip]
    extra = tail.shape[2]
    heads = tail.shape[1]
    head_dim = tail.shape[3]

    def copies(t, start, size, dst, sem):
        own = 2 * chip + core
        other = 2 * chip + 1 - core
        rows = pl.ds(start, size)
        yield pltpu.make_async_copy((k_ref, v_ref)[t].at[me, rows], dst.at[own], sem)
        yield pltpu.make_async_copy(land.at[t, 3, 1 - core, rows], dst.at[other], sem)
        far = pl.ds(pl.multiple_of(offset + start, ALIGN), size)
        for k in range(3):
            for q in range(2):
                yield pltpu.make_async_copy(land.at[t, k, q, far], dst.at[2 * chips[k + 1] + q], sem)

    def heads_of_row():
        q_width = ovec.shape[1]
        group = q_width // (heads * head_dim)

        def part(at):
            return proj_ref[:1, at:at + head_dim]

        angles = n.astype(jnp.float32) * freq_ref[...]
        lane = lax.broadcasted_iota(jnp.int32, angles.shape, 1)
        cos, sin = jnp.cos(angles), jnp.sin(angles)
        sin = jnp.where(lane < head_dim // 2, -sin, sin)

        def turned(at):
            vals = part(at).astype(jnp.float32)
            return (vals * cos + pltpu.roll(vals, head_dim // 2, 1) * sin).astype(q_ref.dtype)

        for h in range(heads):
            q_ref[h] = jnp.concatenate([turned((h * group + g) * head_dim) for g in range(group)] + [jnp.zeros((q_ref.shape[1] - group, head_dim), q_ref.dtype)], axis=0)
        knew_ref[...] = jnp.concatenate([turned(q_width + h * head_dim) for h in range(heads)], axis=0)
        vnew_ref[...] = jnp.concatenate([part(q_width + (heads + h) * head_dim) for h in range(heads)], axis=0)

    def chunk(s, then):
        for t in range(2):
            local = s - t * steps
            pl.when((local >= 0) & (local < steps) & (local * STEP < n))(functools.partial(then, t, local))

    def fetch(s):
        def then(t, local):
            for copy in copies(t, pl.multiple_of(local * STEP, STEP), STEP, ring.at[s % depth], ring_sem.at[s % depth]):
                copy.start()
        chunk(s, then)

    def arrived(s):
        def then(t, local):
            whole = ring.at[s % depth]
            pltpu.make_async_copy(whole, whole, ring_sem.at[s % depth]).wait()
        chunk(s, then)

    def fetch_tail(t):
        @pl.when(n > WINDOW)
        def _():
            for copy in copies(t, WINDOW, extra, tail.at[t], tail_sem.at[t]):
                copy.start()

    def save(b, out_ref, local):
        size = BLOCK * heads // SAVES
        for i in range(SAVES):
            at = b * BLOCK * heads + i * size
            here = pl.ds(pl.multiple_of(at, size), size)
            there = pl.ds(pl.multiple_of(local * STEP * heads + at, size), size)
            pltpu.make_async_copy(made.at[step % MADE, here], out_ref.at[there], made_sem.at[step % MADE]).start()

    def saved(s):
        whole = made.at[s % MADE]
        pltpu.make_async_copy(whole, whole, made_sem.at[s % MADE]).wait()

    @pl.when(step == 0)
    def _():
        fetch_tail(0)
        for s in range(depth - 1):
            fetch(jnp.int32(s))
        fetch_tail(1)
        mixed[...] = jnp.zeros_like(mixed)
        heads_of_row()
    fetch(step + depth - 1)
    arrived(step)

    @pl.when(step >= MADE)
    def _():
        saved(step)

    def assemble(t, local, new_ref, out_ref, use):
        first = local * STEP
        newest = lax.rem(n, WINDOW)
        wraps = (local == 0) & (n > WINDOW)
        dead = first > n
        plain = (first + STEP <= n) & ~wraps & ((newest < first) | (newest >= first + STEP))
        slot = step % depth
        out = step % MADE

        @pl.when(wraps)
        def _():
            whole = tail.at[t]
            pltpu.make_async_copy(whole, whole, tail_sem.at[t]).wait()

        @pl.when(~plain & ~dead)
        def _():
            pos = first + lax.broadcasted_iota(jnp.int32, (STEP, head_dim), 0)
            for h in range(heads):
                vals = ring[slot, h]
                low = jnp.where(pos[:extra] < n - WINDOW, tail[t, h], vals[:extra])
                vals = jnp.concatenate([low, vals[extra:]], axis=0)
                vals = jnp.where(pos < n, vals, jnp.zeros_like(vals))
                ring[slot, h] = jnp.where(pos == newest, jnp.broadcast_to(new_ref[h:h + 1, :], vals.shape), vals)

        @pl.when(dead)
        def _():
            made[out] = jnp.zeros(made.shape[1:], made.dtype)
            for b in range(STEP // BLOCK):
                save(b, out_ref, local)
            use(None, None, None)

        @pl.when(~dead)
        def _():
            def mix(b, carry):
                for h in range(heads):
                    vals = ring[slot, h, pl.ds(pl.multiple_of(b * BLOCK, BLOCK), BLOCK), :]
                    wide[pl.ds(h, BLOCK, stride=PITCH), :] = vals.astype(jnp.float32)
                    use(h, b, vals)
                rows = jnp.concatenate([wide[PITCH * p:PITCH * p + heads, :] for p in range(BLOCK)], axis=0)
                made[out, pl.ds(pl.multiple_of(b * BLOCK * heads, BLOCK * heads), BLOCK * heads), :] = rows.astype(made.dtype)
                save(b, out_ref, local)
                return carry
            lax.fori_loop(0, STEP // BLOCK, mix, 0)

    def slots_of(local, b, size):
        return pl.ds(pl.multiple_of(local * STEP + b * BLOCK, BLOCK), size)

    @pl.when(step < steps)
    def _():
        def use(h, b, vals):
            if h is None:
                scores[:, slots_of(step, 0, STEP)] = jnp.full((scores.shape[0], STEP), -jnp.inf)
                return
            slots = step * STEP + b * BLOCK + lax.broadcasted_iota(jnp.int32, (8, BLOCK), 1)
            live = (slots <= n) | (n >= WINDOW)
            s = lax.dot_general(q_ref[h], vals, (((1,), (1,)), ((), ())), preferred_element_type=jnp.float32) / head_dim ** 0.5
            scores[pl.ds(8 * h, 8), slots_of(step, b, BLOCK)] = jnp.where(live, s, -jnp.inf)
        assemble(0, step, knew_ref, kc_ref, use)

    @pl.when(step == steps)
    def _():
        for h in range(heads):
            s = scores[8 * h:8 * h + 8, :]
            e = jnp.exp(s - jnp.max(s, axis=-1, keepdims=True))
            probs[h] = (e / jnp.sum(e, axis=-1, keepdims=True)).astype(probs.dtype)

    @pl.when(step >= steps)
    def _():
        local = step - steps

        def use(h, b, vals):
            if h is None:
                return
            p = probs[h, :, slots_of(local, b, BLOCK)]
            mixed[h] += jnp.dot(p, vals, preferred_element_type=jnp.float32)
        assemble(1, local, vnew_ref, vc_ref, use)

    @pl.when(step == 2 * steps - 1)
    def _():
        group = ovec.shape[1] // (heads * head_dim)
        for h in range(heads):
            o = mixed[h].astype(ovec.dtype)
            for g in range(group):
                cols = pl.ds((h * group + g) * head_dim, head_dim)
                ovec[:, cols] = jnp.broadcast_to(o[g:g + 1], (ovec.shape[0], head_dim))
        slabs, part, slab = w_refs[0].shape
        width = GROUP * slab

        def column(c, carry):
            acc = jnp.zeros((ovec.shape[0], width), jnp.float32)
            for i, w_ref in enumerate(w_refs):
                block = jnp.concatenate([w_ref[c * GROUP + j] for j in range(GROUP)], axis=1)
                acc += jnp.dot(ovec[:, i * part:(i + 1) * part], block, preferred_element_type=jnp.float32)
            cols = pl.ds(pl.multiple_of(c * width, width), width)
            xout_ref[:, cols] = (res_ref[:, cols].astype(jnp.float32) + acc[:1]).astype(xout_ref.dtype)
            return carry
        lax.fori_loop(0, slabs // GROUP, column, 0)
        for s in range(2 * steps - MADE, 2 * steps):
            saved(s)


def build(lengths, proj, freq, residual, w_out, k_rows, v_rows, land, heads):
    seq_len, head_dim = k_rows.shape[1:]
    steps = WINDOW // STEP
    depth = 6
    dtype = k_rows.dtype
    cache = jax.ShapeDtypeStruct((WINDOW * heads, head_dim), dtype)
    dma = pltpu.SemaphoreType.DMA
    return pl.pallas_call(
        functools.partial(build_kernel, depth=depth),
        grid=(2 * steps,),
        out_shape=(cache, cache, jax.ShapeDtypeStruct(residual.shape, dtype)),
        in_specs=[SMEM, VMEM, VMEM, VMEM] + PARTS * [VMEM] + [HBM, HBM, HBM],
        out_specs=(HBM, HBM, VMEM),
        scratch_shapes=[
            pltpu.VMEM((depth, heads, STEP, head_dim), dtype),
            pltpu.VMEM((2, heads, seq_len - WINDOW, head_dim), dtype),
            pltpu.VMEM((BLOCK * PITCH, head_dim), jnp.float32),
            pltpu.VMEM((MADE, STEP * heads, head_dim), dtype),
            pltpu.VMEM((8 * heads, WINDOW), jnp.float32),
            pltpu.VMEM((heads, 8, WINDOW), dtype),
            pltpu.VMEM((heads, 8, head_dim), jnp.float32),
            pltpu.VMEM((LANES, PARTS * w_out[0].shape[1]), dtype),
            pltpu.VMEM((heads, 8, head_dim), dtype),
            pltpu.VMEM((heads, head_dim), dtype),
            pltpu.VMEM((heads, head_dim), dtype),
            dma((depth,)), dma((2,)), dma((MADE,)),
        ],
        compiler_params=pltpu.CompilerParams(vmem_limit_bytes=BUILD_VMEM),
        name='build',
    )(lengths, proj, freq, residual, *w_out, k_rows, v_rows, land)


def frequencies(head_dim):
    half = THETA ** (-2.0 * np.arange(head_dim // 2, dtype=np.float64) / head_dim)
    return np.concatenate([half, half])[None].astype(np.float32)


def solution(mesh):
    head_spec = P('dp', None, 'sh', None)
    row_spec = P(('dp', 'sh'))
    full_spec = P(None, None)

    def per_device(k_prefill, v_prefill, lengths, residual, norm_gain, w_query, w_key, w_value, w_out):
        num_rows, seq_len, _, head_dim = k_prefill.shape
        kv_heads = w_key.shape[1] // head_dim
        k_rows = k_prefill.reshape(num_rows, seq_len, head_dim)
        v_rows = v_prefill.reshape(num_rows, seq_len, head_dim)
        packed, size = pack(lengths, k_rows, v_rows)
        sizes = (list_length(seq_len) - BASE) // QUANTUM
        land = lax.switch(size[0], [functools.partial(more, extra=i * QUANTUM) for i in range(sizes + 1)], packed)
        land, proj, *held = base(packed, k_rows, v_rows, residual, norm_gain.reshape(-1, head_dim), w_query, w_key, w_value, w_out, land)
        k_cache, v_cache, resid_out = build(lengths, proj, jnp.asarray(frequencies(head_dim)), residual, held, k_rows, v_rows, land, kv_heads)
        shape = (1, WINDOW, kv_heads, head_dim)
        return resid_out, k_cache.reshape(shape), v_cache.reshape(shape)
    return jax.shard_map(per_device, mesh=mesh, in_specs=(head_spec, head_spec, P('dp'), P(('dp', 'sh'), None), P(None), full_spec, full_spec, full_spec, full_spec), out_specs=(P(('dp', 'sh'), None), row_spec, row_spec), check_vma=False)
```

```python
import functools

import jax
import jax.numpy as jnp
import numpy as np
from jax import lax
from jax.experimental import pallas as pl
from jax.experimental.pallas import tpu as pltpu
from jax.sharding import PartitionSpec as P

WINDOW = 4096
THETA = 10000.0
EPS = 1e-5
ALIGN = 16
HALF = 2208
BASE = 2 * HALF
CUTS = 4
PIECES = 2
QUANTUM = 128
STEP = 1024
SLAB = 128
GROUP = 4
MADE = 2
SAVES = 2
BLOCK = 128
PITCH = 12
PARTS = 4
BASE_VMEM = 14 * 2**20
BUILD_VMEM = 18 * 2**20
LANES = 16
ORDER = [(t, k) for k in range(3) for t in range(2)]
ANY = pl.BlockSpec(memory_space=pl.ANY)
VMEM = pl.BlockSpec(memory_space=pltpu.VMEM)
SMEM = pl.BlockSpec(memory_space=pltpu.SMEM)
HBM = pl.BlockSpec(memory_space=pltpu.HBM)


def list_length(seq_len):
    return BASE + -(-(2 * seq_len - BASE) // QUANTUM) * QUANTUM


def span(length):
    return (length + (ALIGN - 1)) // ALIGN * ALIGN


def pack_kernel(len_ref, k_ref, v_ref, out_ref, size_ref, lists, first_sem, second_sem, store_sem, *, seq_len):
    chip = lax.axis_index('sh') // 2
    list_len = lists.shape[2]
    peers = [chip + 1 - 2 * (chip % 2), (chip + 2) % 4, 3 - chip]

    part = seq_len // CUTS

    def spans_of(k):
        return span(len_ref[2 * peers[k]]), span(len_ref[2 * peers[k] + 1])

    def loads(t, k, second):
        src = (k_ref, v_ref)[t]
        spans = spans_of(k)
        for i in range(CUTS):
            start = pl.multiple_of(second * spans[0] + i * part, ALIGN)
            yield spans[second] > i * part, pltpu.make_async_copy(src.at[2 * peers[k] + second, pl.ds(i * part, part)], lists.at[t, k, pl.ds(start, part)], (first_sem, second_sem)[second].at[t, k, i])

    def stores(t, k):
        size = list_len // (2 * CUTS)
        for i in range(2 * CUTS):
            rows = pl.ds(i * size, size)
            yield sum(spans_of(k)) > i * size, pltpu.make_async_copy(lists.at[t, k, rows], out_ref.at[t, k, rows], store_sem.at[t, k, i])

    def start(copies):
        for live, copy in copies:
            pl.when(live)(copy.start)

    def wait(copies):
        for live, copy in copies:
            pl.when(live)(copy.wait)

    for t, k in ORDER:
        start(loads(t, k, 0))
    longest = span(len_ref[0]) + span(len_ref[1])
    for c in range(1, len_ref.shape[0] // 2):
        longest = jnp.maximum(longest, span(len_ref[2 * c]) + span(len_ref[2 * c + 1]))
    size_ref[0] = jnp.clip((longest - BASE + QUANTUM - 1) // QUANTUM, 0, (list_len - BASE) // QUANTUM)
    for t, k in ORDER:
        wait(loads(t, k, 0))
        start(loads(t, k, 1))
    for t, k in ORDER:
        wait(loads(t, k, 1))
        start(stores(t, k))
    for t, k in ORDER:
        wait(stores(t, k))


def pack(lengths, k_rows, v_rows):
    seq_len, head_dim = k_rows.shape[1:]
    shape = (2, 3, list_length(seq_len), head_dim)
    return pl.pallas_call(
        functools.partial(pack_kernel, seq_len=seq_len),
        out_shape=(jax.ShapeDtypeStruct(shape, k_rows.dtype), jax.ShapeDtypeStruct((1,), jnp.int32)),
        in_specs=[SMEM, HBM, HBM],
        out_specs=(HBM, SMEM),
        scratch_shapes=[pltpu.VMEM(shape, k_rows.dtype), pltpu.SemaphoreType.DMA((2, 3, CUTS)), pltpu.SemaphoreType.DMA((2, 3, CUTS)), pltpu.SemaphoreType.DMA((2, 3, 2 * CUTS))],
        compiler_params=pltpu.CompilerParams(vmem_limit_bytes=60 * 2**20),
        name='pack',
    )(lengths, k_rows, v_rows)


def project(res_ref, gain_ref, weights, proj_ref, normed, total, ring, ring_sem):
    depth, side, _ = ring.shape
    resid = res_ref[...].astype(jnp.float32)
    inv_rms = lax.rsqrt(jnp.sum(resid * resid, axis=-1, keepdims=True) / resid.shape[-1] + EPS)
    lanes = gain_ref.shape[1]
    for r in range(gain_ref.shape[0]):
        cols = slice(r * lanes, (r + 1) * lanes)
        row = (resid[:, cols] * inv_rms * gain_ref[r:r + 1, :].astype(jnp.float32)).astype(normed.dtype)
        normed[:, cols] = jnp.broadcast_to(row, (normed.shape[0], lanes))
    total[...] = jnp.zeros_like(total)
    deep = normed.shape[1] // side

    def at(i):
        return pl.multiple_of(i // deep * side, side), pl.multiple_of(i % deep * side, side)

    def fetch(i):
        left, top = at(i)
        first = 0
        for w_ref in weights:
            width = w_ref.shape[1]

            @pl.when((left >= first) & (left < first + width))
            def _(w_ref=w_ref, first=first):
                here = pl.multiple_of(left - first, side)
                pltpu.make_async_copy(w_ref.at[pl.ds(top, side), pl.ds(here, side)], ring.at[i % depth], ring_sem.at[i % depth]).start()
            first += width

    blocks = total.shape[1] // side * deep

    def prime(i, carry):
        fetch(i)
        return carry
    lax.fori_loop(0, depth - 1, prime, 0)

    def step(i, carry):
        @pl.when(i + depth - 1 < blocks)
        def _():
            fetch(i + depth - 1)
        pltpu.make_async_copy(weights[0].at[pl.ds(0, side), pl.ds(0, side)], ring.at[i % depth], ring_sem.at[i % depth]).wait()
        left, top = at(i)
        total[:, pl.ds(left, side)] += jnp.dot(normed[:, pl.ds(top, side)], ring[i % depth], preferred_element_type=jnp.float32)
        return carry
    lax.fori_loop(0, blocks, step, 0)
    proj_ref[...] = total[...].astype(proj_ref.dtype)


def remote(src, dst, send, recv, device):
    return pltpu.make_async_remote_copy(src_ref=src, dst_ref=dst, send_sem=send, recv_sem=recv, device_id={'sh': device}, device_id_type=pl.DeviceIdType.MESH)


def more_kernel(packed, land, send_sem, recv_sem, *, extra):
    me = lax.axis_index('sh')
    core = me % 2
    chip = me // 2
    peers = [chip + 1 - 2 * (chip % 2), (chip + 2) % 4, 3 - chip]
    rows = pl.ds(BASE, extra)

    def out(t, k):
        return remote(packed.at[t, k, rows], land.at[t, k, core, rows], send_sem.at[t, k], recv_sem.at[t, k, core], 2 * peers[k] + 1)

    def into(t, k, q):
        here = land.at[t, k, q, rows]
        return remote(here, here, send_sem.at[t, k], recv_sem.at[t, k, q], me)

    for t, k in ORDER:
        out(t, k).start()
    for t, k in ORDER:
        out(t, k).wait_send()

    @pl.when(core == 1)
    def _():
        for t, k in ORDER:
            for q in range(2):
                into(t, k, q).wait_recv()


def nothing_kernel(packed, land):
    pass


def more(packed, *, extra):
    shape = jax.ShapeDtypeStruct((2, 4, 2) + packed.shape[2:], packed.dtype)
    if not extra:
        return pl.pallas_call(nothing_kernel, out_shape=shape, in_specs=[HBM], out_specs=HBM, compiler_params=pltpu.CompilerParams(vmem_limit_bytes=60 * 2**20), name='more_0')(packed)
    dma = pltpu.SemaphoreType.DMA
    return pl.pallas_call(
        functools.partial(more_kernel, extra=extra),
        out_shape=shape,
        in_specs=[HBM],
        out_specs=HBM,
        scratch_shapes=[dma((2, 3)), dma((2, 3, 2))],
        compiler_params=pltpu.CompilerParams(has_side_effects=True, vmem_limit_bytes=60 * 2**20),
        name=f'more_{extra}',
    )(packed)


def base_kernel(packed, k_ref, v_ref, res_ref, gain_ref, wq_ref, wk_ref, wv_ref, wout_ref, _, land, proj_ref, *rest):
    held_refs, (normed, total, ring, ring_sem, held_sem, send_sem, recv_sem, fsend_sem, frecv_sem, ssend_sem, srecv_sem) = rest[:PARTS], rest[PARTS:]
    me = lax.axis_index('sh')
    core = me % 2
    chip = me // 2
    partner = me + 1 - 2 * core
    peers = [chip + 1 - 2 * (chip % 2), (chip + 2) % 4, 3 - chip]

    size = HALF // PIECES

    def main(t, k, half, p):
        rows = pl.ds(half * HALF + p * size, size)
        return remote(packed.at[t, k, rows], land.at[t, k, core, rows], send_sem.at[t, k, half, p], recv_sem.at[t, k, core, p], 2 * peers[k] + half)

    def forward(t, k, q, p):
        rows = land.at[t, k, q, pl.ds(core * HALF + p * size, size)]
        return remote(rows, rows, fsend_sem.at[t, k, q, p], frecv_sem.at[t, k, q, p], partner)

    def main_in(t, k, q, p):
        rows = land.at[t, k, q, pl.ds(core * HALF + p * size, size)]
        return remote(rows, rows, fsend_sem.at[t, k, q, p], recv_sem.at[t, k, q, p], partner)

    def forward_in(t, k, q, p):
        rows = land.at[t, k, q, pl.ds((1 - core) * HALF + p * size, size)]
        return remote(rows, rows, fsend_sem.at[t, k, q, p], frecv_sem.at[t, k, q, p], partner)

    def across(t):
        return remote((k_ref, v_ref)[t].at[partner], land.at[t, 3, core, pl.ds(0, k_ref.shape[1])], ssend_sem.at[t], srecv_sem.at[t], partner)

    def across_in(t):
        rows = land.at[t, 3, 1 - core, pl.ds(0, k_ref.shape[1])]
        return remote(rows, rows, ssend_sem.at[t], srecv_sem.at[t], partner)

    for t, k in ORDER:
        for half in range(2):
            for p in range(PIECES):
                main(t, k, half, p).start()
    for t in range(2):
        across(t).start()
    project(res_ref, gain_ref, (wq_ref, wk_ref, wv_ref), proj_ref, normed, total, ring, ring_sem)
    slabs, part, slab = held_refs[0].shape

    def hold(c, carry):
        for i in range(PARTS):
            pltpu.make_async_copy(wout_ref.at[pl.ds(i * part, part), pl.ds(pl.multiple_of(c * slab, slab), slab)], held_refs[i].at[c], held_sem.at[i]).start()
        return carry
    lax.fori_loop(0, slabs, hold, 0)
    for t, k in ORDER:
        for p in range(PIECES):
            for q in range(2):
                main_in(t, k, q, p).wait_recv()
                forward(t, k, q, p).start()
    for t in range(2):
        across(t).wait_send()
        across_in(t).wait_recv()
    for t, k in ORDER:
        for half in range(2):
            for p in range(PIECES):
                main(t, k, half, p).wait_send()
    for t, k in ORDER:
        for q in range(2):
            for p in range(PIECES):
                forward(t, k, q, p).wait_send()
                forward_in(t, k, q, p).wait_recv()
    for i in range(PARTS):
        pltpu.make_async_copy(held_refs[i], held_refs[i], held_sem.at[i]).wait()


def base(packed, k_rows, v_rows, residual, gain, w_query, w_key, w_value, w_out, land):
    dtype = k_rows.dtype
    dma = pltpu.SemaphoreType.DMA
    model_dim = residual.shape[1]
    proj_dim = w_query.shape[1] + w_key.shape[1] + w_value.shape[1]
    return pl.pallas_call(
        base_kernel,
        out_shape=(jax.ShapeDtypeStruct(land.shape, dtype), jax.ShapeDtypeStruct((LANES, proj_dim), dtype), )+ PARTS * (jax.ShapeDtypeStruct((w_out.shape[1] // SLAB, w_out.shape[0] // PARTS, SLAB), dtype),),
        in_specs=[HBM, HBM, HBM, VMEM, VMEM, HBM, HBM, HBM, HBM, HBM],
        out_specs=(HBM, VMEM) + PARTS * (ANY,),
        scratch_shapes=[
            pltpu.VMEM((LANES, model_dim), dtype), pltpu.VMEM((LANES, proj_dim), jnp.float32), pltpu.VMEM((8, 512, 512), dtype), dma((8,)), dma((PARTS,)),
            dma((2, 3, 2, PIECES)), dma((2, 3, 2, PIECES)), dma((2, 3, 2, PIECES)), dma((2, 3, 2, PIECES)), dma((2,)), dma((2,)),
        ],
        input_output_aliases={9: 0},
        compiler_params=pltpu.CompilerParams(has_side_effects=True, vmem_limit_bytes=BASE_VMEM),
        name='base',
    )(packed, k_rows, v_rows, residual, gain, w_query, w_key, w_value, w_out, land)


def build_kernel(len_ref, proj_ref, freq_ref, res_ref, *rest, depth):
    w_refs, (k_ref, v_ref, land, kc_ref, vc_ref, xout_ref, ring, tail, wide, made, scores, probs, mixed, ovec, q_ref, knew_ref, vnew_ref, ring_sem, tail_sem, made_sem) = rest[:PARTS], rest[PARTS:]
    step = pl.program_id(0)
    steps = WINDOW // STEP
    me = lax.axis_index('sh')
    core, chip, n = me % 2, me // 2, len_ref[me]
    offset = core * span(len_ref[2 * chip])
    chips = [chip, chip + 1 - 2 * (chip % 2), (chip + 2) % 4, 3 - chip]
    extra = tail.shape[2]
    heads = tail.shape[1]
    head_dim = tail.shape[3]

    def copies(t, start, size, dst, sem):
        own = 2 * chip + core
        other = 2 * chip + 1 - core
        rows = pl.ds(start, size)
        yield pltpu.make_async_copy((k_ref, v_ref)[t].at[me, rows], dst.at[own], sem)
        yield pltpu.make_async_copy(land.at[t, 3, 1 - core, rows], dst.at[other], sem)
        far = pl.ds(pl.multiple_of(offset + start, ALIGN), size)
        for k in range(3):
            for q in range(2):
                yield pltpu.make_async_copy(land.at[t, k, q, far], dst.at[2 * chips[k + 1] + q], sem)

    def heads_of_row():
        q_width = ovec.shape[1]
        group = q_width // (heads * head_dim)

        def part(at):
            return proj_ref[:1, at:at + head_dim]

        angles = n.astype(jnp.float32) * freq_ref[...]
        lane = lax.broadcasted_iota(jnp.int32, angles.shape, 1)
        cos, sin = jnp.cos(angles), jnp.sin(angles)
        sin = jnp.where(lane < head_dim // 2, -sin, sin)

        def turned(at):
            vals = part(at).astype(jnp.float32)
            return (vals * cos + pltpu.roll(vals, head_dim // 2, 1) * sin).astype(q_ref.dtype)

        for h in range(heads):
            q_ref[h] = jnp.concatenate([turned((h * group + g) * head_dim) for g in range(group)] + [jnp.zeros((q_ref.shape[1] - group, head_dim), q_ref.dtype)], axis=0)
        knew_ref[...] = jnp.concatenate([turned(q_width + h * head_dim) for h in range(heads)], axis=0)
        vnew_ref[...] = jnp.concatenate([part(q_width + (heads + h) * head_dim) for h in range(heads)], axis=0)

    def chunk(s, then):
        for t in range(2):
            local = s - t * steps
            pl.when((local >= 0) & (local < steps) & (local * STEP < n))(functools.partial(then, t, local))

    def fetch(s):
        def then(t, local):
            for copy in copies(t, pl.multiple_of(local * STEP, STEP), STEP, ring.at[s % depth], ring_sem.at[s % depth]):
                copy.start()
        chunk(s, then)

    def arrived(s):
        def then(t, local):
            whole = ring.at[s % depth]
            pltpu.make_async_copy(whole, whole, ring_sem.at[s % depth]).wait()
        chunk(s, then)

    def fetch_tail(t):
        @pl.when(n > WINDOW)
        def _():
            for copy in copies(t, WINDOW, extra, tail.at[t], tail_sem.at[t]):
                copy.start()

    def save(b, out_ref, local):
        size = BLOCK * heads // SAVES
        for i in range(SAVES):
            at = b * BLOCK * heads + i * size
            here = pl.ds(pl.multiple_of(at, size), size)
            there = pl.ds(pl.multiple_of(local * STEP * heads + at, size), size)
            pltpu.make_async_copy(made.at[step % MADE, here], out_ref.at[there], made_sem.at[step % MADE]).start(priority=1)

    def saved(s):
        whole = made.at[s % MADE]
        pltpu.make_async_copy(whole, whole, made_sem.at[s % MADE]).wait()

    @pl.when(step == 0)
    def _():
        fetch_tail(0)
        for s in range(depth - 1):
            fetch(jnp.int32(s))
        fetch_tail(1)
        mixed[...] = jnp.zeros_like(mixed)
        heads_of_row()
    fetch(step + depth - 1)
    arrived(step)

    @pl.when(step >= MADE)
    def _():
        saved(step)

    def assemble(t, local, new_ref, out_ref, use):
        first = local * STEP
        newest = lax.rem(n, WINDOW)
        wraps = (local == 0) & (n > WINDOW)
        dead = first > n
        plain = (first + STEP <= n) & ~wraps & ((newest < first) | (newest >= first + STEP))
        slot = step % depth
        out = step % MADE

        @pl.when(wraps)
        def _():
            whole = tail.at[t]
            pltpu.make_async_copy(whole, whole, tail_sem.at[t]).wait()

        @pl.when(~plain & ~dead)
        def _():
            def patch(c, carry):
                rows = pl.ds(pl.multiple_of(c * extra, extra), extra)
                pos = first + c * extra + lax.broadcasted_iota(jnp.int32, (extra, head_dim), 0)
                for h in range(heads):
                    vals = jnp.where(pos < n - WINDOW, tail[t, h], ring[slot, h, rows, :])
                    vals = jnp.where(pos < n, vals, jnp.zeros_like(vals))
                    ring[slot, h, rows, :] = jnp.where(pos == newest, jnp.broadcast_to(new_ref[h:h + 1, :], vals.shape), vals)
                return carry
            lax.fori_loop(0, STEP // extra, patch, 0)

        @pl.when(dead)
        def _():
            def clear(b, carry):
                made[out, pl.ds(pl.multiple_of(b * BLOCK * heads, BLOCK * heads), BLOCK * heads), :] = jnp.zeros((BLOCK * heads, head_dim), made.dtype)
                save(b, out_ref, local)
                return carry
            lax.fori_loop(0, STEP // BLOCK, clear, 0)
            use(None, None, None)

        @pl.when(~dead)
        def _():
            def mix(b, carry):
                for h in range(heads):
                    vals = ring[slot, h, pl.ds(pl.multiple_of(b * BLOCK, BLOCK), BLOCK), :]
                    wide[pl.ds(h, BLOCK, stride=PITCH), :] = vals.astype(jnp.float32)
                    use(h, b, vals)
                rows = jnp.concatenate([wide[PITCH * p:PITCH * p + heads, :] for p in range(BLOCK)], axis=0)
                made[out, pl.ds(pl.multiple_of(b * BLOCK * heads, BLOCK * heads), BLOCK * heads), :] = rows.astype(made.dtype)
                save(b, out_ref, local)
                return carry
            lax.fori_loop(0, STEP // BLOCK, mix, 0)

    def slots_of(local, b, size):
        return pl.ds(pl.multiple_of(local * STEP + b * BLOCK, BLOCK), size)

    @pl.when(step < steps)
    def _():
        def use(h, b, vals):
            if h is None:
                scores[:, slots_of(step, 0, STEP)] = jnp.full((scores.shape[0], STEP), -jnp.inf)
                return
            slots = step * STEP + b * BLOCK + lax.broadcasted_iota(jnp.int32, (8, BLOCK), 1)
            live = (slots <= n) | (n >= WINDOW)
            s = lax.dot_general(q_ref[h], vals, (((1,), (1,)), ((), ())), preferred_element_type=jnp.float32) / head_dim ** 0.5
            scores[pl.ds(8 * h, 8), slots_of(step, b, BLOCK)] = jnp.where(live, s, -jnp.inf)
        assemble(0, step, knew_ref, kc_ref, use)

    @pl.when(step == steps)
    def _():
        for h in range(heads):
            s = scores[8 * h:8 * h + 8, :]
            e = jnp.exp(s - jnp.max(s, axis=-1, keepdims=True))
            probs[h] = (e / jnp.sum(e, axis=-1, keepdims=True)).astype(probs.dtype)

    @pl.when(step >= steps)
    def _():
        local = step - steps

        def use(h, b, vals):
            if h is None:
                return
            p = probs[h, :, slots_of(local, b, BLOCK)]
            mixed[h] += jnp.dot(p, vals, preferred_element_type=jnp.float32)
        assemble(1, local, vnew_ref, vc_ref, use)

    @pl.when(step == 2 * steps - 1)
    def _():
        group = ovec.shape[1] // (heads * head_dim)
        for h in range(heads):
            o = mixed[h].astype(ovec.dtype)
            for g in range(group):
                cols = pl.ds((h * group + g) * head_dim, head_dim)
                ovec[:, cols] = jnp.broadcast_to(o[g:g + 1], (ovec.shape[0], head_dim))
        slabs, part, slab = w_refs[0].shape
        width = GROUP * slab

        def column(c, carry):
            acc = jnp.zeros((ovec.shape[0], width), jnp.float32)
            for i, w_ref in enumerate(w_refs):
                block = jnp.concatenate([w_ref[c * GROUP + j] for j in range(GROUP)], axis=1)
                acc += jnp.dot(ovec[:, i * part:(i + 1) * part], block, preferred_element_type=jnp.float32)
            cols = pl.ds(pl.multiple_of(c * width, width), width)
            xout_ref[:, cols] = (res_ref[:, cols].astype(jnp.float32) + acc[:1]).astype(xout_ref.dtype)
            return carry
        lax.fori_loop(0, slabs // GROUP, column, 0)
        for s in range(2 * steps - MADE, 2 * steps):
            saved(s)


def build(lengths, proj, freq, residual, w_out, k_rows, v_rows, land, heads):
    seq_len, head_dim = k_rows.shape[1:]
    steps = WINDOW // STEP
    depth = 3
    dtype = k_rows.dtype
    cache = jax.ShapeDtypeStruct((WINDOW * heads, head_dim), dtype)
    dma = pltpu.SemaphoreType.DMA
    return pl.pallas_call(
        functools.partial(build_kernel, depth=depth),
        grid=(2 * steps,),
        out_shape=(cache, cache, jax.ShapeDtypeStruct(residual.shape, dtype)),
        in_specs=[SMEM, VMEM, VMEM, VMEM] + PARTS * [VMEM] + [HBM, HBM, HBM],
        out_specs=(HBM, HBM, VMEM),
        scratch_shapes=[
            pltpu.VMEM((depth, heads, STEP, head_dim), dtype),
            pltpu.VMEM((2, heads, seq_len - WINDOW, head_dim), dtype),
            pltpu.VMEM((BLOCK * PITCH, head_dim), jnp.float32),
            pltpu.VMEM((MADE, STEP * heads, head_dim), dtype),
            pltpu.VMEM((8 * heads, WINDOW), jnp.float32),
            pltpu.VMEM((heads, 8, WINDOW), dtype),
            pltpu.VMEM((heads, 8, head_dim), jnp.float32),
            pltpu.VMEM((LANES, PARTS * w_out[0].shape[1]), dtype),
            pltpu.VMEM((heads, 8, head_dim), dtype),
            pltpu.VMEM((heads, head_dim), dtype),
            pltpu.VMEM((heads, head_dim), dtype),
            dma((depth,)), dma((2,)), dma((MADE,)),
        ],
        compiler_params=pltpu.CompilerParams(vmem_limit_bytes=BUILD_VMEM),
        name='build',
    )(lengths, proj, freq, residual, *w_out, k_rows, v_rows, land)


def frequencies(head_dim):
    half = THETA ** (-2.0 * np.arange(head_dim // 2, dtype=np.float64) / head_dim)
    return np.concatenate([half, half])[None].astype(np.float32)


def solution(mesh):
    head_spec = P('dp', None, 'sh', None)
    row_spec = P(('dp', 'sh'))
    full_spec = P(None, None)

    def per_device(k_prefill, v_prefill, lengths, residual, norm_gain, w_query, w_key, w_value, w_out):
        num_rows, seq_len, _, head_dim = k_prefill.shape
        kv_heads = w_key.shape[1] // head_dim
        k_rows = k_prefill.reshape(num_rows, seq_len, head_dim)
        v_rows = v_prefill.reshape(num_rows, seq_len, head_dim)
        packed, size = pack(lengths, k_rows, v_rows)
        sizes = (list_length(seq_len) - BASE) // QUANTUM
        land = lax.switch(size[0], [functools.partial(more, extra=i * QUANTUM) for i in range(sizes + 1)], packed)
        land, proj, *held = base(packed, k_rows, v_rows, residual, norm_gain.reshape(-1, head_dim), w_query, w_key, w_value, w_out, land)
        k_cache, v_cache, resid_out = build(lengths, proj, jnp.asarray(frequencies(head_dim)), residual, held, k_rows, v_rows, land, kv_heads)
        shape = (1, WINDOW, kv_heads, head_dim)
        return resid_out, k_cache.reshape(shape), v_cache.reshape(shape)
    return jax.shard_map(per_device, mesh=mesh, in_specs=(head_spec, head_spec, P('dp'), P(('dp', 'sh'), None), P(None), full_spec, full_spec, full_spec, full_spec), out_specs=(P(('dp', 'sh'), None), row_spec, row_spec), check_vma=False)
```

```python
import functools

import jax
import jax.numpy as jnp
import numpy as np
from jax import lax
from jax.experimental import pallas as pl
from jax.experimental.pallas import tpu as pltpu
from jax.sharding import PartitionSpec as P

WINDOW = 4096
THETA = 10000.0
EPS = 1e-5
ALIGN = 16
HALF = 2208
BASE = 2 * HALF
CUTS = 4
PIECES = 2
QUANTUM = 128
STEP = 512
SLAB = 128
GROUP = 4
MADE = 4
SAVES = 2
BLOCK = 128
PITCH = 9
PARTS = 4
BASE_VMEM = 14 * 2**20
BUILD_VMEM = 18 * 2**20
LANES = 16
ORDER = [(t, k) for k in range(3) for t in range(2)]
ANY = pl.BlockSpec(memory_space=pl.ANY)
VMEM = pl.BlockSpec(memory_space=pltpu.VMEM)
SMEM = pl.BlockSpec(memory_space=pltpu.SMEM)
HBM = pl.BlockSpec(memory_space=pltpu.HBM)


def list_length(seq_len):
    return BASE + -(-(2 * seq_len - BASE) // QUANTUM) * QUANTUM


def span(length):
    return (length + (ALIGN - 1)) // ALIGN * ALIGN


def pack_kernel(len_ref, k_ref, v_ref, out_ref, size_ref, lists, first_sem, second_sem, store_sem, *, seq_len):
    chip = lax.axis_index('sh') // 2
    list_len = lists.shape[2]
    peers = [chip + 1 - 2 * (chip % 2), (chip + 2) % 4, 3 - chip]

    part = seq_len // CUTS

    def spans_of(k):
        return span(len_ref[2 * peers[k]]), span(len_ref[2 * peers[k] + 1])

    def loads(t, k, second):
        src = (k_ref, v_ref)[t]
        spans = spans_of(k)
        for i in range(CUTS):
            start = pl.multiple_of(second * spans[0] + i * part, ALIGN)
            yield spans[second] > i * part, pltpu.make_async_copy(src.at[2 * peers[k] + second, pl.ds(i * part, part)], lists.at[t, k, pl.ds(start, part)], (first_sem, second_sem)[second].at[t, k, i])

    def stores(t, k):
        size = list_len // (2 * CUTS)
        for i in range(2 * CUTS):
            rows = pl.ds(i * size, size)
            yield sum(spans_of(k)) > i * size, pltpu.make_async_copy(lists.at[t, k, rows], out_ref.at[t, k, rows], store_sem.at[t, k, i])

    def start(copies):
        for live, copy in copies:
            pl.when(live)(copy.start)

    def wait(copies):
        for live, copy in copies:
            pl.when(live)(copy.wait)

    for t, k in ORDER:
        start(loads(t, k, 0))
    longest = span(len_ref[0]) + span(len_ref[1])
    for c in range(1, len_ref.shape[0] // 2):
        longest = jnp.maximum(longest, span(len_ref[2 * c]) + span(len_ref[2 * c + 1]))
    size_ref[0] = jnp.clip((longest - BASE + QUANTUM - 1) // QUANTUM, 0, (list_len - BASE) // QUANTUM)
    for t, k in ORDER:
        wait(loads(t, k, 0))
        start(loads(t, k, 1))
    for t, k in ORDER:
        wait(loads(t, k, 1))
        start(stores(t, k))
    for t, k in ORDER:
        wait(stores(t, k))


def pack(lengths, k_rows, v_rows):
    seq_len, head_dim = k_rows.shape[1:]
    shape = (2, 3, list_length(seq_len), head_dim)
    return pl.pallas_call(
        functools.partial(pack_kernel, seq_len=seq_len),
        out_shape=(jax.ShapeDtypeStruct(shape, k_rows.dtype), jax.ShapeDtypeStruct((1,), jnp.int32)),
        in_specs=[SMEM, HBM, HBM],
        out_specs=(HBM, SMEM),
        scratch_shapes=[pltpu.VMEM(shape, k_rows.dtype), pltpu.SemaphoreType.DMA((2, 3, CUTS)), pltpu.SemaphoreType.DMA((2, 3, CUTS)), pltpu.SemaphoreType.DMA((2, 3, 2 * CUTS))],
        compiler_params=pltpu.CompilerParams(vmem_limit_bytes=60 * 2**20),
        name='pack',
    )(lengths, k_rows, v_rows)


def project(res_ref, gain_ref, weights, proj_ref, normed, total, ring, ring_sem):
    depth, side, _ = ring.shape
    resid = res_ref[...].astype(jnp.float32)
    inv_rms = lax.rsqrt(jnp.sum(resid * resid, axis=-1, keepdims=True) / resid.shape[-1] + EPS)
    lanes = gain_ref.shape[1]
    for r in range(gain_ref.shape[0]):
        cols = slice(r * lanes, (r + 1) * lanes)
        row = (resid[:, cols] * inv_rms * gain_ref[r:r + 1, :].astype(jnp.float32)).astype(normed.dtype)
        normed[:, cols] = jnp.broadcast_to(row, (normed.shape[0], lanes))
    total[...] = jnp.zeros_like(total)
    deep = normed.shape[1] // side

    def at(i):
        return pl.multiple_of(i // deep * side, side), pl.multiple_of(i % deep * side, side)

    def fetch(i):
        left, top = at(i)
        first = 0
        for w_ref in weights:
            width = w_ref.shape[1]

            @pl.when((left >= first) & (left < first + width))
            def _(w_ref=w_ref, first=first):
                here = pl.multiple_of(left - first, side)
                pltpu.make_async_copy(w_ref.at[pl.ds(top, side), pl.ds(here, side)], ring.at[i % depth], ring_sem.at[i % depth]).start()
            first += width

    blocks = total.shape[1] // side * deep

    def prime(i, carry):
        fetch(i)
        return carry
    lax.fori_loop(0, depth - 1, prime, 0)

    def step(i, carry):
        @pl.when(i + depth - 1 < blocks)
        def _():
            fetch(i + depth - 1)
        pltpu.make_async_copy(weights[0].at[pl.ds(0, side), pl.ds(0, side)], ring.at[i % depth], ring_sem.at[i % depth]).wait()
        left, top = at(i)
        total[:, pl.ds(left, side)] += jnp.dot(normed[:, pl.ds(top, side)], ring[i % depth], preferred_element_type=jnp.float32)
        return carry
    lax.fori_loop(0, blocks, step, 0)
    proj_ref[...] = total[...].astype(proj_ref.dtype)


def remote(src, dst, send, recv, device):
    return pltpu.make_async_remote_copy(src_ref=src, dst_ref=dst, send_sem=send, recv_sem=recv, device_id={'sh': device}, device_id_type=pl.DeviceIdType.MESH)


def more_kernel(packed, land, send_sem, recv_sem, *, extra):
    me = lax.axis_index('sh')
    core = me % 2
    chip = me // 2
    peers = [chip + 1 - 2 * (chip % 2), (chip + 2) % 4, 3 - chip]
    rows = pl.ds(BASE, extra)

    def out(t, k):
        return remote(packed.at[t, k, rows], land.at[t, k, core, rows], send_sem.at[t, k], recv_sem.at[t, k, core], 2 * peers[k] + 1)

    def into(t, k, q):
        here = land.at[t, k, q, rows]
        return remote(here, here, send_sem.at[t, k], recv_sem.at[t, k, q], me)

    for t, k in ORDER:
        out(t, k).start()
    for t, k in ORDER:
        out(t, k).wait_send()

    @pl.when(core == 1)
    def _():
        for t, k in ORDER:
            for q in range(2):
                into(t, k, q).wait_recv()


def nothing_kernel(packed, land):
    pass


def more(packed, *, extra):
    shape = jax.ShapeDtypeStruct((2, 4, 2) + packed.shape[2:], packed.dtype)
    if not extra:
        return pl.pallas_call(nothing_kernel, out_shape=shape, in_specs=[HBM], out_specs=HBM, compiler_params=pltpu.CompilerParams(vmem_limit_bytes=60 * 2**20), name='more_0')(packed)
    dma = pltpu.SemaphoreType.DMA
    return pl.pallas_call(
        functools.partial(more_kernel, extra=extra),
        out_shape=shape,
        in_specs=[HBM],
        out_specs=HBM,
        scratch_shapes=[dma((2, 3)), dma((2, 3, 2))],
        compiler_params=pltpu.CompilerParams(has_side_effects=True, vmem_limit_bytes=60 * 2**20),
        name=f'more_{extra}',
    )(packed)


def base_kernel(packed, k_ref, v_ref, res_ref, gain_ref, wq_ref, wk_ref, wv_ref, wout_ref, _, land, proj_ref, *rest):
    held_refs, (normed, total, ring, ring_sem, held_sem, send_sem, recv_sem, fsend_sem, frecv_sem, ssend_sem, srecv_sem) = rest[:PARTS], rest[PARTS:]
    me = lax.axis_index('sh')
    core = me % 2
    chip = me // 2
    partner = me + 1 - 2 * core
    peers = [chip + 1 - 2 * (chip % 2), (chip + 2) % 4, 3 - chip]

    size = HALF // PIECES

    def main(t, k, half, p):
        rows = pl.ds(half * HALF + p * size, size)
        return remote(packed.at[t, k, rows], land.at[t, k, core, rows], send_sem.at[t, k, half, p], recv_sem.at[t, k, core, p], 2 * peers[k] + half)

    def forward(t, k, q, p):
        rows = land.at[t, k, q, pl.ds(core * HALF + p * size, size)]
        return remote(rows, rows, fsend_sem.at[t, k, q, p], frecv_sem.at[t, k, q, p], partner)

    def main_in(t, k, q, p):
        rows = land.at[t, k, q, pl.ds(core * HALF + p * size, size)]
        return remote(rows, rows, fsend_sem.at[t, k, q, p], recv_sem.at[t, k, q, p], partner)

    def forward_in(t, k, q, p):
        rows = land.at[t, k, q, pl.ds((1 - core) * HALF + p * size, size)]
        return remote(rows, rows, fsend_sem.at[t, k, q, p], frecv_sem.at[t, k, q, p], partner)

    def across(t):
        return remote((k_ref, v_ref)[t].at[partner], land.at[t, 3, core, pl.ds(0, k_ref.shape[1])], ssend_sem.at[t], srecv_sem.at[t], partner)

    def across_in(t):
        rows = land.at[t, 3, 1 - core, pl.ds(0, k_ref.shape[1])]
        return remote(rows, rows, ssend_sem.at[t], srecv_sem.at[t], partner)

    for t, k in ORDER:
        for half in range(2):
            for p in range(PIECES):
                main(t, k, half, p).start()
    for t in range(2):
        across(t).start()
    project(res_ref, gain_ref, (wq_ref, wk_ref, wv_ref), proj_ref, normed, total, ring, ring_sem)
    slabs, part, slab = held_refs[0].shape

    def hold(c, carry):
        for i in range(PARTS):
            pltpu.make_async_copy(wout_ref.at[pl.ds(i * part, part), pl.ds(pl.multiple_of(c * slab, slab), slab)], held_refs[i].at[c], held_sem.at[i]).start()
        return carry
    lax.fori_loop(0, slabs, hold, 0)
    for t, k in ORDER:
        for p in range(PIECES):
            for q in range(2):
                main_in(t, k, q, p).wait_recv()
                forward(t, k, q, p).start()
    for t in range(2):
        across(t).wait_send()
        across_in(t).wait_recv()
    for t, k in ORDER:
        for half in range(2):
            for p in range(PIECES):
                main(t, k, half, p).wait_send()
    for t, k in ORDER:
        for q in range(2):
            for p in range(PIECES):
                forward(t, k, q, p).wait_send()
                forward_in(t, k, q, p).wait_recv()
    for i in range(PARTS):
        pltpu.make_async_copy(held_refs[i], held_refs[i], held_sem.at[i]).wait()


def base(packed, k_rows, v_rows, residual, gain, w_query, w_key, w_value, w_out, land):
    dtype = k_rows.dtype
    dma = pltpu.SemaphoreType.DMA
    model_dim = residual.shape[1]
    proj_dim = w_query.shape[1] + w_key.shape[1] + w_value.shape[1]
    return pl.pallas_call(
        base_kernel,
        out_shape=(jax.ShapeDtypeStruct(land.shape, dtype), jax.ShapeDtypeStruct((LANES, proj_dim), dtype), )+ PARTS * (jax.ShapeDtypeStruct((w_out.shape[1] // SLAB, w_out.shape[0] // PARTS, SLAB), dtype),),
        in_specs=[HBM, HBM, HBM, VMEM, VMEM, HBM, HBM, HBM, HBM, HBM],
        out_specs=(HBM, VMEM) + PARTS * (ANY,),
        scratch_shapes=[
            pltpu.VMEM((LANES, model_dim), dtype), pltpu.VMEM((LANES, proj_dim), jnp.float32), pltpu.VMEM((8, 512, 512), dtype), dma((8,)), dma((PARTS,)),
            dma((2, 3, 2, PIECES)), dma((2, 3, 2, PIECES)), dma((2, 3, 2, PIECES)), dma((2, 3, 2, PIECES)), dma((2,)), dma((2,)),
        ],
        input_output_aliases={9: 0},
        compiler_params=pltpu.CompilerParams(has_side_effects=True, vmem_limit_bytes=BASE_VMEM),
        name='base',
    )(packed, k_rows, v_rows, residual, gain, w_query, w_key, w_value, w_out, land)


def build_kernel(len_ref, proj_ref, freq_ref, res_ref, *rest, depth):
    w_refs, (k_ref, v_ref, land, kc_ref, vc_ref, xout_ref, ring, tail, wide, made, scores, probs, mixed, ovec, q_ref, knew_ref, vnew_ref, ring_sem, tail_sem, made_sem) = rest[:PARTS], rest[PARTS:]
    step = pl.program_id(0)
    steps = WINDOW // STEP
    me = lax.axis_index('sh')
    core, chip, n = me % 2, me // 2, len_ref[me]
    offset = core * span(len_ref[2 * chip])
    chips = [chip, chip + 1 - 2 * (chip % 2), (chip + 2) % 4, 3 - chip]
    extra = tail.shape[2]
    heads = tail.shape[1]
    head_dim = tail.shape[3]

    def copies(t, start, size, dst, sem):
        own = 2 * chip + core
        other = 2 * chip + 1 - core
        rows = pl.ds(start, size)
        yield pltpu.make_async_copy((k_ref, v_ref)[t].at[me, rows], dst.at[own], sem)
        yield pltpu.make_async_copy(land.at[t, 3, 1 - core, rows], dst.at[other], sem)
        far = pl.ds(pl.multiple_of(offset + start, ALIGN), size)
        for k in range(3):
            for q in range(2):
                yield pltpu.make_async_copy(land.at[t, k, q, far], dst.at[2 * chips[k + 1] + q], sem)

    def heads_of_row():
        q_width = ovec.shape[1]
        group = q_width // (heads * head_dim)

        def part(at):
            return proj_ref[:1, at:at + head_dim]

        angles = n.astype(jnp.float32) * freq_ref[...]
        lane = lax.broadcasted_iota(jnp.int32, angles.shape, 1)
        cos, sin = jnp.cos(angles), jnp.sin(angles)
        sin = jnp.where(lane < head_dim // 2, -sin, sin)

        def turned(at):
            vals = part(at).astype(jnp.float32)
            return (vals * cos + pltpu.roll(vals, head_dim // 2, 1) * sin).astype(q_ref.dtype)

        for h in range(heads):
            q_ref[h] = jnp.concatenate([turned((h * group + g) * head_dim) for g in range(group)] + [jnp.zeros((q_ref.shape[1] - group, head_dim), q_ref.dtype)], axis=0)
        knew_ref[...] = jnp.concatenate([turned(q_width + h * head_dim) for h in range(heads)], axis=0)
        vnew_ref[...] = jnp.concatenate([part(q_width + (heads + h) * head_dim) for h in range(heads)], axis=0)

    def chunk(s, then):
        for t in range(2):
            local = s - t * steps
            pl.when((local >= 0) & (local < steps) & (local * STEP < n))(functools.partial(then, t, local))

    def fetch(s):
        def then(t, local):
            for copy in copies(t, pl.multiple_of(local * STEP, STEP), STEP, ring.at[s % depth], ring_sem.at[s % depth]):
                copy.start()
        chunk(s, then)

    def arrived(s):
        def then(t, local):
            whole = ring.at[s % depth]
            pltpu.make_async_copy(whole, whole, ring_sem.at[s % depth]).wait()
        chunk(s, then)

    def fetch_tail(t):
        @pl.when(n > WINDOW)
        def _():
            for copy in copies(t, WINDOW, extra, tail.at[t], tail_sem.at[t]):
                copy.start()

    def save(b, out_ref, local):
        size = BLOCK * heads // SAVES
        for i in range(SAVES):
            at = b * BLOCK * heads + i * size
            here = pl.ds(pl.multiple_of(at, size), size)
            there = pl.ds(pl.multiple_of(local * STEP * heads + at, size), size)
            pltpu.make_async_copy(made.at[step % MADE, here], out_ref.at[there], made_sem.at[step % MADE]).start(priority=1)

    def saved(s):
        whole = made.at[s % MADE]
        pltpu.make_async_copy(whole, whole, made_sem.at[s % MADE]).wait()

    @pl.when(step == 0)
    def _():
        fetch_tail(0)
        for s in range(depth - 1):
            fetch(jnp.int32(s))
        fetch_tail(1)
        mixed[...] = jnp.zeros_like(mixed)
        heads_of_row()
    fetch(step + depth - 1)
    arrived(step)

    @pl.when(step >= MADE)
    def _():
        saved(step)

    def assemble(t, local, new_ref, out_ref, use):
        first = local * STEP
        newest = lax.rem(n, WINDOW)
        wraps = (local == 0) & (n > WINDOW)
        dead = first > n
        plain = (first + STEP <= n) & ~wraps & ((newest < first) | (newest >= first + STEP))
        slot = step % depth
        out = step % MADE

        @pl.when(wraps)
        def _():
            whole = tail.at[t]
            pltpu.make_async_copy(whole, whole, tail_sem.at[t]).wait()

        @pl.when(~plain & ~dead)
        def _():
            def patch(c, carry):
                low = first + c * extra
                rows = pl.ds(pl.multiple_of(c * extra, extra), extra)

                @pl.when((low < n - WINDOW) | (low + extra > n) | ((newest >= low) & (newest < low + extra)))
                def _():
                    pos = low + lax.broadcasted_iota(jnp.int32, (extra, head_dim), 0)
                    for h in range(heads):
                        vals = jnp.where(pos < n - WINDOW, tail[t, h], ring[slot, h, rows, :])
                        vals = jnp.where(pos < n, vals, jnp.zeros_like(vals))
                        ring[slot, h, rows, :] = jnp.where(pos == newest, jnp.broadcast_to(new_ref[h:h + 1, :], vals.shape), vals)
                return carry
            lax.fori_loop(0, STEP // extra, patch, 0)

        @pl.when(dead)
        def _():
            def clear(b, carry):
                made[out, pl.ds(pl.multiple_of(b * BLOCK * heads, BLOCK * heads), BLOCK * heads), :] = jnp.zeros((BLOCK * heads, head_dim), made.dtype)
                save(b, out_ref, local)
                return carry
            lax.fori_loop(0, STEP // BLOCK, clear, 0)
            use(None, None, None)

        @pl.when(~dead)
        def _():
            def mix(b, carry):
                for h in range(heads):
                    vals = ring[slot, h, pl.ds(pl.multiple_of(b * BLOCK, BLOCK), BLOCK), :]
                    wide[pl.ds(h, BLOCK, stride=PITCH), :] = vals.astype(jnp.float32)
                    use(h, b, vals)
                rows = jnp.concatenate([wide[PITCH * p:PITCH * p + heads, :] for p in range(BLOCK)], axis=0)
                made[out, pl.ds(pl.multiple_of(b * BLOCK * heads, BLOCK * heads), BLOCK * heads), :] = rows.astype(made.dtype)
                save(b, out_ref, local)
                return carry
            lax.fori_loop(0, STEP // BLOCK, mix, 0)

    def slots_of(local, b, size):
        return pl.ds(pl.multiple_of(local * STEP + b * BLOCK, BLOCK), size)

    @pl.when(step < steps)
    def _():
        def use(h, b, vals):
            if h is None:
                scores[:, slots_of(step, 0, STEP)] = jnp.full((scores.shape[0], STEP), -jnp.inf)
                return
            slots = step * STEP + b * BLOCK + lax.broadcasted_iota(jnp.int32, (8, BLOCK), 1)
            live = (slots <= n) | (n >= WINDOW)
            s = lax.dot_general(q_ref[h], vals, (((1,), (1,)), ((), ())), preferred_element_type=jnp.float32) / head_dim ** 0.5
            scores[pl.ds(8 * h, 8), slots_of(step, b, BLOCK)] = jnp.where(live, s, -jnp.inf)
        assemble(0, step, knew_ref, kc_ref, use)

    @pl.when(step == steps)
    def _():
        for h in range(heads):
            s = scores[8 * h:8 * h + 8, :]
            e = jnp.exp(s - jnp.max(s, axis=-1, keepdims=True))
            probs[h] = (e / jnp.sum(e, axis=-1, keepdims=True)).astype(probs.dtype)

    @pl.when(step >= steps)
    def _():
        local = step - steps

        def use(h, b, vals):
            if h is None:
                return
            p = probs[h, :, slots_of(local, b, BLOCK)]
            mixed[h] += jnp.dot(p, vals, preferred_element_type=jnp.float32)
        assemble(1, local, vnew_ref, vc_ref, use)

    @pl.when(step == 2 * steps - 1)
    def _():
        group = ovec.shape[1] // (heads * head_dim)
        for h in range(heads):
            o = mixed[h].astype(ovec.dtype)
            for g in range(group):
                cols = pl.ds((h * group + g) * head_dim, head_dim)
                ovec[:, cols] = jnp.broadcast_to(o[g:g + 1], (ovec.shape[0], head_dim))
        slabs, part, slab = w_refs[0].shape
        width = GROUP * slab

        def column(c, carry):
            acc = jnp.zeros((ovec.shape[0], width), jnp.float32)
            for i, w_ref in enumerate(w_refs):
                block = jnp.concatenate([w_ref[c * GROUP + j] for j in range(GROUP)], axis=1)
                acc += jnp.dot(ovec[:, i * part:(i + 1) * part], block, preferred_element_type=jnp.float32)
            cols = pl.ds(pl.multiple_of(c * width, width), width)
            xout_ref[:, cols] = (res_ref[:, cols].astype(jnp.float32) + acc[:1]).astype(xout_ref.dtype)
            return carry
        lax.fori_loop(0, slabs // GROUP, column, 0)
        for s in range(2 * steps - MADE, 2 * steps):
            saved(s)


def build(lengths, proj, freq, residual, w_out, k_rows, v_rows, land, heads):
    seq_len, head_dim = k_rows.shape[1:]
    steps = WINDOW // STEP
    depth = 6
    dtype = k_rows.dtype
    cache = jax.ShapeDtypeStruct((WINDOW * heads, head_dim), dtype)
    dma = pltpu.SemaphoreType.DMA
    return pl.pallas_call(
        functools.partial(build_kernel, depth=depth),
        grid=(2 * steps,),
        out_shape=(cache, cache, jax.ShapeDtypeStruct(residual.shape, dtype)),
        in_specs=[SMEM, VMEM, VMEM, VMEM] + PARTS * [VMEM] + [HBM, HBM, HBM],
        out_specs=(HBM, HBM, VMEM),
        scratch_shapes=[
            pltpu.VMEM((depth, heads, STEP, head_dim), dtype),
            pltpu.VMEM((2, heads, seq_len - WINDOW, head_dim), dtype),
            pltpu.VMEM((BLOCK * PITCH, head_dim), jnp.float32),
            pltpu.VMEM((MADE, STEP * heads, head_dim), dtype),
            pltpu.VMEM((8 * heads, WINDOW), jnp.float32),
            pltpu.VMEM((heads, 8, WINDOW), dtype),
            pltpu.VMEM((heads, 8, head_dim), jnp.float32),
            pltpu.VMEM((LANES, PARTS * w_out[0].shape[1]), dtype),
            pltpu.VMEM((heads, 8, head_dim), dtype),
            pltpu.VMEM((heads, head_dim), dtype),
            pltpu.VMEM((heads, head_dim), dtype),
            dma((depth,)), dma((2,)), dma((MADE,)),
        ],
        compiler_params=pltpu.CompilerParams(vmem_limit_bytes=BUILD_VMEM),
        name='build',
    )(lengths, proj, freq, residual, *w_out, k_rows, v_rows, land)


def frequencies(head_dim):
    half = THETA ** (-2.0 * np.arange(head_dim // 2, dtype=np.float64) / head_dim)
    return np.concatenate([half, half])[None].astype(np.float32)


def solution(mesh):
    head_spec = P('dp', None, 'sh', None)
    row_spec = P(('dp', 'sh'))
    full_spec = P(None, None)

    def per_device(k_prefill, v_prefill, lengths, residual, norm_gain, w_query, w_key, w_value, w_out):
        num_rows, seq_len, _, head_dim = k_prefill.shape
        kv_heads = w_key.shape[1] // head_dim
        k_rows = k_prefill.reshape(num_rows, seq_len, head_dim)
        v_rows = v_prefill.reshape(num_rows, seq_len, head_dim)
        packed, size = pack(lengths, k_rows, v_rows)
        sizes = (list_length(seq_len) - BASE) // QUANTUM
        land = lax.switch(size[0], [functools.partial(more, extra=i * QUANTUM) for i in range(sizes + 1)], packed)
        land, proj, *held = base(packed, k_rows, v_rows, residual, norm_gain.reshape(-1, head_dim), w_query, w_key, w_value, w_out, land)
        k_cache, v_cache, resid_out = build(lengths, proj, jnp.asarray(frequencies(head_dim)), residual, held, k_rows, v_rows, land, kv_heads)
        shape = (1, WINDOW, kv_heads, head_dim)
        return resid_out, k_cache.reshape(shape), v_cache.reshape(shape)
    return jax.shard_map(per_device, mesh=mesh, in_specs=(head_spec, head_spec, P('dp'), P(('dp', 'sh'), None), P(None), full_spec, full_spec, full_spec, full_spec), out_specs=(P(('dp', 'sh'), None), row_spec, row_spec), check_vma=False)
```

```python
import functools

import jax
import jax.numpy as jnp
import numpy as np
from jax import lax
from jax.experimental import pallas as pl
from jax.experimental.pallas import tpu as pltpu
from jax.sharding import PartitionSpec as P

WINDOW = 4096
THETA = 10000.0
EPS = 1e-5
ALIGN = 16
HALF = 2208
BASE = 2 * HALF
CUTS = 4
PIECES = 2
QUANTUM = 128
STEP = 512
SLAB = 128
GROUP = 4
DEPTH = 12
MADE = 4
SAVES = 2
BLOCK = 128
PITCH = 9
PARTS = 4
BASE_VMEM = 14 * 2**20
BUILD_VMEM = 20 * 2**20 + 2**18
LANES = 16
ORDER = [(t, k) for k in range(3) for t in range(2)]
ANY = pl.BlockSpec(memory_space=pl.ANY)
VMEM = pl.BlockSpec(memory_space=pltpu.VMEM)
SMEM = pl.BlockSpec(memory_space=pltpu.SMEM)
HBM = pl.BlockSpec(memory_space=pltpu.HBM)


def list_length(seq_len):
    return BASE + -(-(2 * seq_len - BASE) // QUANTUM) * QUANTUM


def span(length):
    return (length + (ALIGN - 1)) // ALIGN * ALIGN


def pack_kernel(len_ref, k_ref, v_ref, out_ref, size_ref, lists, first_sem, second_sem, store_sem, *, seq_len):
    chip = lax.axis_index('sh') // 2
    list_len = lists.shape[2]
    peers = [chip + 1 - 2 * (chip % 2), (chip + 2) % 4, 3 - chip]

    part = seq_len // CUTS

    def spans_of(k):
        return span(len_ref[2 * peers[k]]), span(len_ref[2 * peers[k] + 1])

    def loads(t, k, second):
        src = (k_ref, v_ref)[t]
        spans = spans_of(k)
        for i in range(CUTS):
            start = pl.multiple_of(second * spans[0] + i * part, ALIGN)
            yield spans[second] > i * part, pltpu.make_async_copy(src.at[2 * peers[k] + second, pl.ds(i * part, part)], lists.at[t, k, pl.ds(start, part)], (first_sem, second_sem)[second].at[t, k, i])

    def stores(t, k):
        size = list_len // (2 * CUTS)
        for i in range(2 * CUTS):
            rows = pl.ds(i * size, size)
            yield sum(spans_of(k)) > i * size, pltpu.make_async_copy(lists.at[t, k, rows], out_ref.at[t, k, rows], store_sem.at[t, k, i])

    def start(copies):
        for live, copy in copies:
            pl.when(live)(copy.start)

    def wait(copies):
        for live, copy in copies:
            pl.when(live)(copy.wait)

    for t, k in ORDER:
        start(loads(t, k, 0))
    longest = span(len_ref[0]) + span(len_ref[1])
    for c in range(1, len_ref.shape[0] // 2):
        longest = jnp.maximum(longest, span(len_ref[2 * c]) + span(len_ref[2 * c + 1]))
    size_ref[0] = jnp.clip((longest - BASE + QUANTUM - 1) // QUANTUM, 0, (list_len - BASE) // QUANTUM)
    for t, k in ORDER:
        wait(loads(t, k, 0))
        start(loads(t, k, 1))
    for t, k in ORDER:
        wait(loads(t, k, 1))
        start(stores(t, k))
    for t, k in ORDER:
        wait(stores(t, k))


def pack(lengths, k_rows, v_rows):
    seq_len, head_dim = k_rows.shape[1:]
    shape = (2, 3, list_length(seq_len), head_dim)
    return pl.pallas_call(
        functools.partial(pack_kernel, seq_len=seq_len),
        out_shape=(jax.ShapeDtypeStruct(shape, k_rows.dtype), jax.ShapeDtypeStruct((1,), jnp.int32)),
        in_specs=[SMEM, HBM, HBM],
        out_specs=(HBM, SMEM),
        scratch_shapes=[pltpu.VMEM(shape, k_rows.dtype), pltpu.SemaphoreType.DMA((2, 3, CUTS)), pltpu.SemaphoreType.DMA((2, 3, CUTS)), pltpu.SemaphoreType.DMA((2, 3, 2 * CUTS))],
        compiler_params=pltpu.CompilerParams(vmem_limit_bytes=60 * 2**20),
        name='pack',
    )(lengths, k_rows, v_rows)


def project(res_ref, gain_ref, weights, proj_ref, normed, total, ring, ring_sem):
    depth, side, _ = ring.shape
    resid = res_ref[...].astype(jnp.float32)
    inv_rms = lax.rsqrt(jnp.sum(resid * resid, axis=-1, keepdims=True) / resid.shape[-1] + EPS)
    lanes = gain_ref.shape[1]
    for r in range(gain_ref.shape[0]):
        cols = slice(r * lanes, (r + 1) * lanes)
        row = (resid[:, cols] * inv_rms * gain_ref[r:r + 1, :].astype(jnp.float32)).astype(normed.dtype)
        normed[:, cols] = jnp.broadcast_to(row, (normed.shape[0], lanes))
    total[...] = jnp.zeros_like(total)
    deep = normed.shape[1] // side

    def at(i):
        return pl.multiple_of(i // deep * side, side), pl.multiple_of(i % deep * side, side)

    def fetch(i):
        left, top = at(i)
        first = 0
        for w_ref in weights:
            width = w_ref.shape[1]

            @pl.when((left >= first) & (left < first + width))
            def _(w_ref=w_ref, first=first):
                here = pl.multiple_of(left - first, side)
                pltpu.make_async_copy(w_ref.at[pl.ds(top, side), pl.ds(here, side)], ring.at[i % depth], ring_sem.at[i % depth]).start()
            first += width

    blocks = total.shape[1] // side * deep

    def prime(i, carry):
        fetch(i)
        return carry
    lax.fori_loop(0, depth - 1, prime, 0)

    def step(i, carry):
        @pl.when(i + depth - 1 < blocks)
        def _():
            fetch(i + depth - 1)
        pltpu.make_async_copy(weights[0].at[pl.ds(0, side), pl.ds(0, side)], ring.at[i % depth], ring_sem.at[i % depth]).wait()
        left, top = at(i)
        total[:, pl.ds(left, side)] += jnp.dot(normed[:, pl.ds(top, side)], ring[i % depth], preferred_element_type=jnp.float32)
        return carry
    lax.fori_loop(0, blocks, step, 0)
    proj_ref[...] = total[...].astype(proj_ref.dtype)


def remote(src, dst, send, recv, device):
    return pltpu.make_async_remote_copy(src_ref=src, dst_ref=dst, send_sem=send, recv_sem=recv, device_id={'sh': device}, device_id_type=pl.DeviceIdType.MESH)


def more_kernel(packed, land, send_sem, recv_sem, *, extra):
    me = lax.axis_index('sh')
    core = me % 2
    chip = me // 2
    peers = [chip + 1 - 2 * (chip % 2), (chip + 2) % 4, 3 - chip]
    rows = pl.ds(BASE, extra)

    def out(t, k):
        return remote(packed.at[t, k, rows], land.at[t, k, core, rows], send_sem.at[t, k], recv_sem.at[t, k, core], 2 * peers[k] + 1)

    def into(t, k, q):
        here = land.at[t, k, q, rows]
        return remote(here, here, send_sem.at[t, k], recv_sem.at[t, k, q], me)

    for t, k in ORDER:
        out(t, k).start()
    for t, k in ORDER:
        out(t, k).wait_send()

    @pl.when(core == 1)
    def _():
        for t, k in ORDER:
            for q in range(2):
                into(t, k, q).wait_recv()


def nothing_kernel(packed, land):
    pass


def more(packed, *, extra):
    shape = jax.ShapeDtypeStruct((2, 4, 2) + packed.shape[2:], packed.dtype)
    if not extra:
        return pl.pallas_call(nothing_kernel, out_shape=shape, in_specs=[HBM], out_specs=HBM, compiler_params=pltpu.CompilerParams(vmem_limit_bytes=60 * 2**20), name='more_0')(packed)
    dma = pltpu.SemaphoreType.DMA
    return pl.pallas_call(
        functools.partial(more_kernel, extra=extra),
        out_shape=shape,
        in_specs=[HBM],
        out_specs=HBM,
        scratch_shapes=[dma((2, 3)), dma((2, 3, 2))],
        compiler_params=pltpu.CompilerParams(has_side_effects=True, vmem_limit_bytes=60 * 2**20),
        name=f'more_{extra}',
    )(packed)


def base_kernel(packed, k_ref, v_ref, res_ref, gain_ref, wq_ref, wk_ref, wv_ref, wout_ref, _, land, proj_ref, *rest):
    held_refs, (normed, total, ring, ring_sem, held_sem, send_sem, recv_sem, fsend_sem, frecv_sem, ssend_sem, srecv_sem) = rest[:PARTS], rest[PARTS:]
    me = lax.axis_index('sh')
    core = me % 2
    chip = me // 2
    partner = me + 1 - 2 * core
    peers = [chip + 1 - 2 * (chip % 2), (chip + 2) % 4, 3 - chip]

    size = HALF // PIECES

    def main(t, k, half, p):
        rows = pl.ds(half * HALF + p * size, size)
        return remote(packed.at[t, k, rows], land.at[t, k, core, rows], send_sem.at[t, k, half, p], recv_sem.at[t, k, core, p], 2 * peers[k] + half)

    def forward(t, k, q, p):
        rows = land.at[t, k, q, pl.ds(core * HALF + p * size, size)]
        return remote(rows, rows, fsend_sem.at[t, k, q, p], frecv_sem.at[t, k, q, p], partner)

    def main_in(t, k, q, p):
        rows = land.at[t, k, q, pl.ds(core * HALF + p * size, size)]
        return remote(rows, rows, fsend_sem.at[t, k, q, p], recv_sem.at[t, k, q, p], partner)

    def forward_in(t, k, q, p):
        rows = land.at[t, k, q, pl.ds((1 - core) * HALF + p * size, size)]
        return remote(rows, rows, fsend_sem.at[t, k, q, p], frecv_sem.at[t, k, q, p], partner)

    def across(t):
        return remote((k_ref, v_ref)[t].at[partner], land.at[t, 3, core, pl.ds(0, k_ref.shape[1])], ssend_sem.at[t], srecv_sem.at[t], partner)

    def across_in(t):
        rows = land.at[t, 3, 1 - core, pl.ds(0, k_ref.shape[1])]
        return remote(rows, rows, ssend_sem.at[t], srecv_sem.at[t], partner)

    for t, k in ORDER:
        for half in range(2):
            for p in range(PIECES):
                main(t, k, half, p).start()
    for t in range(2):
        across(t).start()
    project(res_ref, gain_ref, (wq_ref, wk_ref, wv_ref), proj_ref, normed, total, ring, ring_sem)
    slabs, part, slab = held_refs[0].shape

    def hold(c, carry):
        for i in range(PARTS):
            pltpu.make_async_copy(wout_ref.at[pl.ds(i * part, part), pl.ds(pl.multiple_of(c * slab, slab), slab)], held_refs[i].at[c], held_sem.at[i]).start()
        return carry
    lax.fori_loop(0, slabs, hold, 0)
    for t, k in ORDER:
        for p in range(PIECES):
            for q in range(2):
                main_in(t, k, q, p).wait_recv()
                forward(t, k, q, p).start()
    for t in range(2):
        across(t).wait_send()
        across_in(t).wait_recv()
    for t, k in ORDER:
        for half in range(2):
            for p in range(PIECES):
                main(t, k, half, p).wait_send()
    for t, k in ORDER:
        for q in range(2):
            for p in range(PIECES):
                forward(t, k, q, p).wait_send()
                forward_in(t, k, q, p).wait_recv()
    for i in range(PARTS):
        pltpu.make_async_copy(held_refs[i], held_refs[i], held_sem.at[i]).wait()


def base(packed, k_rows, v_rows, residual, gain, w_query, w_key, w_value, w_out, land):
    dtype = k_rows.dtype
    dma = pltpu.SemaphoreType.DMA
    model_dim = residual.shape[1]
    proj_dim = w_query.shape[1] + w_key.shape[1] + w_value.shape[1]
    return pl.pallas_call(
        base_kernel,
        out_shape=(jax.ShapeDtypeStruct(land.shape, dtype), jax.ShapeDtypeStruct((LANES, proj_dim), dtype), )+ PARTS * (jax.ShapeDtypeStruct((w_out.shape[1] // SLAB, w_out.shape[0] // PARTS, SLAB), dtype),),
        in_specs=[HBM, HBM, HBM, VMEM, VMEM, HBM, HBM, HBM, HBM, HBM],
        out_specs=(HBM, VMEM) + PARTS * (ANY,),
        scratch_shapes=[
            pltpu.VMEM((LANES, model_dim), dtype), pltpu.VMEM((LANES, proj_dim), jnp.float32), pltpu.VMEM((8, 512, 512), dtype), dma((8,)), dma((PARTS,)),
            dma((2, 3, 2, PIECES)), dma((2, 3, 2, PIECES)), dma((2, 3, 2, PIECES)), dma((2, 3, 2, PIECES)), dma((2,)), dma((2,)),
        ],
        input_output_aliases={9: 0},
        compiler_params=pltpu.CompilerParams(has_side_effects=True, vmem_limit_bytes=BASE_VMEM),
        name='base',
    )(packed, k_rows, v_rows, residual, gain, w_query, w_key, w_value, w_out, land)


def build_kernel(len_ref, proj_ref, freq_ref, res_ref, *rest, depth):
    w_refs, (k_ref, v_ref, land, kc_ref, vc_ref, xout_ref, ring, tail, wide, made, scores, probs, mixed, ovec, q_ref, knew_ref, vnew_ref, ring_sem, tail_sem, made_sem) = rest[:PARTS], rest[PARTS:]
    step = pl.program_id(0)
    steps = WINDOW // STEP
    me = lax.axis_index('sh')
    core, chip, n = me % 2, me // 2, len_ref[me]
    offset = core * span(len_ref[2 * chip])
    chips = [chip, chip + 1 - 2 * (chip % 2), (chip + 2) % 4, 3 - chip]
    extra = tail.shape[2]
    heads = tail.shape[1]
    head_dim = tail.shape[3]

    def copies(t, start, size, dst, sem):
        own = 2 * chip + core
        other = 2 * chip + 1 - core
        rows = pl.ds(start, size)
        yield pltpu.make_async_copy((k_ref, v_ref)[t].at[me, rows], dst.at[own], sem)
        yield pltpu.make_async_copy(land.at[t, 3, 1 - core, rows], dst.at[other], sem)
        far = pl.ds(pl.multiple_of(offset + start, ALIGN), size)
        for k in range(3):
            for q in range(2):
                yield pltpu.make_async_copy(land.at[t, k, q, far], dst.at[2 * chips[k + 1] + q], sem)

    def heads_of_row():
        q_width = ovec.shape[1]
        group = q_width // (heads * head_dim)

        def part(at):
            return proj_ref[:1, at:at + head_dim]

        angles = n.astype(jnp.float32) * freq_ref[...]
        lane = lax.broadcasted_iota(jnp.int32, angles.shape, 1)
        cos, sin = jnp.cos(angles), jnp.sin(angles)
        sin = jnp.where(lane < head_dim // 2, -sin, sin)

        def turned(at):
            vals = part(at).astype(jnp.float32)
            return (vals * cos + pltpu.roll(vals, head_dim // 2, 1) * sin).astype(q_ref.dtype)

        for h in range(heads):
            q_ref[h] = jnp.concatenate([turned((h * group + g) * head_dim) for g in range(group)] + [jnp.zeros((q_ref.shape[1] - group, head_dim), q_ref.dtype)], axis=0)
        knew_ref[...] = jnp.concatenate([turned(q_width + h * head_dim) for h in range(heads)], axis=0)
        vnew_ref[...] = jnp.concatenate([part(q_width + (heads + h) * head_dim) for h in range(heads)], axis=0)

    def chunk(s, then):
        for t in range(2):
            local = s - t * steps
            pl.when((local >= 0) & (local < steps) & (local * STEP < n))(functools.partial(then, t, local))

    def fetch(s):
        def then(t, local):
            for copy in copies(t, pl.multiple_of(local * STEP, STEP), STEP, ring.at[s % depth], ring_sem.at[s % depth]):
                copy.start()
        chunk(s, then)

    def arrived(s):
        def then(t, local):
            whole = ring.at[s % depth]
            pltpu.make_async_copy(whole, whole, ring_sem.at[s % depth]).wait()
        chunk(s, then)

    def fetch_tail(t):
        @pl.when(n > WINDOW)
        def _():
            for copy in copies(t, WINDOW, extra, tail.at[t], tail_sem.at[t]):
                copy.start()

    def save(b, out_ref, local):
        size = BLOCK * heads // SAVES
        for i in range(SAVES):
            at = b * BLOCK * heads + i * size
            here = pl.ds(pl.multiple_of(at, size), size)
            there = pl.ds(pl.multiple_of(local * STEP * heads + at, size), size)
            pltpu.make_async_copy(made.at[step % MADE, here], out_ref.at[there], made_sem.at[step % MADE]).start(priority=1)

    def saved(s):
        whole = made.at[s % MADE]
        pltpu.make_async_copy(whole, whole, made_sem.at[s % MADE]).wait()

    @pl.when(step == 0)
    def _():
        def ahead(s, carry):
            fetch(s)
            return carry
        fetch(jnp.int32(0))
        fetch_tail(0)
        lax.fori_loop(1, depth - 1, ahead, 0)
        fetch_tail(1)
        mixed[...] = jnp.zeros_like(mixed)
        heads_of_row()
    fetch(step + depth - 1)
    arrived(step)

    @pl.when(step >= MADE)
    def _():
        saved(step)

    def assemble(t, local, new_ref, out_ref, use):
        first = local * STEP
        newest = lax.rem(n, WINDOW)
        wraps = (local == 0) & (n > WINDOW)
        dead = first > n
        plain = (first + STEP <= n) & ~wraps & ((newest < first) | (newest >= first + STEP))
        slot = step % depth
        out = step % MADE

        @pl.when(wraps)
        def _():
            whole = tail.at[t]
            pltpu.make_async_copy(whole, whole, tail_sem.at[t]).wait()

        @pl.when(~plain & ~dead)
        def _():
            def patch(c, carry):
                low = first + c * extra
                rows = pl.ds(pl.multiple_of(c * extra, extra), extra)

                @pl.when((low < n - WINDOW) | (low + extra > n) | ((newest >= low) & (newest < low + extra)))
                def _():
                    pos = low + lax.broadcasted_iota(jnp.int32, (extra, head_dim), 0)
                    for h in range(heads):
                        vals = jnp.where(pos < n - WINDOW, tail[t, h], ring[slot, h, rows, :])
                        vals = jnp.where(pos < n, vals, jnp.zeros_like(vals))
                        ring[slot, h, rows, :] = jnp.where(pos == newest, jnp.broadcast_to(new_ref[h:h + 1, :], vals.shape), vals)
                return carry
            lax.fori_loop(0, STEP // extra, patch, 0)

        @pl.when(dead)
        def _():
            def clear(b, carry):
                made[out, pl.ds(pl.multiple_of(b * BLOCK * heads, BLOCK * heads), BLOCK * heads), :] = jnp.zeros((BLOCK * heads, head_dim), made.dtype)
                save(b, out_ref, local)
                return carry
            lax.fori_loop(0, STEP // BLOCK, clear, 0)
            use(None, None, None)

        @pl.when(~dead)
        def _():
            def mix(b, carry):
                for h in range(heads):
                    vals = ring[slot, h, pl.ds(pl.multiple_of(b * BLOCK, BLOCK), BLOCK), :]
                    wide[pl.ds(h, BLOCK, stride=PITCH), :] = vals.astype(jnp.float32)
                    use(h, b, vals)
                rows = jnp.concatenate([wide[PITCH * p:PITCH * p + heads, :] for p in range(BLOCK)], axis=0)
                made[out, pl.ds(pl.multiple_of(b * BLOCK * heads, BLOCK * heads), BLOCK * heads), :] = rows.astype(made.dtype)
                save(b, out_ref, local)
                return carry
            lax.fori_loop(0, STEP // BLOCK, mix, 0)

    def slots_of(local, b, size):
        return pl.ds(pl.multiple_of(local * STEP + b * BLOCK, BLOCK), size)

    @pl.when(step < steps)
    def _():
        def use(h, b, vals):
            if h is None:
                scores[:, slots_of(step, 0, STEP)] = jnp.full((scores.shape[0], STEP), -jnp.inf)
                return
            slots = step * STEP + b * BLOCK + lax.broadcasted_iota(jnp.int32, (8, BLOCK), 1)
            live = (slots <= n) | (n >= WINDOW)
            s = lax.dot_general(q_ref[h], vals, (((1,), (1,)), ((), ())), preferred_element_type=jnp.float32) / head_dim ** 0.5
            scores[pl.ds(8 * h, 8), slots_of(step, b, BLOCK)] = jnp.where(live, s, -jnp.inf)
        assemble(0, step, knew_ref, kc_ref, use)

    @pl.when(step == steps)
    def _():
        for h in range(heads):
            s = scores[8 * h:8 * h + 8, :]
            e = jnp.exp(s - jnp.max(s, axis=-1, keepdims=True))
            probs[h] = (e / jnp.sum(e, axis=-1, keepdims=True)).astype(probs.dtype)

    @pl.when(step >= steps)
    def _():
        local = step - steps

        def use(h, b, vals):
            if h is None:
                return
            p = probs[h, :, slots_of(local, b, BLOCK)]
            mixed[h] += jnp.dot(p, vals, preferred_element_type=jnp.float32)
        assemble(1, local, vnew_ref, vc_ref, use)

    @pl.when(step == 2 * steps - 1)
    def _():
        group = ovec.shape[1] // (heads * head_dim)
        for h in range(heads):
            o = mixed[h].astype(ovec.dtype)
            for g in range(group):
                cols = pl.ds((h * group + g) * head_dim, head_dim)
                ovec[:, cols] = jnp.broadcast_to(o[g:g + 1], (ovec.shape[0], head_dim))
        slabs, part, slab = w_refs[0].shape
        width = GROUP * slab

        def column(c, carry):
            acc = jnp.zeros((ovec.shape[0], width), jnp.float32)
            for i, w_ref in enumerate(w_refs):
                block = jnp.concatenate([w_ref[c * GROUP + j] for j in range(GROUP)], axis=1)
                acc += jnp.dot(ovec[:, i * part:(i + 1) * part], block, preferred_element_type=jnp.float32)
            cols = pl.ds(pl.multiple_of(c * width, width), width)
            xout_ref[:, cols] = (res_ref[:, cols].astype(jnp.float32) + acc[:1]).astype(xout_ref.dtype)
            return carry
        lax.fori_loop(0, slabs // GROUP, column, 0)
        for s in range(2 * steps - MADE, 2 * steps):
            saved(s)


def build(lengths, proj, freq, residual, w_out, k_rows, v_rows, land, heads):
    seq_len, head_dim = k_rows.shape[1:]
    steps = WINDOW // STEP
    depth = DEPTH
    dtype = k_rows.dtype
    cache = jax.ShapeDtypeStruct((WINDOW * heads, head_dim), dtype)
    dma = pltpu.SemaphoreType.DMA
    return pl.pallas_call(
        functools.partial(build_kernel, depth=depth),
        grid=(2 * steps,),
        out_shape=(cache, cache, jax.ShapeDtypeStruct(residual.shape, dtype)),
        in_specs=[SMEM, VMEM, VMEM, VMEM] + PARTS * [VMEM] + [HBM, HBM, HBM],
        out_specs=(HBM, HBM, VMEM),
        scratch_shapes=[
            pltpu.VMEM((depth, heads, STEP, head_dim), dtype),
            pltpu.VMEM((2, heads, seq_len - WINDOW, head_dim), dtype),
            pltpu.VMEM((BLOCK * PITCH, head_dim), jnp.float32),
            pltpu.VMEM((MADE, STEP * heads, head_dim), dtype),
            pltpu.VMEM((8 * heads, WINDOW), jnp.float32),
            pltpu.VMEM((heads, 8, WINDOW), dtype),
            pltpu.VMEM((heads, 8, head_dim), jnp.float32),
            pltpu.VMEM((LANES, PARTS * w_out[0].shape[1]), dtype),
            pltpu.VMEM((heads, 8, head_dim), dtype),
            pltpu.VMEM((heads, head_dim), dtype),
            pltpu.VMEM((heads, head_dim), dtype),
            dma((depth,)), dma((2,)), dma((MADE,)),
        ],
        compiler_params=pltpu.CompilerParams(vmem_limit_bytes=BUILD_VMEM),
        name='build',
    )(lengths, proj, freq, residual, *w_out, k_rows, v_rows, land)


def frequencies(head_dim):
    half = THETA ** (-2.0 * np.arange(head_dim // 2, dtype=np.float64) / head_dim)
    return np.concatenate([half, half])[None].astype(np.float32)


def solution(mesh):
    head_spec = P('dp', None, 'sh', None)
    row_spec = P(('dp', 'sh'))
    full_spec = P(None, None)

    def per_device(k_prefill, v_prefill, lengths, residual, norm_gain, w_query, w_key, w_value, w_out):
        num_rows, seq_len, _, head_dim = k_prefill.shape
        kv_heads = w_key.shape[1] // head_dim
        k_rows = k_prefill.reshape(num_rows, seq_len, head_dim)
        v_rows = v_prefill.reshape(num_rows, seq_len, head_dim)
        packed, size = pack(lengths, k_rows, v_rows)
        sizes = (list_length(seq_len) - BASE) // QUANTUM
        land = lax.switch(size[0], [functools.partial(more, extra=i * QUANTUM) for i in range(sizes + 1)], packed)
        land, proj, *held = base(packed, k_rows, v_rows, residual, norm_gain.reshape(-1, head_dim), w_query, w_key, w_value, w_out, land)
        k_cache, v_cache, resid_out = build(lengths, proj, jnp.asarray(frequencies(head_dim)), residual, held, k_rows, v_rows, land, kv_heads)
        shape = (1, WINDOW, kv_heads, head_dim)
        return resid_out, k_cache.reshape(shape), v_cache.reshape(shape)
    return jax.shard_map(per_device, mesh=mesh, in_specs=(head_spec, head_spec, P('dp'), P(('dp', 'sh'), None), P(None), full_spec, full_spec, full_spec, full_spec), out_specs=(P(('dp', 'sh'), None), row_spec, row_spec), check_vma=False)
```

```python
import functools

import jax
import jax.numpy as jnp
import numpy as np
from jax import lax
from jax.experimental import pallas as pl
from jax.experimental.pallas import tpu as pltpu
from jax.sharding import PartitionSpec as P

WINDOW = 4096
THETA = 10000.0
EPS = 1e-5
ALIGN = 16
HALF = 2208
BASE = 2 * HALF
CUTS = 4
PIECES = 2
QUANTUM = 128
STEP = 512
SLAB = 128
GROUP = 4
DEPTH = 10
MADE = 4
SAVES = 4
BLOCK = 256
PITCH = 9
PARTS = 4
BASE_VMEM = 14 * 2**20
BUILD_VMEM = 19 * 2**20
LANES = 16
ORDER = [(t, k) for k in range(3) for t in range(2)]
ANY = pl.BlockSpec(memory_space=pl.ANY)
VMEM = pl.BlockSpec(memory_space=pltpu.VMEM)
SMEM = pl.BlockSpec(memory_space=pltpu.SMEM)
HBM = pl.BlockSpec(memory_space=pltpu.HBM)


def list_length(seq_len):
    return BASE + -(-(2 * seq_len - BASE) // QUANTUM) * QUANTUM


def span(length):
    return (length + (ALIGN - 1)) // ALIGN * ALIGN


def pack_kernel(len_ref, k_ref, v_ref, out_ref, size_ref, lists, first_sem, second_sem, store_sem, *, seq_len):
    chip = lax.axis_index('sh') // 2
    list_len = lists.shape[2]
    peers = [chip + 1 - 2 * (chip % 2), (chip + 2) % 4, 3 - chip]

    part = seq_len // CUTS

    def spans_of(k):
        return span(len_ref[2 * peers[k]]), span(len_ref[2 * peers[k] + 1])

    def loads(t, k, second):
        src = (k_ref, v_ref)[t]
        spans = spans_of(k)
        for i in range(CUTS):
            start = pl.multiple_of(second * spans[0] + i * part, ALIGN)
            yield spans[second] > i * part, pltpu.make_async_copy(src.at[2 * peers[k] + second, pl.ds(i * part, part)], lists.at[t, k, pl.ds(start, part)], (first_sem, second_sem)[second].at[t, k, i])

    def stores(t, k):
        size = list_len // (2 * CUTS)
        for i in range(2 * CUTS):
            rows = pl.ds(i * size, size)
            yield sum(spans_of(k)) > i * size, pltpu.make_async_copy(lists.at[t, k, rows], out_ref.at[t, k, rows], store_sem.at[t, k, i])

    def start(copies):
        for live, copy in copies:
            pl.when(live)(copy.start)

    def wait(copies):
        for live, copy in copies:
            pl.when(live)(copy.wait)

    for t, k in ORDER:
        start(loads(t, k, 0))
    longest = span(len_ref[0]) + span(len_ref[1])
    for c in range(1, len_ref.shape[0] // 2):
        longest = jnp.maximum(longest, span(len_ref[2 * c]) + span(len_ref[2 * c + 1]))
    size_ref[0] = jnp.clip((longest - BASE + QUANTUM - 1) // QUANTUM, 0, (list_len - BASE) // QUANTUM)
    for t, k in ORDER:
        wait(loads(t, k, 0))
        start(loads(t, k, 1))
    for t, k in ORDER:
        wait(loads(t, k, 1))
        start(stores(t, k))
    for t, k in ORDER:
        wait(stores(t, k))


def pack(lengths, k_rows, v_rows):
    seq_len, head_dim = k_rows.shape[1:]
    shape = (2, 3, list_length(seq_len), head_dim)
    return pl.pallas_call(
        functools.partial(pack_kernel, seq_len=seq_len),
        out_shape=(jax.ShapeDtypeStruct(shape, k_rows.dtype), jax.ShapeDtypeStruct((1,), jnp.int32)),
        in_specs=[SMEM, HBM, HBM],
        out_specs=(HBM, SMEM),
        scratch_shapes=[pltpu.VMEM(shape, k_rows.dtype), pltpu.SemaphoreType.DMA((2, 3, CUTS)), pltpu.SemaphoreType.DMA((2, 3, CUTS)), pltpu.SemaphoreType.DMA((2, 3, 2 * CUTS))],
        compiler_params=pltpu.CompilerParams(vmem_limit_bytes=60 * 2**20),
        name='pack',
    )(lengths, k_rows, v_rows)


def project(res_ref, gain_ref, weights, proj_ref, normed, total, ring, ring_sem):
    depth, side, _ = ring.shape
    resid = res_ref[...].astype(jnp.float32)
    inv_rms = lax.rsqrt(jnp.sum(resid * resid, axis=-1, keepdims=True) / resid.shape[-1] + EPS)
    lanes = gain_ref.shape[1]
    for r in range(gain_ref.shape[0]):
        cols = slice(r * lanes, (r + 1) * lanes)
        row = (resid[:, cols] * inv_rms * gain_ref[r:r + 1, :].astype(jnp.float32)).astype(normed.dtype)
        normed[:, cols] = jnp.broadcast_to(row, (normed.shape[0], lanes))
    total[...] = jnp.zeros_like(total)
    deep = normed.shape[1] // side

    def at(i):
        return pl.multiple_of(i // deep * side, side), pl.multiple_of(i % deep * side, side)

    def fetch(i):
        left, top = at(i)
        first = 0
        for w_ref in weights:
            width = w_ref.shape[1]

            @pl.when((left >= first) & (left < first + width))
            def _(w_ref=w_ref, first=first):
                here = pl.multiple_of(left - first, side)
                pltpu.make_async_copy(w_ref.at[pl.ds(top, side), pl.ds(here, side)], ring.at[i % depth], ring_sem.at[i % depth]).start()
            first += width

    blocks = total.shape[1] // side * deep

    def prime(i, carry):
        fetch(i)
        return carry
    lax.fori_loop(0, depth - 1, prime, 0)

    def step(i, carry):
        @pl.when(i + depth - 1 < blocks)
        def _():
            fetch(i + depth - 1)
        pltpu.make_async_copy(weights[0].at[pl.ds(0, side), pl.ds(0, side)], ring.at[i % depth], ring_sem.at[i % depth]).wait()
        left, top = at(i)
        total[:, pl.ds(left, side)] += jnp.dot(normed[:, pl.ds(top, side)], ring[i % depth], preferred_element_type=jnp.float32)
        return carry
    lax.fori_loop(0, blocks, step, 0)
    proj_ref[...] = total[...].astype(proj_ref.dtype)


def remote(src, dst, send, recv, device):
    return pltpu.make_async_remote_copy(src_ref=src, dst_ref=dst, send_sem=send, recv_sem=recv, device_id={'sh': device}, device_id_type=pl.DeviceIdType.MESH)


def more_kernel(packed, land, send_sem, recv_sem, *, extra):
    me = lax.axis_index('sh')
    core = me % 2
    chip = me // 2
    peers = [chip + 1 - 2 * (chip % 2), (chip + 2) % 4, 3 - chip]
    rows = pl.ds(BASE, extra)

    def out(t, k):
        return remote(packed.at[t, k, rows], land.at[t, k, core, rows], send_sem.at[t, k], recv_sem.at[t, k, core], 2 * peers[k] + 1)

    def into(t, k, q):
        here = land.at[t, k, q, rows]
        return remote(here, here, send_sem.at[t, k], recv_sem.at[t, k, q], me)

    for t, k in ORDER:
        out(t, k).start()
    for t, k in ORDER:
        out(t, k).wait_send()

    @pl.when(core == 1)
    def _():
        for t, k in ORDER:
            for q in range(2):
                into(t, k, q).wait_recv()


def nothing_kernel(packed, land):
    pass


def more(packed, *, extra):
    shape = jax.ShapeDtypeStruct((2, 4, 2) + packed.shape[2:], packed.dtype)
    if not extra:
        return pl.pallas_call(nothing_kernel, out_shape=shape, in_specs=[HBM], out_specs=HBM, compiler_params=pltpu.CompilerParams(vmem_limit_bytes=60 * 2**20), name='more_0')(packed)
    dma = pltpu.SemaphoreType.DMA
    return pl.pallas_call(
        functools.partial(more_kernel, extra=extra),
        out_shape=shape,
        in_specs=[HBM],
        out_specs=HBM,
        scratch_shapes=[dma((2, 3)), dma((2, 3, 2))],
        compiler_params=pltpu.CompilerParams(has_side_effects=True, vmem_limit_bytes=60 * 2**20),
        name=f'more_{extra}',
    )(packed)


def base_kernel(packed, k_ref, v_ref, res_ref, gain_ref, wq_ref, wk_ref, wv_ref, wout_ref, _, land, proj_ref, *rest):
    held_refs, (normed, total, ring, ring_sem, held_sem, send_sem, recv_sem, fsend_sem, frecv_sem, ssend_sem, srecv_sem) = rest[:PARTS], rest[PARTS:]
    me = lax.axis_index('sh')
    core = me % 2
    chip = me // 2
    partner = me + 1 - 2 * core
    peers = [chip + 1 - 2 * (chip % 2), (chip + 2) % 4, 3 - chip]

    size = HALF // PIECES

    def main(t, k, half, p):
        rows = pl.ds(half * HALF + p * size, size)
        return remote(packed.at[t, k, rows], land.at[t, k, core, rows], send_sem.at[t, k, half, p], recv_sem.at[t, k, core, p], 2 * peers[k] + half)

    def forward(t, k, q, p):
        rows = land.at[t, k, q, pl.ds(core * HALF + p * size, size)]
        return remote(rows, rows, fsend_sem.at[t, k, q, p], frecv_sem.at[t, k, q, p], partner)

    def main_in(t, k, q, p):
        rows = land.at[t, k, q, pl.ds(core * HALF + p * size, size)]
        return remote(rows, rows, fsend_sem.at[t, k, q, p], recv_sem.at[t, k, q, p], partner)

    def forward_in(t, k, q, p):
        rows = land.at[t, k, q, pl.ds((1 - core) * HALF + p * size, size)]
        return remote(rows, rows, fsend_sem.at[t, k, q, p], frecv_sem.at[t, k, q, p], partner)

    def across(t):
        return remote((k_ref, v_ref)[t].at[partner], land.at[t, 3, core, pl.ds(0, k_ref.shape[1])], ssend_sem.at[t], srecv_sem.at[t], partner)

    def across_in(t):
        rows = land.at[t, 3, 1 - core, pl.ds(0, k_ref.shape[1])]
        return remote(rows, rows, ssend_sem.at[t], srecv_sem.at[t], partner)

    for t, k in ORDER:
        for half in range(2):
            for p in range(PIECES):
                main(t, k, half, p).start()
    for t in range(2):
        across(t).start()
    project(res_ref, gain_ref, (wq_ref, wk_ref, wv_ref), proj_ref, normed, total, ring, ring_sem)
    slabs, part, slab = held_refs[0].shape

    def hold(c, carry):
        for i in range(PARTS):
            pltpu.make_async_copy(wout_ref.at[pl.ds(i * part, part), pl.ds(pl.multiple_of(c * slab, slab), slab)], held_refs[i].at[c], held_sem.at[i]).start()
        return carry
    lax.fori_loop(0, slabs, hold, 0)
    for t, k in ORDER:
        for p in range(PIECES):
            for q in range(2):
                main_in(t, k, q, p).wait_recv()
                forward(t, k, q, p).start()
    for t in range(2):
        across(t).wait_send()
        across_in(t).wait_recv()
    for t, k in ORDER:
        for half in range(2):
            for p in range(PIECES):
                main(t, k, half, p).wait_send()
    for t, k in ORDER:
        for q in range(2):
            for p in range(PIECES):
                forward(t, k, q, p).wait_send()
                forward_in(t, k, q, p).wait_recv()
    for i in range(PARTS):
        pltpu.make_async_copy(held_refs[i], held_refs[i], held_sem.at[i]).wait()


def base(packed, k_rows, v_rows, residual, gain, w_query, w_key, w_value, w_out, land):
    dtype = k_rows.dtype
    dma = pltpu.SemaphoreType.DMA
    model_dim = residual.shape[1]
    proj_dim = w_query.shape[1] + w_key.shape[1] + w_value.shape[1]
    return pl.pallas_call(
        base_kernel,
        out_shape=(jax.ShapeDtypeStruct(land.shape, dtype), jax.ShapeDtypeStruct((LANES, proj_dim), dtype), )+ PARTS * (jax.ShapeDtypeStruct((w_out.shape[1] // SLAB, w_out.shape[0] // PARTS, SLAB), dtype),),
        in_specs=[HBM, HBM, HBM, VMEM, VMEM, HBM, HBM, HBM, HBM, HBM],
        out_specs=(HBM, VMEM) + PARTS * (ANY,),
        scratch_shapes=[
            pltpu.VMEM((LANES, model_dim), dtype), pltpu.VMEM((LANES, proj_dim), jnp.float32), pltpu.VMEM((8, 512, 512), dtype), dma((8,)), dma((PARTS,)),
            dma((2, 3, 2, PIECES)), dma((2, 3, 2, PIECES)), dma((2, 3, 2, PIECES)), dma((2, 3, 2, PIECES)), dma((2,)), dma((2,)),
        ],
        input_output_aliases={9: 0},
        compiler_params=pltpu.CompilerParams(has_side_effects=True, vmem_limit_bytes=BASE_VMEM),
        name='base',
    )(packed, k_rows, v_rows, residual, gain, w_query, w_key, w_value, w_out, land)


def build_kernel(len_ref, proj_ref, freq_ref, res_ref, *rest, depth):
    w_refs, (k_ref, v_ref, land, kc_ref, vc_ref, xout_ref, ring, tail, wide, made, scores, probs, mixed, ovec, q_ref, knew_ref, vnew_ref, ring_sem, tail_sem, made_sem) = rest[:PARTS], rest[PARTS:]
    step = pl.program_id(0)
    steps = WINDOW // STEP
    me = lax.axis_index('sh')
    core, chip, n = me % 2, me // 2, len_ref[me]
    offset = core * span(len_ref[2 * chip])
    chips = [chip, chip + 1 - 2 * (chip % 2), (chip + 2) % 4, 3 - chip]
    extra = tail.shape[2]
    heads = tail.shape[1]
    head_dim = tail.shape[3]

    def copies(t, start, size, dst, sem):
        own = 2 * chip + core
        other = 2 * chip + 1 - core
        rows = pl.ds(start, size)
        yield pltpu.make_async_copy((k_ref, v_ref)[t].at[me, rows], dst.at[own], sem)
        yield pltpu.make_async_copy(land.at[t, 3, 1 - core, rows], dst.at[other], sem)
        far = pl.ds(pl.multiple_of(offset + start, ALIGN), size)
        for k in range(3):
            for q in range(2):
                yield pltpu.make_async_copy(land.at[t, k, q, far], dst.at[2 * chips[k + 1] + q], sem)

    def heads_of_row():
        q_width = ovec.shape[1]
        group = q_width // (heads * head_dim)

        def part(at):
            return proj_ref[:1, at:at + head_dim]

        angles = n.astype(jnp.float32) * freq_ref[...]
        lane = lax.broadcasted_iota(jnp.int32, angles.shape, 1)
        cos, sin = jnp.cos(angles), jnp.sin(angles)
        sin = jnp.where(lane < head_dim // 2, -sin, sin)

        def turned(at):
            vals = part(at).astype(jnp.float32)
            return (vals * cos + pltpu.roll(vals, head_dim // 2, 1) * sin).astype(q_ref.dtype)

        for pair in range(heads // 2):
            for half in range(2):
                h = 2 * pair + half
                rows = jnp.concatenate([turned((h * group + g) * head_dim) for g in range(group)] + [jnp.zeros((8 - group, head_dim), q_ref.dtype)], axis=0)
                none = jnp.zeros_like(rows)
                q_ref[pair, 8 * half:8 * half + 8, :] = jnp.concatenate([rows, none] if half == 0 else [none, rows], axis=1)
        knew_ref[...] = jnp.concatenate([turned(q_width + h * head_dim) for h in range(heads)], axis=0)
        vnew_ref[...] = jnp.concatenate([part(q_width + (heads + h) * head_dim) for h in range(heads)], axis=0)

    def chunk(s, then):
        for t in range(2):
            local = s - t * steps
            pl.when((local >= 0) & (local < steps) & (local * STEP < n))(functools.partial(then, t, local))

    def fetch(s):
        def then(t, local):
            for copy in copies(t, pl.multiple_of(local * STEP, STEP), STEP, ring.at[s % depth], ring_sem.at[s % depth]):
                copy.start()
        chunk(s, then)

    def arrived(s):
        def then(t, local):
            whole = ring.at[s % depth]
            pltpu.make_async_copy(whole, whole, ring_sem.at[s % depth]).wait()
        chunk(s, then)

    def fetch_tail(t):
        @pl.when(n > WINDOW)
        def _():
            for copy in copies(t, WINDOW, extra, tail.at[t], tail_sem.at[t]):
                copy.start()

    def save(b, out_ref, local):
        size = BLOCK * heads // SAVES
        for i in range(SAVES):
            at = b * BLOCK * heads + i * size
            here = pl.ds(pl.multiple_of(at, size), size)
            there = pl.ds(pl.multiple_of(local * STEP * heads + at, size), size)
            pltpu.make_async_copy(made.at[step % MADE, here], out_ref.at[there], made_sem.at[step % MADE]).start(priority=1)

    def saved(s):
        whole = made.at[s % MADE]
        pltpu.make_async_copy(whole, whole, made_sem.at[s % MADE]).wait()

    @pl.when(step == 0)
    def _():
        def ahead(s, carry):
            fetch(s)
            return carry
        fetch(jnp.int32(0))
        fetch_tail(0)
        lax.fori_loop(1, depth - 1, ahead, 0)
        fetch_tail(1)
        mixed[...] = jnp.zeros_like(mixed)
        heads_of_row()
    fetch(step + depth - 1)
    arrived(step)

    @pl.when(step >= MADE)
    def _():
        saved(step)

    def assemble(t, local, new_ref, out_ref, use):
        first = local * STEP
        newest = lax.rem(n, WINDOW)
        wraps = (local == 0) & (n > WINDOW)
        dead = first > n
        plain = (first + STEP <= n) & ~wraps & ((newest < first) | (newest >= first + STEP))
        slot = step % depth
        out = step % MADE

        @pl.when(wraps)
        def _():
            whole = tail.at[t]
            pltpu.make_async_copy(whole, whole, tail_sem.at[t]).wait()

        @pl.when(~plain & ~dead)
        def _():
            def patch(c, carry):
                low = first + c * extra
                rows = pl.ds(pl.multiple_of(c * extra, extra), extra)

                @pl.when((low < n - WINDOW) | (low + extra > n) | ((newest >= low) & (newest < low + extra)))
                def _():
                    pos = low + lax.broadcasted_iota(jnp.int32, (extra, head_dim), 0)
                    for h in range(heads):
                        vals = jnp.where(pos < n - WINDOW, tail[t, h], ring[slot, h, rows, :])
                        vals = jnp.where(pos < n, vals, jnp.zeros_like(vals))
                        ring[slot, h, rows, :] = jnp.where(pos == newest, jnp.broadcast_to(new_ref[h:h + 1, :], vals.shape), vals)
                return carry
            lax.fori_loop(0, STEP // extra, patch, 0)

        @pl.when(dead)
        def _():
            def clear(b, carry):
                made[out, pl.ds(pl.multiple_of(b * BLOCK * heads, BLOCK * heads), BLOCK * heads), :] = jnp.zeros((BLOCK * heads, head_dim), made.dtype)
                save(b, out_ref, local)
                return carry
            lax.fori_loop(0, STEP // BLOCK, clear, 0)
            use(None, None, None)

        @pl.when(~dead)
        def _():
            def mix(b, carry):
                for pair in range(heads // 2):
                    both = []
                    for h in (2 * pair, 2 * pair + 1):
                        vals = ring[slot, h, pl.ds(pl.multiple_of(b * BLOCK, BLOCK), BLOCK), :]
                        wide[pl.ds(h, BLOCK, stride=PITCH), :] = vals.astype(jnp.float32)
                        both.append(vals)
                    use(pair, b, jnp.concatenate(both, axis=1))
                rows = jnp.concatenate([wide[PITCH * p:PITCH * p + heads, :] for p in range(BLOCK)], axis=0)
                made[out, pl.ds(pl.multiple_of(b * BLOCK * heads, BLOCK * heads), BLOCK * heads), :] = rows.astype(made.dtype)
                save(b, out_ref, local)
                return carry
            lax.fori_loop(0, STEP // BLOCK, mix, 0)

    def slots_of(local, b, size):
        return pl.ds(pl.multiple_of(local * STEP + b * BLOCK, BLOCK), size)

    @pl.when(step < steps)
    def _():
        def use(pair, b, vals):
            if pair is None:
                scores[:, slots_of(step, 0, STEP)] = jnp.full((scores.shape[0], STEP), -jnp.inf)
                return
            slots = step * STEP + b * BLOCK + lax.broadcasted_iota(jnp.int32, (16, BLOCK), 1)
            live = (slots <= n) | (n >= WINDOW)
            s = lax.dot_general(q_ref[pair], vals, (((1,), (1,)), ((), ())), preferred_element_type=jnp.float32) / head_dim ** 0.5
            scores[pl.ds(16 * pair, 16), slots_of(step, b, BLOCK)] = jnp.where(live, s, -jnp.inf)
        assemble(0, step, knew_ref, kc_ref, use)

    @pl.when(step == steps)
    def _():
        for pair in range(heads // 2):
            s = scores[16 * pair:16 * pair + 16, :]
            e = jnp.exp(s - jnp.max(s, axis=-1, keepdims=True))
            probs[pair] = (e / jnp.sum(e, axis=-1, keepdims=True)).astype(probs.dtype)

    @pl.when(step >= steps)
    def _():
        local = step - steps

        def use(pair, b, vals):
            if pair is None:
                return
            mix = jnp.dot(probs[pair, :, slots_of(local, b, BLOCK)], vals, preferred_element_type=jnp.float32)
            mixed[2 * pair] += mix[:8, :head_dim]
            mixed[2 * pair + 1] += mix[8:, head_dim:]
        assemble(1, local, vnew_ref, vc_ref, use)

    @pl.when(step == 2 * steps - 1)
    def _():
        group = ovec.shape[1] // (heads * head_dim)
        for h in range(heads):
            o = mixed[h].astype(ovec.dtype)
            for g in range(group):
                cols = pl.ds((h * group + g) * head_dim, head_dim)
                ovec[:, cols] = jnp.broadcast_to(o[g:g + 1], (ovec.shape[0], head_dim))
        slabs, part, slab = w_refs[0].shape
        width = GROUP * slab

        def column(c, carry):
            acc = jnp.zeros((ovec.shape[0], width), jnp.float32)
            for i, w_ref in enumerate(w_refs):
                block = jnp.concatenate([w_ref[c * GROUP + j] for j in range(GROUP)], axis=1)
                acc += jnp.dot(ovec[:, i * part:(i + 1) * part], block, preferred_element_type=jnp.float32)
            cols = pl.ds(pl.multiple_of(c * width, width), width)
            xout_ref[:, cols] = (res_ref[:, cols].astype(jnp.float32) + acc[:1]).astype(xout_ref.dtype)
            return carry
        lax.fori_loop(0, slabs // GROUP, column, 0)
        for s in range(2 * steps - MADE, 2 * steps):
            saved(s)


def build(lengths, proj, freq, residual, w_out, k_rows, v_rows, land, heads):
    seq_len, head_dim = k_rows.shape[1:]
    steps = WINDOW // STEP
    depth = DEPTH
    dtype = k_rows.dtype
    cache = jax.ShapeDtypeStruct((WINDOW * heads, head_dim), dtype)
    dma = pltpu.SemaphoreType.DMA
    return pl.pallas_call(
        functools.partial(build_kernel, depth=depth),
        grid=(2 * steps,),
        out_shape=(cache, cache, jax.ShapeDtypeStruct(residual.shape, dtype)),
        in_specs=[SMEM, VMEM, VMEM, VMEM] + PARTS * [VMEM] + [HBM, HBM, HBM],
        out_specs=(HBM, HBM, VMEM),
        scratch_shapes=[
            pltpu.VMEM((depth, heads, STEP, head_dim), dtype),
            pltpu.VMEM((2, heads, seq_len - WINDOW, head_dim), dtype),
            pltpu.VMEM((BLOCK * PITCH, head_dim), jnp.float32),
            pltpu.VMEM((MADE, STEP * heads, head_dim), dtype),
            pltpu.VMEM((8 * heads, WINDOW), jnp.float32),
            pltpu.VMEM((heads // 2, 16, WINDOW), dtype),
            pltpu.VMEM((heads, 8, head_dim), jnp.float32),
            pltpu.VMEM((LANES, PARTS * w_out[0].shape[1]), dtype),
            pltpu.VMEM((heads // 2, 16, 2 * head_dim), dtype),
            pltpu.VMEM((heads, head_dim), dtype),
            pltpu.VMEM((heads, head_dim), dtype),
            dma((depth,)), dma((2,)), dma((MADE,)),
        ],
        compiler_params=pltpu.CompilerParams(vmem_limit_bytes=BUILD_VMEM),
        name='build',
    )(lengths, proj, freq, residual, *w_out, k_rows, v_rows, land)


def frequencies(head_dim):
    half = THETA ** (-2.0 * np.arange(head_dim // 2, dtype=np.float64) / head_dim)
    return np.concatenate([half, half])[None].astype(np.float32)


def solution(mesh):
    head_spec = P('dp', None, 'sh', None)
    row_spec = P(('dp', 'sh'))
    full_spec = P(None, None)

    def per_device(k_prefill, v_prefill, lengths, residual, norm_gain, w_query, w_key, w_value, w_out):
        num_rows, seq_len, _, head_dim = k_prefill.shape
        kv_heads = w_key.shape[1] // head_dim
        k_rows = k_prefill.reshape(num_rows, seq_len, head_dim)
        v_rows = v_prefill.reshape(num_rows, seq_len, head_dim)
        packed, size = pack(lengths, k_rows, v_rows)
        sizes = (list_length(seq_len) - BASE) // QUANTUM
        land = lax.switch(size[0], [functools.partial(more, extra=i * QUANTUM) for i in range(sizes + 1)], packed)
        land, proj, *held = base(packed, k_rows, v_rows, residual, norm_gain.reshape(-1, head_dim), w_query, w_key, w_value, w_out, land)
        k_cache, v_cache, resid_out = build(lengths, proj, jnp.asarray(frequencies(head_dim)), residual, held, k_rows, v_rows, land, kv_heads)
        shape = (1, WINDOW, kv_heads, head_dim)
        return resid_out, k_cache.reshape(shape), v_cache.reshape(shape)
    return jax.shard_map(per_device, mesh=mesh, in_specs=(head_spec, head_spec, P('dp'), P(('dp', 'sh'), None), P(None), full_spec, full_spec, full_spec, full_spec), out_specs=(P(('dp', 'sh'), None), row_spec, row_spec), check_vma=False)
```

```python
import functools

import jax
import jax.numpy as jnp
import numpy as np
from jax import lax
from jax.experimental import pallas as pl
from jax.experimental.pallas import tpu as pltpu
from jax.sharding import PartitionSpec as P

WINDOW = 4096
THETA = 10000.0
EPS = 1e-5
ALIGN = 16
HALF = 2208
BASE = 2 * HALF
CUTS = 4
PIECES = 2
QUANTUM = 128
STEP = 512
SLAB = 128
GROUP = 16
ON_MXU = 6
DEPTH = 8
MADE = 4
SAVES = 4
BLOCK = 256
PITCH = 9
PARTS = 4
BASE_VMEM = 14 * 2**20
BUILD_VMEM = 19 * 2**20
LANES = 16
ORDER = [(t, k) for k in range(3) for t in range(2)]
ANY = pl.BlockSpec(memory_space=pl.ANY)
VMEM = pl.BlockSpec(memory_space=pltpu.VMEM)
SMEM = pl.BlockSpec(memory_space=pltpu.SMEM)
HBM = pl.BlockSpec(memory_space=pltpu.HBM)


def list_length(seq_len):
    return BASE + -(-(2 * seq_len - BASE) // QUANTUM) * QUANTUM


def span(length):
    return (length + (ALIGN - 1)) // ALIGN * ALIGN


def pack_kernel(len_ref, k_ref, v_ref, out_ref, size_ref, lists, first_sem, second_sem, store_sem, *, seq_len):
    chip = lax.axis_index('sh') // 2
    list_len = lists.shape[2]
    peers = [chip + 1 - 2 * (chip % 2), (chip + 2) % 4, 3 - chip]

    part = seq_len // CUTS

    def spans_of(k):
        return span(len_ref[2 * peers[k]]), span(len_ref[2 * peers[k] + 1])

    def loads(t, k, second):
        src = (k_ref, v_ref)[t]
        spans = spans_of(k)
        for i in range(CUTS):
            start = pl.multiple_of(second * spans[0] + i * part, ALIGN)
            yield spans[second] > i * part, pltpu.make_async_copy(src.at[2 * peers[k] + second, pl.ds(i * part, part)], lists.at[t, k, pl.ds(start, part)], (first_sem, second_sem)[second].at[t, k, i])

    def stores(t, k):
        size = list_len // (2 * CUTS)
        for i in range(2 * CUTS):
            rows = pl.ds(i * size, size)
            yield sum(spans_of(k)) > i * size, pltpu.make_async_copy(lists.at[t, k, rows], out_ref.at[t, k, rows], store_sem.at[t, k, i])

    def start(copies):
        for live, copy in copies:
            pl.when(live)(copy.start)

    def wait(copies):
        for live, copy in copies:
            pl.when(live)(copy.wait)

    for t, k in ORDER:
        start(loads(t, k, 0))
    longest = span(len_ref[0]) + span(len_ref[1])
    for c in range(1, len_ref.shape[0] // 2):
        longest = jnp.maximum(longest, span(len_ref[2 * c]) + span(len_ref[2 * c + 1]))
    size_ref[0] = jnp.clip((longest - BASE + QUANTUM - 1) // QUANTUM, 0, (list_len - BASE) // QUANTUM)
    for t, k in ORDER:
        wait(loads(t, k, 0))
        start(loads(t, k, 1))
    for t, k in ORDER:
        wait(loads(t, k, 1))
        start(stores(t, k))
    for t, k in ORDER:
        wait(stores(t, k))


def pack(lengths, k_rows, v_rows):
    seq_len, head_dim = k_rows.shape[1:]
    shape = (2, 3, list_length(seq_len), head_dim)
    return pl.pallas_call(
        functools.partial(pack_kernel, seq_len=seq_len),
        out_shape=(jax.ShapeDtypeStruct(shape, k_rows.dtype), jax.ShapeDtypeStruct((1,), jnp.int32)),
        in_specs=[SMEM, HBM, HBM],
        out_specs=(HBM, SMEM),
        scratch_shapes=[pltpu.VMEM(shape, k_rows.dtype), pltpu.SemaphoreType.DMA((2, 3, CUTS)), pltpu.SemaphoreType.DMA((2, 3, CUTS)), pltpu.SemaphoreType.DMA((2, 3, 2 * CUTS))],
        compiler_params=pltpu.CompilerParams(vmem_limit_bytes=60 * 2**20),
        name='pack',
    )(lengths, k_rows, v_rows)


def project(res_ref, gain_ref, weights, proj_ref, normed, total, ring, ring_sem):
    depth, side, _ = ring.shape
    resid = res_ref[...].astype(jnp.float32)
    inv_rms = lax.rsqrt(jnp.sum(resid * resid, axis=-1, keepdims=True) / resid.shape[-1] + EPS)
    lanes = gain_ref.shape[1]
    for r in range(gain_ref.shape[0]):
        cols = slice(r * lanes, (r + 1) * lanes)
        row = (resid[:, cols] * inv_rms * gain_ref[r:r + 1, :].astype(jnp.float32)).astype(normed.dtype)
        normed[:, cols] = jnp.broadcast_to(row, (normed.shape[0], lanes))
    total[...] = jnp.zeros_like(total)
    deep = normed.shape[1] // side

    def at(i):
        return pl.multiple_of(i // deep * side, side), pl.multiple_of(i % deep * side, side)

    def fetch(i):
        left, top = at(i)
        first = 0
        for w_ref in weights:
            width = w_ref.shape[1]

            @pl.when((left >= first) & (left < first + width))
            def _(w_ref=w_ref, first=first):
                here = pl.multiple_of(left - first, side)
                pltpu.make_async_copy(w_ref.at[pl.ds(top, side), pl.ds(here, side)], ring.at[i % depth], ring_sem.at[i % depth]).start()
            first += width

    blocks = total.shape[1] // side * deep

    def prime(i, carry):
        fetch(i)
        return carry
    lax.fori_loop(0, depth - 1, prime, 0)

    def step(i, carry):
        @pl.when(i + depth - 1 < blocks)
        def _():
            fetch(i + depth - 1)
        pltpu.make_async_copy(weights[0].at[pl.ds(0, side), pl.ds(0, side)], ring.at[i % depth], ring_sem.at[i % depth]).wait()
        left, top = at(i)
        total[:, pl.ds(left, side)] += jnp.dot(normed[:, pl.ds(top, side)], ring[i % depth], preferred_element_type=jnp.float32)
        return carry
    lax.fori_loop(0, blocks, step, 0)
    proj_ref[...] = total[...].astype(proj_ref.dtype)


def remote(src, dst, send, recv, device):
    return pltpu.make_async_remote_copy(src_ref=src, dst_ref=dst, send_sem=send, recv_sem=recv, device_id={'sh': device}, device_id_type=pl.DeviceIdType.MESH)


def more_kernel(packed, land, send_sem, recv_sem, *, extra):
    me = lax.axis_index('sh')
    core = me % 2
    chip = me // 2
    peers = [chip + 1 - 2 * (chip % 2), (chip + 2) % 4, 3 - chip]
    rows = pl.ds(BASE, extra)

    def out(t, k):
        return remote(packed.at[t, k, rows], land.at[t, k, core, rows], send_sem.at[t, k], recv_sem.at[t, k, core], 2 * peers[k] + 1)

    def into(t, k, q):
        here = land.at[t, k, q, rows]
        return remote(here, here, send_sem.at[t, k], recv_sem.at[t, k, q], me)

    for t, k in ORDER:
        out(t, k).start()
    for t, k in ORDER:
        out(t, k).wait_send()

    @pl.when(core == 1)
    def _():
        for t, k in ORDER:
            for q in range(2):
                into(t, k, q).wait_recv()


def nothing_kernel(packed, land):
    pass


def more(packed, *, extra):
    shape = jax.ShapeDtypeStruct((2, 4, 2) + packed.shape[2:], packed.dtype)
    if not extra:
        return pl.pallas_call(nothing_kernel, out_shape=shape, in_specs=[HBM], out_specs=HBM, compiler_params=pltpu.CompilerParams(vmem_limit_bytes=60 * 2**20), name='more_0')(packed)
    dma = pltpu.SemaphoreType.DMA
    return pl.pallas_call(
        functools.partial(more_kernel, extra=extra),
        out_shape=shape,
        in_specs=[HBM],
        out_specs=HBM,
        scratch_shapes=[dma((2, 3)), dma((2, 3, 2))],
        compiler_params=pltpu.CompilerParams(has_side_effects=True, vmem_limit_bytes=60 * 2**20),
        name=f'more_{extra}',
    )(packed)


def base_kernel(packed, k_ref, v_ref, res_ref, gain_ref, wq_ref, wk_ref, wv_ref, wout_ref, _, land, proj_ref, *rest):
    held_refs, (normed, total, ring, ring_sem, held_sem, send_sem, recv_sem, fsend_sem, frecv_sem, ssend_sem, srecv_sem) = rest[:PARTS], rest[PARTS:]
    me = lax.axis_index('sh')
    core = me % 2
    chip = me // 2
    partner = me + 1 - 2 * core
    peers = [chip + 1 - 2 * (chip % 2), (chip + 2) % 4, 3 - chip]

    size = HALF // PIECES

    def main(t, k, half, p):
        rows = pl.ds(half * HALF + p * size, size)
        return remote(packed.at[t, k, rows], land.at[t, k, core, rows], send_sem.at[t, k, half, p], recv_sem.at[t, k, core, p], 2 * peers[k] + half)

    def forward(t, k, q, p):
        rows = land.at[t, k, q, pl.ds(core * HALF + p * size, size)]
        return remote(rows, rows, fsend_sem.at[t, k, q, p], frecv_sem.at[t, k, q, p], partner)

    def main_in(t, k, q, p):
        rows = land.at[t, k, q, pl.ds(core * HALF + p * size, size)]
        return remote(rows, rows, fsend_sem.at[t, k, q, p], recv_sem.at[t, k, q, p], partner)

    def forward_in(t, k, q, p):
        rows = land.at[t, k, q, pl.ds((1 - core) * HALF + p * size, size)]
        return remote(rows, rows, fsend_sem.at[t, k, q, p], frecv_sem.at[t, k, q, p], partner)

    def across(t):
        return remote((k_ref, v_ref)[t].at[partner], land.at[t, 3, core, pl.ds(0, k_ref.shape[1])], ssend_sem.at[t], srecv_sem.at[t], partner)

    def across_in(t):
        rows = land.at[t, 3, 1 - core, pl.ds(0, k_ref.shape[1])]
        return remote(rows, rows, ssend_sem.at[t], srecv_sem.at[t], partner)

    for t, k in ORDER:
        for half in range(2):
            for p in range(PIECES):
                main(t, k, half, p).start()
    for t in range(2):
        across(t).start()
    project(res_ref, gain_ref, (wq_ref, wk_ref, wv_ref), proj_ref, normed, total, ring, ring_sem)
    slabs, part, slab = held_refs[0].shape

    def hold(c, carry):
        for i in range(PARTS):
            pltpu.make_async_copy(wout_ref.at[pl.ds(i * part, part), pl.ds(pl.multiple_of(c * slab, slab), slab)], held_refs[i].at[c], held_sem.at[i]).start()
        return carry
    lax.fori_loop(0, slabs, hold, 0)
    for t, k in ORDER:
        for p in range(PIECES):
            for q in range(2):
                main_in(t, k, q, p).wait_recv()
                forward(t, k, q, p).start()
    for t in range(2):
        across(t).wait_send()
        across_in(t).wait_recv()
    for t, k in ORDER:
        for half in range(2):
            for p in range(PIECES):
                main(t, k, half, p).wait_send()
    for t, k in ORDER:
        for q in range(2):
            for p in range(PIECES):
                forward(t, k, q, p).wait_send()
                forward_in(t, k, q, p).wait_recv()
    for i in range(PARTS):
        pltpu.make_async_copy(held_refs[i], held_refs[i], held_sem.at[i]).wait()


def base(packed, k_rows, v_rows, residual, gain, w_query, w_key, w_value, w_out, land):
    dtype = k_rows.dtype
    dma = pltpu.SemaphoreType.DMA
    model_dim = residual.shape[1]
    proj_dim = w_query.shape[1] + w_key.shape[1] + w_value.shape[1]
    return pl.pallas_call(
        base_kernel,
        out_shape=(jax.ShapeDtypeStruct(land.shape, dtype), jax.ShapeDtypeStruct((LANES, proj_dim), dtype), )+ PARTS * (jax.ShapeDtypeStruct((w_out.shape[1] // SLAB, w_out.shape[0] // PARTS, SLAB), dtype),),
        in_specs=[HBM, HBM, HBM, VMEM, VMEM, HBM, HBM, HBM, HBM, HBM],
        out_specs=(HBM, VMEM) + PARTS * (ANY,),
        scratch_shapes=[
            pltpu.VMEM((LANES, model_dim), dtype), pltpu.VMEM((LANES, proj_dim), jnp.float32), pltpu.VMEM((8, 512, 512), dtype), dma((8,)), dma((PARTS,)),
            dma((2, 3, 2, PIECES)), dma((2, 3, 2, PIECES)), dma((2, 3, 2, PIECES)), dma((2, 3, 2, PIECES)), dma((2,)), dma((2,)),
        ],
        input_output_aliases={9: 0},
        compiler_params=pltpu.CompilerParams(has_side_effects=True, vmem_limit_bytes=BASE_VMEM),
        name='base',
    )(packed, k_rows, v_rows, residual, gain, w_query, w_key, w_value, w_out, land)


def build_kernel(len_ref, proj_ref, freq_ref, res_ref, *rest, depth):
    w_refs, (k_ref, v_ref, land, kc_ref, vc_ref, xout_ref, ring, tail, wide, made, scores, probs, mixed, ovec, ostack, spread, q_ref, knew_ref, vnew_ref, ring_sem, tail_sem, made_sem) = rest[:PARTS], rest[PARTS:]
    step = pl.program_id(0)
    steps = WINDOW // STEP
    me = lax.axis_index('sh')
    core, chip, n = me % 2, me // 2, len_ref[me]
    offset = core * span(len_ref[2 * chip])
    chips = [chip, chip + 1 - 2 * (chip % 2), (chip + 2) % 4, 3 - chip]
    extra = tail.shape[2]
    heads = tail.shape[1]
    head_dim = tail.shape[3]

    def copies(t, start, size, dst, sem):
        own = 2 * chip + core
        other = 2 * chip + 1 - core
        rows = pl.ds(start, size)
        yield pltpu.make_async_copy((k_ref, v_ref)[t].at[me, rows], dst.at[own], sem)
        yield pltpu.make_async_copy(land.at[t, 3, 1 - core, rows], dst.at[other], sem)
        far = pl.ds(pl.multiple_of(offset + start, ALIGN), size)
        for k in range(3):
            for q in range(2):
                yield pltpu.make_async_copy(land.at[t, k, q, far], dst.at[2 * chips[k + 1] + q], sem)

    def heads_of_row():
        q_width = ovec.shape[1]
        group = q_width // (heads * head_dim)

        def part(at):
            return proj_ref[:1, at:at + head_dim]

        angles = n.astype(jnp.float32) * freq_ref[...]
        lane = lax.broadcasted_iota(jnp.int32, angles.shape, 1)
        cos, sin = jnp.cos(angles), jnp.sin(angles)
        sin = jnp.where(lane < head_dim // 2, -sin, sin)

        def turned(at):
            vals = part(at).astype(jnp.float32)
            return (vals * cos + pltpu.roll(vals, head_dim // 2, 1) * sin).astype(q_ref.dtype)

        for pair in range(heads // 2):
            for half in range(2):
                h = 2 * pair + half
                rows = jnp.concatenate([turned((h * group + g) * head_dim) for g in range(group)] + [jnp.zeros((8 - group, head_dim), q_ref.dtype)], axis=0)
                none = jnp.zeros_like(rows)
                q_ref[pair, 8 * half:8 * half + 8, :] = jnp.concatenate([rows, none] if half == 0 else [none, rows], axis=1)
        knew_ref[...] = jnp.concatenate([turned(q_width + h * head_dim) for h in range(heads)], axis=0)
        vnew_ref[...] = jnp.concatenate([part(q_width + (heads + h) * head_dim) for h in range(heads)], axis=0)

    def chunk(s, then):
        for t in range(2):
            local = s - t * steps
            pl.when((local >= 0) & (local < steps) & (local * STEP < n))(functools.partial(then, t, local))

    def fetch(s):
        def then(t, local):
            for copy in copies(t, pl.multiple_of(local * STEP, STEP), STEP, ring.at[s % depth], ring_sem.at[s % depth]):
                copy.start()
        chunk(s, then)

    def arrived(s):
        def then(t, local):
            whole = ring.at[s % depth]
            pltpu.make_async_copy(whole, whole, ring_sem.at[s % depth]).wait()
        chunk(s, then)

    def fetch_tail(t):
        @pl.when(n > WINDOW)
        def _():
            for copy in copies(t, WINDOW, extra, tail.at[t], tail_sem.at[t]):
                copy.start()

    def save(b, out_ref, local):
        size = BLOCK * heads // SAVES
        for i in range(SAVES):
            at = b * BLOCK * heads + i * size
            here = pl.ds(pl.multiple_of(at, size), size)
            there = pl.ds(pl.multiple_of(local * STEP * heads + at, size), size)
            pltpu.make_async_copy(made.at[step % MADE, here], out_ref.at[there], made_sem.at[step % MADE]).start(priority=1)

    def saved(s):
        whole = made.at[s % MADE]
        pltpu.make_async_copy(whole, whole, made_sem.at[s % MADE]).wait()

    @pl.when(step == 0)
    def _():
        def ahead(s, carry):
            fetch(s)
            return carry
        fetch(jnp.int32(0))
        fetch_tail(0)
        lax.fori_loop(1, depth - 1, ahead, 0)
        fetch_tail(1)
        mixed[...] = jnp.zeros_like(mixed)
        heads_of_row()
    fetch(step + depth - 1)
    arrived(step)

    @pl.when(step >= MADE)
    def _():
        saved(step)

    def assemble(t, local, new_ref, out_ref, use):
        first = local * STEP
        newest = lax.rem(n, WINDOW)
        wraps = (local == 0) & (n > WINDOW)
        dead = first > n
        plain = (first + STEP <= n) & ~wraps & ((newest < first) | (newest >= first + STEP))
        slot = step % depth
        out = step % MADE

        @pl.when(wraps)
        def _():
            whole = tail.at[t]
            pltpu.make_async_copy(whole, whole, tail_sem.at[t]).wait()

        @pl.when(~plain & ~dead)
        def _():
            def patch(c, carry):
                low = first + c * extra
                rows = pl.ds(pl.multiple_of(c * extra, extra), extra)

                @pl.when((low < n - WINDOW) | (low + extra > n) | ((newest >= low) & (newest < low + extra)))
                def _():
                    pos = low + lax.broadcasted_iota(jnp.int32, (extra, head_dim), 0)
                    for h in range(heads):
                        vals = jnp.where(pos < n - WINDOW, tail[t, h], ring[slot, h, rows, :])
                        vals = jnp.where(pos < n, vals, jnp.zeros_like(vals))
                        ring[slot, h, rows, :] = jnp.where(pos == newest, jnp.broadcast_to(new_ref[h:h + 1, :], vals.shape), vals)
                return carry
            lax.fori_loop(0, STEP // extra, patch, 0)

        @pl.when(dead)
        def _():
            def clear(b, carry):
                made[out, pl.ds(pl.multiple_of(b * BLOCK * heads, BLOCK * heads), BLOCK * heads), :] = jnp.zeros((BLOCK * heads, head_dim), made.dtype)
                save(b, out_ref, local)
                return carry
            lax.fori_loop(0, STEP // BLOCK, clear, 0)
            use(None, None, None)

        @pl.when(~dead)
        def _():
            def mix(b, carry):
                for pair in range(heads // 2):
                    both = []
                    for h in (2 * pair, 2 * pair + 1):
                        vals = ring[slot, h, pl.ds(pl.multiple_of(b * BLOCK, BLOCK), BLOCK), :]
                        wide[pl.ds(h, BLOCK, stride=PITCH), :] = vals.astype(jnp.float32)
                        both.append(vals)
                    use(pair, b, jnp.concatenate(both, axis=1))
                rows = jnp.concatenate([wide[PITCH * p:PITCH * p + heads, :] for p in range(BLOCK)], axis=0)
                made[out, pl.ds(pl.multiple_of(b * BLOCK * heads, BLOCK * heads), BLOCK * heads), :] = rows.astype(made.dtype)
                save(b, out_ref, local)
                return carry
            lax.fori_loop(0, STEP // BLOCK, mix, 0)

    def slots_of(local, b, size):
        return pl.ds(pl.multiple_of(local * STEP + b * BLOCK, BLOCK), size)

    @pl.when(step < steps)
    def _():
        def use(pair, b, vals):
            if pair is None:
                scores[:, slots_of(step, 0, STEP)] = jnp.full((scores.shape[0], STEP), -jnp.inf)
                return
            slots = step * STEP + b * BLOCK + lax.broadcasted_iota(jnp.int32, (16, BLOCK), 1)
            live = (slots <= n) | (n >= WINDOW)
            s = lax.dot_general(q_ref[pair], vals, (((1,), (1,)), ((), ())), preferred_element_type=jnp.float32) / head_dim ** 0.5
            scores[pl.ds(16 * pair, 16), slots_of(step, b, BLOCK)] = jnp.where(live, s, -jnp.inf)
        assemble(0, step, knew_ref, kc_ref, use)

    @pl.when(step == steps)
    def _():
        for pair in range(heads // 2):
            s = scores[16 * pair:16 * pair + 16, :]
            e = jnp.exp(s - jnp.max(s, axis=-1, keepdims=True))
            probs[pair] = (e / jnp.sum(e, axis=-1, keepdims=True)).astype(probs.dtype)

    @pl.when(step >= steps)
    def _():
        local = step - steps

        def use(pair, b, vals):
            if pair is None:
                return
            mix = jnp.dot(probs[pair, :, slots_of(local, b, BLOCK)], vals, preferred_element_type=jnp.float32)
            mixed[2 * pair] += mix[:8, :head_dim]
            mixed[2 * pair + 1] += mix[8:, head_dim:]
        assemble(1, local, vnew_ref, vc_ref, use)

    @pl.when(step == 2 * steps - 1)
    def _():
        group = ovec.shape[1] // (heads * head_dim)
        for h in range(heads):
            o = mixed[h].astype(ovec.dtype)
            for g in range(group):
                cols = pl.ds((h * group + g) * head_dim, head_dim)
                ovec[:, cols] = jnp.broadcast_to(o[g:g + 1], (ovec.shape[0], head_dim))
                ostack[h * group + g:h * group + g + 1, :] = o[g:g + 1]
        lane = lax.broadcasted_iota(jnp.int32, (LANES, LANES * head_dim), 1)
        row = lax.broadcasted_iota(jnp.int32, (LANES, LANES * head_dim), 0)
        pick = ((lane >= row * head_dim) & (lane < (row + 1) * head_dim)).astype(jnp.float32).astype(ostack.dtype)
        for i in range(ostack.shape[0] // LANES):
            cols = lax.dot_general(ostack[i * LANES:(i + 1) * LANES, :], pick, (((0,), (0,)), ((), ())), preferred_element_type=jnp.float32)
            for r in range(LANES):
                spread[pl.ds((i * LANES + r) * head_dim, head_dim), :] = cols[:, r * head_dim:(r + 1) * head_dim]
        slabs, part, slab = w_refs[0].shape

        def finish(at, vals):
            cols = pl.ds(pl.multiple_of(at * slab, slab), vals.shape[1])
            xout_ref[:, cols] = (res_ref[:, cols].astype(jnp.float32) + vals).astype(xout_ref.dtype)

        def column(c, carry):
            acc = jnp.zeros((ovec.shape[0], ON_MXU * slab), jnp.float32)
            for i, w_ref in enumerate(w_refs):
                block = jnp.concatenate([w_ref[c * GROUP + j] for j in range(ON_MXU)], axis=1)
                acc += jnp.dot(ovec[:, i * part:(i + 1) * part], block, preferred_element_type=jnp.float32)
            finish(c * GROUP, acc[:1])
            for j in range(ON_MXU, GROUP):
                total = jnp.zeros((8, slab), jnp.float32)
                for i, w_ref in enumerate(w_refs):
                    products = w_ref[c * GROUP + j].astype(jnp.float32) * spread[i * part:(i + 1) * part, :]
                    total += jnp.sum(products.reshape(part // 8, 8, slab), axis=0)
                finish(c * GROUP + j, jnp.sum(total, axis=0, keepdims=True))
            return carry
        lax.fori_loop(0, slabs // GROUP, column, 0)
        for s in range(2 * steps - MADE, 2 * steps):
            saved(s)


def build(lengths, proj, freq, residual, w_out, k_rows, v_rows, land, heads):
    seq_len, head_dim = k_rows.shape[1:]
    steps = WINDOW // STEP
    depth = DEPTH
    dtype = k_rows.dtype
    cache = jax.ShapeDtypeStruct((WINDOW * heads, head_dim), dtype)
    dma = pltpu.SemaphoreType.DMA
    return pl.pallas_call(
        functools.partial(build_kernel, depth=depth),
        grid=(2 * steps,),
        out_shape=(cache, cache, jax.ShapeDtypeStruct(residual.shape, dtype)),
        in_specs=[SMEM, VMEM, VMEM, VMEM] + PARTS * [VMEM] + [HBM, HBM, HBM],
        out_specs=(HBM, HBM, VMEM),
        scratch_shapes=[
            pltpu.VMEM((depth, heads, STEP, head_dim), dtype),
            pltpu.VMEM((2, heads, seq_len - WINDOW, head_dim), dtype),
            pltpu.VMEM((BLOCK * PITCH, head_dim), jnp.float32),
            pltpu.VMEM((MADE, STEP * heads, head_dim), dtype),
            pltpu.VMEM((8 * heads, WINDOW), jnp.float32),
            pltpu.VMEM((heads // 2, 16, WINDOW), dtype),
            pltpu.VMEM((heads, 8, head_dim), jnp.float32),
            pltpu.VMEM((LANES, PARTS * w_out[0].shape[1]), dtype),
            pltpu.VMEM((PARTS * w_out[0].shape[1] // head_dim, head_dim), dtype),
            pltpu.VMEM((PARTS * w_out[0].shape[1], head_dim), jnp.float32),
            pltpu.VMEM((heads // 2, 16, 2 * head_dim), dtype),
            pltpu.VMEM((heads, head_dim), dtype),
            pltpu.VMEM((heads, head_dim), dtype),
            dma((depth,)), dma((2,)), dma((MADE,)),
        ],
        compiler_params=pltpu.CompilerParams(vmem_limit_bytes=BUILD_VMEM),
        name='build',
    )(lengths, proj, freq, residual, *w_out, k_rows, v_rows, land)


def frequencies(head_dim):
    half = THETA ** (-2.0 * np.arange(head_dim // 2, dtype=np.float64) / head_dim)
    return np.concatenate([half, half])[None].astype(np.float32)


def solution(mesh):
    head_spec = P('dp', None, 'sh', None)
    row_spec = P(('dp', 'sh'))
    full_spec = P(None, None)

    def per_device(k_prefill, v_prefill, lengths, residual, norm_gain, w_query, w_key, w_value, w_out):
        num_rows, seq_len, _, head_dim = k_prefill.shape
        kv_heads = w_key.shape[1] // head_dim
        k_rows = k_prefill.reshape(num_rows, seq_len, head_dim)
        v_rows = v_prefill.reshape(num_rows, seq_len, head_dim)
        packed, size = pack(lengths, k_rows, v_rows)
        sizes = (list_length(seq_len) - BASE) // QUANTUM
        land = lax.switch(size[0], [functools.partial(more, extra=i * QUANTUM) for i in range(sizes + 1)], packed)
        land, proj, *held = base(packed, k_rows, v_rows, residual, norm_gain.reshape(-1, head_dim), w_query, w_key, w_value, w_out, land)
        k_cache, v_cache, resid_out = build(lengths, proj, jnp.asarray(frequencies(head_dim)), residual, held, k_rows, v_rows, land, kv_heads)
        shape = (1, WINDOW, kv_heads, head_dim)
        return resid_out, k_cache.reshape(shape), v_cache.reshape(shape)
    return jax.shard_map(per_device, mesh=mesh, in_specs=(head_spec, head_spec, P('dp'), P(('dp', 'sh'), None), P(None), full_spec, full_spec, full_spec, full_spec), out_specs=(P(('dp', 'sh'), None), row_spec, row_spec), check_vma=False)
```

```python
import functools

import jax
import jax.numpy as jnp
import numpy as np
from jax import lax
from jax.experimental import pallas as pl
from jax.experimental.pallas import tpu as pltpu
from jax.sharding import PartitionSpec as P

WINDOW = 4096
THETA = 10000.0
EPS = 1e-5
ALIGN = 16
HALF = 2208
BASE = 2 * HALF
CUTS = 4
PIECES = 2
QUANTUM = 64
STEP = 1024
SLAB = 128
GROUP = 4
DEPTH = 5
MADE = 2
SAVES = 4
BLOCK = 256
PITCH = 9
PARTS = 4
BASE_VMEM = 14 * 2**20
BUILD_VMEM = 19 * 2**20
LANES = 16
ORDER = [(t, k) for k in range(3) for t in range(2)]
ANY = pl.BlockSpec(memory_space=pl.ANY)
VMEM = pl.BlockSpec(memory_space=pltpu.VMEM)
SMEM = pl.BlockSpec(memory_space=pltpu.SMEM)
HBM = pl.BlockSpec(memory_space=pltpu.HBM)


def list_length(seq_len):
    return BASE + -(-(2 * seq_len - BASE) // QUANTUM) * QUANTUM


def span(length):
    return (length + (ALIGN - 1)) // ALIGN * ALIGN


def pack_kernel(len_ref, k_ref, v_ref, out_ref, size_ref, lists, first_sem, second_sem, store_sem, *, seq_len):
    chip = lax.axis_index('sh') // 2
    list_len = lists.shape[2]
    peers = [chip + 1 - 2 * (chip % 2), (chip + 2) % 4, 3 - chip]

    part = seq_len // CUTS

    def spans_of(k):
        return span(len_ref[2 * peers[k]]), span(len_ref[2 * peers[k] + 1])

    def loads(t, k, second):
        src = (k_ref, v_ref)[t]
        spans = spans_of(k)
        for i in range(CUTS):
            start = pl.multiple_of(second * spans[0] + i * part, ALIGN)
            yield spans[second] > i * part, pltpu.make_async_copy(src.at[2 * peers[k] + second, pl.ds(i * part, part)], lists.at[t, k, pl.ds(start, part)], (first_sem, second_sem)[second].at[t, k, i])

    def stores(t, k):
        size = list_len // (2 * CUTS)
        for i in range(2 * CUTS):
            rows = pl.ds(i * size, size)
            yield sum(spans_of(k)) > i * size, pltpu.make_async_copy(lists.at[t, k, rows], out_ref.at[t, k, rows], store_sem.at[t, k, i])

    def start(copies):
        for live, copy in copies:
            pl.when(live)(copy.start)

    def wait(copies):
        for live, copy in copies:
            pl.when(live)(copy.wait)

    for t, k in ORDER:
        start(loads(t, k, 0))
    longest = span(len_ref[0]) + span(len_ref[1])
    for c in range(1, len_ref.shape[0] // 2):
        longest = jnp.maximum(longest, span(len_ref[2 * c]) + span(len_ref[2 * c + 1]))
    size_ref[0] = jnp.clip((longest - BASE + QUANTUM - 1) // QUANTUM, 0, (list_len - BASE) // QUANTUM)
    for t, k in ORDER:
        wait(loads(t, k, 0))
        start(loads(t, k, 1))
    for t, k in ORDER:
        wait(loads(t, k, 1))
        start(stores(t, k))
    for t, k in ORDER:
        wait(stores(t, k))


def pack(lengths, k_rows, v_rows):
    seq_len, head_dim = k_rows.shape[1:]
    shape = (2, 3, list_length(seq_len), head_dim)
    return pl.pallas_call(
        functools.partial(pack_kernel, seq_len=seq_len),
        out_shape=(jax.ShapeDtypeStruct(shape, k_rows.dtype), jax.ShapeDtypeStruct((1,), jnp.int32)),
        in_specs=[SMEM, HBM, HBM],
        out_specs=(HBM, SMEM),
        scratch_shapes=[pltpu.VMEM(shape, k_rows.dtype), pltpu.SemaphoreType.DMA((2, 3, CUTS)), pltpu.SemaphoreType.DMA((2, 3, CUTS)), pltpu.SemaphoreType.DMA((2, 3, 2 * CUTS))],
        compiler_params=pltpu.CompilerParams(vmem_limit_bytes=60 * 2**20),
        name='pack',
    )(lengths, k_rows, v_rows)


def project(res_ref, gain_ref, weights, proj_ref, normed, total, ring, ring_sem):
    depth, side, _ = ring.shape
    resid = res_ref[...].astype(jnp.float32)
    inv_rms = lax.rsqrt(jnp.sum(resid * resid, axis=-1, keepdims=True) / resid.shape[-1] + EPS)
    lanes = gain_ref.shape[1]
    for r in range(gain_ref.shape[0]):
        cols = slice(r * lanes, (r + 1) * lanes)
        row = (resid[:, cols] * inv_rms * gain_ref[r:r + 1, :].astype(jnp.float32)).astype(normed.dtype)
        normed[:, cols] = jnp.broadcast_to(row, (normed.shape[0], lanes))
    total[...] = jnp.zeros_like(total)
    deep = normed.shape[1] // side

    def at(i):
        return pl.multiple_of(i // deep * side, side), pl.multiple_of(i % deep * side, side)

    def fetch(i):
        left, top = at(i)
        first = 0
        for w_ref in weights:
            width = w_ref.shape[1]

            @pl.when((left >= first) & (left < first + width))
            def _(w_ref=w_ref, first=first):
                here = pl.multiple_of(left - first, side)
                pltpu.make_async_copy(w_ref.at[pl.ds(top, side), pl.ds(here, side)], ring.at[i % depth], ring_sem.at[i % depth]).start()
            first += width

    blocks = total.shape[1] // side * deep

    def prime(i, carry):
        fetch(i)
        return carry
    lax.fori_loop(0, depth - 1, prime, 0)

    def step(i, carry):
        @pl.when(i + depth - 1 < blocks)
        def _():
            fetch(i + depth - 1)
        pltpu.make_async_copy(weights[0].at[pl.ds(0, side), pl.ds(0, side)], ring.at[i % depth], ring_sem.at[i % depth]).wait()
        left, top = at(i)
        total[:, pl.ds(left, side)] += jnp.dot(normed[:, pl.ds(top, side)], ring[i % depth], preferred_element_type=jnp.float32)
        return carry
    lax.fori_loop(0, blocks, step, 0)
    proj_ref[...] = total[...].astype(proj_ref.dtype)


def remote(src, dst, send, recv, device):
    return pltpu.make_async_remote_copy(src_ref=src, dst_ref=dst, send_sem=send, recv_sem=recv, device_id={'sh': device}, device_id_type=pl.DeviceIdType.MESH)


def more_kernel(packed, land, send_sem, recv_sem, *, extra):
    me = lax.axis_index('sh')
    core = me % 2
    chip = me // 2
    peers = [chip + 1 - 2 * (chip % 2), (chip + 2) % 4, 3 - chip]
    rows = pl.ds(BASE, extra)

    def out(t, k):
        return remote(packed.at[t, k, rows], land.at[t, k, core, rows], send_sem.at[t, k], recv_sem.at[t, k, core], 2 * peers[k] + 1)

    def into(t, k, q):
        here = land.at[t, k, q, rows]
        return remote(here, here, send_sem.at[t, k], recv_sem.at[t, k, q], me)

    for t, k in ORDER:
        out(t, k).start()
    for t, k in ORDER:
        out(t, k).wait_send()

    @pl.when(core == 1)
    def _():
        for t, k in ORDER:
            for q in range(2):
                into(t, k, q).wait_recv()


def nothing_kernel(packed, land):
    pass


def more(packed, *, extra):
    shape = jax.ShapeDtypeStruct((2, 4, 2) + packed.shape[2:], packed.dtype)
    if not extra:
        return pl.pallas_call(nothing_kernel, out_shape=shape, in_specs=[HBM], out_specs=HBM, compiler_params=pltpu.CompilerParams(vmem_limit_bytes=60 * 2**20), name='more_0')(packed)
    dma = pltpu.SemaphoreType.DMA
    return pl.pallas_call(
        functools.partial(more_kernel, extra=extra),
        out_shape=shape,
        in_specs=[HBM],
        out_specs=HBM,
        scratch_shapes=[dma((2, 3)), dma((2, 3, 2))],
        compiler_params=pltpu.CompilerParams(has_side_effects=True, vmem_limit_bytes=60 * 2**20),
        name=f'more_{extra}',
    )(packed)


def base_kernel(packed, k_ref, v_ref, res_ref, gain_ref, wq_ref, wk_ref, wv_ref, wout_ref, _, land, proj_ref, *rest):
    held_refs, (normed, total, ring, ring_sem, held_sem, send_sem, recv_sem, fsend_sem, frecv_sem, ssend_sem, srecv_sem) = rest[:PARTS], rest[PARTS:]
    me = lax.axis_index('sh')
    core = me % 2
    chip = me // 2
    partner = me + 1 - 2 * core
    peers = [chip + 1 - 2 * (chip % 2), (chip + 2) % 4, 3 - chip]

    size = HALF // PIECES

    def main(t, k, half, p):
        rows = pl.ds(half * HALF + p * size, size)
        return remote(packed.at[t, k, rows], land.at[t, k, core, rows], send_sem.at[t, k, half, p], recv_sem.at[t, k, core, p], 2 * peers[k] + half)

    def forward(t, k, q, p):
        rows = land.at[t, k, q, pl.ds(core * HALF + p * size, size)]
        return remote(rows, rows, fsend_sem.at[t, k, q, p], frecv_sem.at[t, k, q, p], partner)

    def main_in(t, k, q, p):
        rows = land.at[t, k, q, pl.ds(core * HALF + p * size, size)]
        return remote(rows, rows, fsend_sem.at[t, k, q, p], recv_sem.at[t, k, q, p], partner)

    def forward_in(t, k, q, p):
        rows = land.at[t, k, q, pl.ds((1 - core) * HALF + p * size, size)]
        return remote(rows, rows, fsend_sem.at[t, k, q, p], frecv_sem.at[t, k, q, p], partner)

    def across(t):
        return remote((k_ref, v_ref)[t].at[partner], land.at[t, 3, core, pl.ds(0, k_ref.shape[1])], ssend_sem.at[t], srecv_sem.at[t], partner)

    def across_in(t):
        rows = land.at[t, 3, 1 - core, pl.ds(0, k_ref.shape[1])]
        return remote(rows, rows, ssend_sem.at[t], srecv_sem.at[t], partner)

    for t, k in ORDER:
        for half in range(2):
            for p in range(PIECES):
                main(t, k, half, p).start()
    for t in range(2):
        across(t).start()
    project(res_ref, gain_ref, (wq_ref, wk_ref, wv_ref), proj_ref, normed, total, ring, ring_sem)
    slabs, part, slab = held_refs[0].shape

    def hold(c, carry):
        for i in range(PARTS):
            pltpu.make_async_copy(wout_ref.at[pl.ds(i * part, part), pl.ds(pl.multiple_of(c * slab, slab), slab)], held_refs[i].at[c], held_sem.at[i]).start()
        return carry
    lax.fori_loop(0, slabs, hold, 0)
    for t, k in ORDER:
        for p in range(PIECES):
            for q in range(2):
                main_in(t, k, q, p).wait_recv()
                forward(t, k, q, p).start()
    for t in range(2):
        across(t).wait_send()
        across_in(t).wait_recv()
    for t, k in ORDER:
        for half in range(2):
            for p in range(PIECES):
                main(t, k, half, p).wait_send()
    for t, k in ORDER:
        for q in range(2):
            for p in range(PIECES):
                forward(t, k, q, p).wait_send()
                forward_in(t, k, q, p).wait_recv()
    for i in range(PARTS):
        pltpu.make_async_copy(held_refs[i], held_refs[i], held_sem.at[i]).wait()


def base(packed, k_rows, v_rows, residual, gain, w_query, w_key, w_value, w_out, land):
    dtype = k_rows.dtype
    dma = pltpu.SemaphoreType.DMA
    model_dim = residual.shape[1]
    proj_dim = w_query.shape[1] + w_key.shape[1] + w_value.shape[1]
    return pl.pallas_call(
        base_kernel,
        out_shape=(jax.ShapeDtypeStruct(land.shape, dtype), jax.ShapeDtypeStruct((LANES, proj_dim), dtype), )+ PARTS * (jax.ShapeDtypeStruct((w_out.shape[1] // SLAB, w_out.shape[0] // PARTS, SLAB), dtype),),
        in_specs=[HBM, HBM, HBM, VMEM, VMEM, HBM, HBM, HBM, HBM, HBM],
        out_specs=(HBM, VMEM) + PARTS * (ANY,),
        scratch_shapes=[
            pltpu.VMEM((LANES, model_dim), dtype), pltpu.VMEM((LANES, proj_dim), jnp.float32), pltpu.VMEM((8, 512, 512), dtype), dma((8,)), dma((PARTS,)),
            dma((2, 3, 2, PIECES)), dma((2, 3, 2, PIECES)), dma((2, 3, 2, PIECES)), dma((2, 3, 2, PIECES)), dma((2,)), dma((2,)),
        ],
        input_output_aliases={9: 0},
        compiler_params=pltpu.CompilerParams(has_side_effects=True, vmem_limit_bytes=BASE_VMEM),
        name='base',
    )(packed, k_rows, v_rows, residual, gain, w_query, w_key, w_value, w_out, land)


def build_kernel(len_ref, proj_ref, freq_ref, res_ref, *rest, depth):
    w_refs, (k_ref, v_ref, land, kc_ref, vc_ref, xout_ref, ring, tail, wide, made, scores, probs, mixed, ovec, q_ref, knew_ref, vnew_ref, ring_sem, tail_sem, made_sem) = rest[:PARTS], rest[PARTS:]
    step = pl.program_id(0)
    steps = WINDOW // STEP
    me = lax.axis_index('sh')
    core, chip, n = me % 2, me // 2, len_ref[me]
    offset = core * span(len_ref[2 * chip])
    chips = [chip, chip + 1 - 2 * (chip % 2), (chip + 2) % 4, 3 - chip]
    extra = tail.shape[2]
    heads = tail.shape[1]
    head_dim = tail.shape[3]

    def copies(t, start, size, dst, sem):
        own = 2 * chip + core
        other = 2 * chip + 1 - core
        rows = pl.ds(start, size)
        yield pltpu.make_async_copy((k_ref, v_ref)[t].at[me, rows], dst.at[own], sem)
        yield pltpu.make_async_copy(land.at[t, 3, 1 - core, rows], dst.at[other], sem)
        far = pl.ds(pl.multiple_of(offset + start, ALIGN), size)
        for k in range(3):
            for q in range(2):
                yield pltpu.make_async_copy(land.at[t, k, q, far], dst.at[2 * chips[k + 1] + q], sem)

    def heads_of_row():
        q_width = ovec.shape[1]
        group = q_width // (heads * head_dim)

        def part(at):
            return proj_ref[:1, at:at + head_dim]

        angles = n.astype(jnp.float32) * freq_ref[...]
        lane = lax.broadcasted_iota(jnp.int32, angles.shape, 1)
        cos, sin = jnp.cos(angles), jnp.sin(angles)
        sin = jnp.where(lane < head_dim // 2, -sin, sin)

        def turned(at):
            vals = part(at).astype(jnp.float32)
            return (vals * cos + pltpu.roll(vals, head_dim // 2, 1) * sin).astype(q_ref.dtype)

        for pair in range(heads // 2):
            for half in range(2):
                h = 2 * pair + half
                rows = jnp.concatenate([turned((h * group + g) * head_dim) for g in range(group)] + [jnp.zeros((8 - group, head_dim), q_ref.dtype)], axis=0)
                none = jnp.zeros_like(rows)
                q_ref[pair, 8 * half:8 * half + 8, :] = jnp.concatenate([rows, none] if half == 0 else [none, rows], axis=1)
        knew_ref[...] = jnp.concatenate([turned(q_width + h * head_dim) for h in range(heads)], axis=0)
        vnew_ref[...] = jnp.concatenate([part(q_width + (heads + h) * head_dim) for h in range(heads)], axis=0)

    def chunk(s, then):
        for t in range(2):
            local = s - t * steps
            pl.when((local >= 0) & (local < steps) & (local * STEP < n))(functools.partial(then, t, local))

    def fetch(s):
        def then(t, local):
            for copy in copies(t, pl.multiple_of(local * STEP, STEP), STEP, ring.at[s % depth], ring_sem.at[s % depth]):
                copy.start()
        chunk(s, then)

    def arrived(s):
        def then(t, local):
            whole = ring.at[s % depth]
            pltpu.make_async_copy(whole, whole, ring_sem.at[s % depth]).wait()
        chunk(s, then)

    def fetch_tail(t):
        @pl.when(n > WINDOW)
        def _():
            for copy in copies(t, WINDOW, extra, tail.at[t], tail_sem.at[t]):
                copy.start()

    def save(b, out_ref, local):
        size = BLOCK * heads // SAVES
        for i in range(SAVES):
            at = b * BLOCK * heads + i * size
            here = pl.ds(pl.multiple_of(at, size), size)
            there = pl.ds(pl.multiple_of(local * STEP * heads + at, size), size)
            pltpu.make_async_copy(made.at[step % MADE, here], out_ref.at[there], made_sem.at[step % MADE]).start(priority=1)

    def saved(s):
        whole = made.at[s % MADE]
        pltpu.make_async_copy(whole, whole, made_sem.at[s % MADE]).wait()

    @pl.when(step == 0)
    def _():
        def ahead(s, carry):
            fetch(s)
            return carry
        fetch(jnp.int32(0))
        fetch_tail(0)
        lax.fori_loop(1, depth - 1, ahead, 0)
        fetch_tail(1)
        mixed[...] = jnp.zeros_like(mixed)
        heads_of_row()
    fetch(step + depth - 1)
    arrived(step)

    @pl.when(step >= MADE)
    def _():
        saved(step)

    def assemble(t, local, new_ref, out_ref, use):
        first = local * STEP
        newest = lax.rem(n, WINDOW)
        wraps = (local == 0) & (n > WINDOW)
        dead = first > n
        plain = (first + STEP <= n) & ~wraps & ((newest < first) | (newest >= first + STEP))
        slot = step % depth
        out = step % MADE

        @pl.when(wraps)
        def _():
            whole = tail.at[t]
            pltpu.make_async_copy(whole, whole, tail_sem.at[t]).wait()

        @pl.when(~plain & ~dead)
        def _():
            def patch(c, carry):
                low = first + c * extra
                rows = pl.ds(pl.multiple_of(c * extra, extra), extra)

                @pl.when((low < n - WINDOW) | (low + extra > n) | ((newest >= low) & (newest < low + extra)))
                def _():
                    pos = low + lax.broadcasted_iota(jnp.int32, (extra, head_dim), 0)
                    for h in range(heads):
                        vals = jnp.where(pos < n - WINDOW, tail[t, h], ring[slot, h, rows, :])
                        vals = jnp.where(pos < n, vals, jnp.zeros_like(vals))
                        ring[slot, h, rows, :] = jnp.where(pos == newest, jnp.broadcast_to(new_ref[h:h + 1, :], vals.shape), vals)
                return carry
            lax.fori_loop(0, STEP // extra, patch, 0)

        @pl.when(dead)
        def _():
            def clear(b, carry):
                made[out, pl.ds(pl.multiple_of(b * BLOCK * heads, BLOCK * heads), BLOCK * heads), :] = jnp.zeros((BLOCK * heads, head_dim), made.dtype)
                save(b, out_ref, local)
                return carry
            lax.fori_loop(0, STEP // BLOCK, clear, 0)
            use(None, None, None)

        @pl.when(~dead)
        def _():
            def mix(b, carry):
                for pair in range(heads // 2):
                    both = []
                    for h in (2 * pair, 2 * pair + 1):
                        vals = ring[slot, h, pl.ds(pl.multiple_of(b * BLOCK, BLOCK), BLOCK), :]
                        wide[pl.ds(h, BLOCK, stride=PITCH), :] = vals.astype(jnp.float32)
                        both.append(vals)
                    use(pair, b, jnp.concatenate(both, axis=1))
                rows = jnp.concatenate([wide[PITCH * p:PITCH * p + heads, :] for p in range(BLOCK)], axis=0)
                made[out, pl.ds(pl.multiple_of(b * BLOCK * heads, BLOCK * heads), BLOCK * heads), :] = rows.astype(made.dtype)
                save(b, out_ref, local)
                return carry
            lax.fori_loop(0, STEP // BLOCK, mix, 0)

    def slots_of(local, b, size):
        return pl.ds(pl.multiple_of(local * STEP + b * BLOCK, BLOCK), size)

    @pl.when(step < steps)
    def _():
        def use(pair, b, vals):
            if pair is None:
                scores[:, slots_of(step, 0, STEP)] = jnp.full((scores.shape[0], STEP), -jnp.inf)
                return
            slots = step * STEP + b * BLOCK + lax.broadcasted_iota(jnp.int32, (16, BLOCK), 1)
            live = (slots <= n) | (n >= WINDOW)
            s = lax.dot_general(q_ref[pair], vals, (((1,), (1,)), ((), ())), preferred_element_type=jnp.float32) / head_dim ** 0.5
            scores[pl.ds(16 * pair, 16), slots_of(step, b, BLOCK)] = jnp.where(live, s, -jnp.inf)
        assemble(0, step, knew_ref, kc_ref, use)

    @pl.when(step == steps)
    def _():
        for pair in range(heads // 2):
            s = scores[16 * pair:16 * pair + 16, :]
            e = jnp.exp(s - jnp.max(s, axis=-1, keepdims=True))
            probs[pair] = (e / jnp.sum(e, axis=-1, keepdims=True)).astype(probs.dtype)

    @pl.when(step >= steps)
    def _():
        local = step - steps

        def use(pair, b, vals):
            if pair is None:
                return
            mix = jnp.dot(probs[pair, :, slots_of(local, b, BLOCK)], vals, preferred_element_type=jnp.float32)
            mixed[2 * pair] += mix[:8, :head_dim]
            mixed[2 * pair + 1] += mix[8:, head_dim:]
        assemble(1, local, vnew_ref, vc_ref, use)

    @pl.when(step == 2 * steps - 1)
    def _():
        group = ovec.shape[1] // (heads * head_dim)
        for h in range(heads):
            o = mixed[h].astype(ovec.dtype)
            for g in range(group):
                cols = pl.ds((h * group + g) * head_dim, head_dim)
                ovec[:, cols] = jnp.broadcast_to(o[g:g + 1], (ovec.shape[0], head_dim))
        slabs, part, slab = w_refs[0].shape
        width = GROUP * slab

        def column(c, carry):
            acc = jnp.zeros((ovec.shape[0], width), jnp.float32)
            for i, w_ref in enumerate(w_refs):
                block = jnp.concatenate([w_ref[c * GROUP + j] for j in range(GROUP)], axis=1)
                acc += jnp.dot(ovec[:, i * part:(i + 1) * part], block, preferred_element_type=jnp.float32)
            cols = pl.ds(pl.multiple_of(c * width, width), width)
            xout_ref[:, cols] = (res_ref[:, cols].astype(jnp.float32) + acc[:1]).astype(xout_ref.dtype)
            return carry
        lax.fori_loop(0, slabs // GROUP, column, 0)
        for s in range(2 * steps - MADE, 2 * steps):
            saved(s)


def build(lengths, proj, freq, residual, w_out, k_rows, v_rows, land, heads):
    seq_len, head_dim = k_rows.shape[1:]
    steps = WINDOW // STEP
    depth = DEPTH
    dtype = k_rows.dtype
    cache = jax.ShapeDtypeStruct((WINDOW * heads, head_dim), dtype)
    dma = pltpu.SemaphoreType.DMA
    return pl.pallas_call(
        functools.partial(build_kernel, depth=depth),
        grid=(2 * steps,),
        out_shape=(cache, cache, jax.ShapeDtypeStruct(residual.shape, dtype)),
        in_specs=[SMEM, VMEM, VMEM, VMEM] + PARTS * [VMEM] + [HBM, HBM, HBM],
        out_specs=(HBM, HBM, VMEM),
        scratch_shapes=[
            pltpu.VMEM((depth, heads, STEP, head_dim), dtype),
            pltpu.VMEM((2, heads, seq_len - WINDOW, head_dim), dtype),
            pltpu.VMEM((BLOCK * PITCH, head_dim), jnp.float32),
            pltpu.VMEM((MADE, STEP * heads, head_dim), dtype),
            pltpu.VMEM((8 * heads, WINDOW), jnp.float32),
            pltpu.VMEM((heads // 2, 16, WINDOW), dtype),
            pltpu.VMEM((heads, 8, head_dim), jnp.float32),
            pltpu.VMEM((LANES, PARTS * w_out[0].shape[1]), dtype),
            pltpu.VMEM((heads // 2, 16, 2 * head_dim), dtype),
            pltpu.VMEM((heads, head_dim), dtype),
            pltpu.VMEM((heads, head_dim), dtype),
            dma((depth,)), dma((2,)), dma((MADE,)),
        ],
        compiler_params=pltpu.CompilerParams(vmem_limit_bytes=BUILD_VMEM),
        name='build',
    )(lengths, proj, freq, residual, *w_out, k_rows, v_rows, land)


def frequencies(head_dim):
    half = THETA ** (-2.0 * np.arange(head_dim // 2, dtype=np.float64) / head_dim)
    return np.concatenate([half, half])[None].astype(np.float32)


def solution(mesh):
    head_spec = P('dp', None, 'sh', None)
    row_spec = P(('dp', 'sh'))
    full_spec = P(None, None)

    def per_device(k_prefill, v_prefill, lengths, residual, norm_gain, w_query, w_key, w_value, w_out):
        num_rows, seq_len, _, head_dim = k_prefill.shape
        kv_heads = w_key.shape[1] // head_dim
        k_rows = k_prefill.reshape(num_rows, seq_len, head_dim)
        v_rows = v_prefill.reshape(num_rows, seq_len, head_dim)
        packed, size = pack(lengths, k_rows, v_rows)
        sizes = (list_length(seq_len) - BASE) // QUANTUM
        land = lax.switch(size[0], [functools.partial(more, extra=i * QUANTUM) for i in range(sizes + 1)], packed)
        land, proj, *held = base(packed, k_rows, v_rows, residual, norm_gain.reshape(-1, head_dim), w_query, w_key, w_value, w_out, land)
        k_cache, v_cache, resid_out = build(lengths, proj, jnp.asarray(frequencies(head_dim)), residual, held, k_rows, v_rows, land, kv_heads)
        shape = (1, WINDOW, kv_heads, head_dim)
        return resid_out, k_cache.reshape(shape), v_cache.reshape(shape)
    return jax.shard_map(per_device, mesh=mesh, in_specs=(head_spec, head_spec, P('dp'), P(('dp', 'sh'), None), P(None), full_spec, full_spec, full_spec, full_spec), out_specs=(P(('dp', 'sh'), None), row_spec, row_spec), check_vma=False)
```

```python
import functools

import jax
import jax.numpy as jnp
import numpy as np
from jax import lax
from jax.experimental import pallas as pl
from jax.experimental.pallas import tpu as pltpu
from jax.sharding import PartitionSpec as P

WINDOW = 4096
THETA = 10000.0
EPS = 1e-5
ALIGN = 16
HALF = 2208
BASE = 2 * HALF
CUTS = 4
PIECES = 3
QUANTUM = 64
STEP = 1024
SLAB = 128
GROUP = 4
DEPTH = 5
MADE = 2
SAVES = 4
BLOCK = 256
PITCH = 9
PARTS = 4
BASE_VMEM = 14 * 2**20
BUILD_VMEM = 19 * 2**20
LANES = 16
ORDER = [(t, k) for k in range(3) for t in range(2)]
ANY = pl.BlockSpec(memory_space=pl.ANY)
VMEM = pl.BlockSpec(memory_space=pltpu.VMEM)
SMEM = pl.BlockSpec(memory_space=pltpu.SMEM)
HBM = pl.BlockSpec(memory_space=pltpu.HBM)


def list_length(seq_len):
    return BASE + -(-(2 * seq_len - BASE) // QUANTUM) * QUANTUM


def span(length):
    return (length + (ALIGN - 1)) // ALIGN * ALIGN


def pack_kernel(len_ref, k_ref, v_ref, out_ref, size_ref, lists, first_sem, second_sem, store_sem, *, seq_len):
    chip = lax.axis_index('sh') // 2
    list_len = lists.shape[2]
    peers = [chip + 1 - 2 * (chip % 2), (chip + 2) % 4, 3 - chip]

    part = seq_len // CUTS

    def spans_of(k):
        return span(len_ref[2 * peers[k]]), span(len_ref[2 * peers[k] + 1])

    def loads(t, k, second):
        src = (k_ref, v_ref)[t]
        spans = spans_of(k)
        for i in range(CUTS):
            start = pl.multiple_of(second * spans[0] + i * part, ALIGN)
            yield spans[second] > i * part, pltpu.make_async_copy(src.at[2 * peers[k] + second, pl.ds(i * part, part)], lists.at[t, k, pl.ds(start, part)], (first_sem, second_sem)[second].at[t, k, i])

    def stores(t, k, early=None):
        size = list_len // (2 * CUTS)
        spans = spans_of(k)
        for i in range(2 * CUTS):
            rows = pl.ds(i * size, size)
            live = sum(spans) > i * size
            if early is not None:
                inside = (i + 1) * size <= spans[0]
                live = live & (inside if early else ~inside)
            yield live, pltpu.make_async_copy(lists.at[t, k, rows], out_ref.at[t, k, rows], store_sem.at[t, k, i])

    def start(copies):
        for live, copy in copies:
            pl.when(live)(copy.start)

    def wait(copies):
        for live, copy in copies:
            pl.when(live)(copy.wait)

    for t, k in ORDER:
        start(loads(t, k, 0))
    longest = span(len_ref[0]) + span(len_ref[1])
    for c in range(1, len_ref.shape[0] // 2):
        longest = jnp.maximum(longest, span(len_ref[2 * c]) + span(len_ref[2 * c + 1]))
    size_ref[0] = jnp.clip((longest - BASE + QUANTUM - 1) // QUANTUM, 0, (list_len - BASE) // QUANTUM)
    for t, k in ORDER:
        wait(loads(t, k, 0))
        start(loads(t, k, 1))
        start(stores(t, k, True))
    for t, k in ORDER:
        wait(loads(t, k, 1))
        start(stores(t, k, False))
    for t, k in ORDER:
        wait(stores(t, k))


def pack(lengths, k_rows, v_rows):
    seq_len, head_dim = k_rows.shape[1:]
    shape = (2, 3, list_length(seq_len), head_dim)
    return pl.pallas_call(
        functools.partial(pack_kernel, seq_len=seq_len),
        out_shape=(jax.ShapeDtypeStruct(shape, k_rows.dtype), jax.ShapeDtypeStruct((1,), jnp.int32)),
        in_specs=[SMEM, HBM, HBM],
        out_specs=(HBM, SMEM),
        scratch_shapes=[pltpu.VMEM(shape, k_rows.dtype), pltpu.SemaphoreType.DMA((2, 3, CUTS)), pltpu.SemaphoreType.DMA((2, 3, CUTS)), pltpu.SemaphoreType.DMA((2, 3, 2 * CUTS))],
        compiler_params=pltpu.CompilerParams(vmem_limit_bytes=60 * 2**20),
        name='pack',
    )(lengths, k_rows, v_rows)


def project(res_ref, gain_ref, weights, proj_ref, normed, total, ring, ring_sem):
    depth, side, _ = ring.shape
    resid = res_ref[...].astype(jnp.float32)
    inv_rms = lax.rsqrt(jnp.sum(resid * resid, axis=-1, keepdims=True) / resid.shape[-1] + EPS)
    lanes = gain_ref.shape[1]
    for r in range(gain_ref.shape[0]):
        cols = slice(r * lanes, (r + 1) * lanes)
        row = (resid[:, cols] * inv_rms * gain_ref[r:r + 1, :].astype(jnp.float32)).astype(normed.dtype)
        normed[:, cols] = jnp.broadcast_to(row, (normed.shape[0], lanes))
    total[...] = jnp.zeros_like(total)
    deep = normed.shape[1] // side

    def at(i):
        return pl.multiple_of(i // deep * side, side), pl.multiple_of(i % deep * side, side)

    def fetch(i):
        left, top = at(i)
        first = 0
        for w_ref in weights:
            width = w_ref.shape[1]

            @pl.when((left >= first) & (left < first + width))
            def _(w_ref=w_ref, first=first):
                here = pl.multiple_of(left - first, side)
                pltpu.make_async_copy(w_ref.at[pl.ds(top, side), pl.ds(here, side)], ring.at[i % depth], ring_sem.at[i % depth]).start()
            first += width

    blocks = total.shape[1] // side * deep

    def prime(i, carry):
        fetch(i)
        return carry
    lax.fori_loop(0, depth - 1, prime, 0)

    def step(i, carry):
        @pl.when(i + depth - 1 < blocks)
        def _():
            fetch(i + depth - 1)
        pltpu.make_async_copy(weights[0].at[pl.ds(0, side), pl.ds(0, side)], ring.at[i % depth], ring_sem.at[i % depth]).wait()
        left, top = at(i)
        total[:, pl.ds(left, side)] += jnp.dot(normed[:, pl.ds(top, side)], ring[i % depth], preferred_element_type=jnp.float32)
        return carry
    lax.fori_loop(0, blocks, step, 0)
    proj_ref[...] = total[...].astype(proj_ref.dtype)


def remote(src, dst, send, recv, device):
    return pltpu.make_async_remote_copy(src_ref=src, dst_ref=dst, send_sem=send, recv_sem=recv, device_id={'sh': device}, device_id_type=pl.DeviceIdType.MESH)


def more_kernel(packed, land, send_sem, recv_sem, *, extra):
    me = lax.axis_index('sh')
    core = me % 2
    chip = me // 2
    peers = [chip + 1 - 2 * (chip % 2), (chip + 2) % 4, 3 - chip]
    rows = pl.ds(BASE, extra)

    def out(t, k):
        return remote(packed.at[t, k, rows], land.at[t, k, core, rows], send_sem.at[t, k], recv_sem.at[t, k, core], 2 * peers[k] + 1)

    def into(t, k, q):
        here = land.at[t, k, q, rows]
        return remote(here, here, send_sem.at[t, k], recv_sem.at[t, k, q], me)

    for t, k in ORDER:
        out(t, k).start()
    for t, k in ORDER:
        out(t, k).wait_send()

    @pl.when(core == 1)
    def _():
        for t, k in ORDER:
            for q in range(2):
                into(t, k, q).wait_recv()


def nothing_kernel(packed, land):
    pass


def more(packed, *, extra):
    shape = jax.ShapeDtypeStruct((2, 4, 2) + packed.shape[2:], packed.dtype)
    if not extra:
        return pl.pallas_call(nothing_kernel, out_shape=shape, in_specs=[HBM], out_specs=HBM, compiler_params=pltpu.CompilerParams(vmem_limit_bytes=60 * 2**20), name='more_0')(packed)
    dma = pltpu.SemaphoreType.DMA
    return pl.pallas_call(
        functools.partial(more_kernel, extra=extra),
        out_shape=shape,
        in_specs=[HBM],
        out_specs=HBM,
        scratch_shapes=[dma((2, 3)), dma((2, 3, 2))],
        compiler_params=pltpu.CompilerParams(has_side_effects=True, vmem_limit_bytes=60 * 2**20),
        name=f'more_{extra}',
    )(packed)


def base_kernel(packed, k_ref, v_ref, res_ref, gain_ref, wq_ref, wk_ref, wv_ref, wout_ref, _, land, proj_ref, *rest):
    held_refs, (normed, total, ring, ring_sem, held_sem, send_sem, recv_sem, fsend_sem, frecv_sem, ssend_sem, srecv_sem) = rest[:PARTS], rest[PARTS:]
    me = lax.axis_index('sh')
    core = me % 2
    chip = me // 2
    partner = me + 1 - 2 * core
    peers = [chip + 1 - 2 * (chip % 2), (chip + 2) % 4, 3 - chip]

    size = HALF // PIECES

    def main(t, k, half, p):
        rows = pl.ds(half * HALF + p * size, size)
        return remote(packed.at[t, k, rows], land.at[t, k, core, rows], send_sem.at[t, k, half, p], recv_sem.at[t, k, core, p], 2 * peers[k] + half)

    def forward(t, k, q, p):
        rows = land.at[t, k, q, pl.ds(core * HALF + p * size, size)]
        return remote(rows, rows, fsend_sem.at[t, k, q, p], frecv_sem.at[t, k, q, p], partner)

    def main_in(t, k, q, p):
        rows = land.at[t, k, q, pl.ds(core * HALF + p * size, size)]
        return remote(rows, rows, fsend_sem.at[t, k, q, p], recv_sem.at[t, k, q, p], partner)

    def forward_in(t, k, q, p):
        rows = land.at[t, k, q, pl.ds((1 - core) * HALF + p * size, size)]
        return remote(rows, rows, fsend_sem.at[t, k, q, p], frecv_sem.at[t, k, q, p], partner)

    def across(t):
        return remote((k_ref, v_ref)[t].at[partner], land.at[t, 3, core, pl.ds(0, k_ref.shape[1])], ssend_sem.at[t], srecv_sem.at[t], partner)

    def across_in(t):
        rows = land.at[t, 3, 1 - core, pl.ds(0, k_ref.shape[1])]
        return remote(rows, rows, ssend_sem.at[t], srecv_sem.at[t], partner)

    for t, k in ORDER:
        for half in range(2):
            for p in range(PIECES):
                main(t, k, half, p).start()
    for t in range(2):
        across(t).start()
    project(res_ref, gain_ref, (wq_ref, wk_ref, wv_ref), proj_ref, normed, total, ring, ring_sem)
    slabs, part, slab = held_refs[0].shape

    def hold(c, carry):
        for i in range(PARTS):
            pltpu.make_async_copy(wout_ref.at[pl.ds(i * part, part), pl.ds(pl.multiple_of(c * slab, slab), slab)], held_refs[i].at[c], held_sem.at[i]).start()
        return carry
    lax.fori_loop(0, slabs, hold, 0)
    for t, k in ORDER:
        for p in range(PIECES):
            for q in range(2):
                main_in(t, k, q, p).wait_recv()
                forward(t, k, q, p).start()
    for t in range(2):
        across(t).wait_send()
        across_in(t).wait_recv()
    for t, k in ORDER:
        for half in range(2):
            for p in range(PIECES):
                main(t, k, half, p).wait_send()
    for t, k in ORDER:
        for q in range(2):
            for p in range(PIECES):
                forward(t, k, q, p).wait_send()
                forward_in(t, k, q, p).wait_recv()
    for i in range(PARTS):
        pltpu.make_async_copy(held_refs[i], held_refs[i], held_sem.at[i]).wait()


def base(packed, k_rows, v_rows, residual, gain, w_query, w_key, w_value, w_out, land):
    dtype = k_rows.dtype
    dma = pltpu.SemaphoreType.DMA
    model_dim = residual.shape[1]
    proj_dim = w_query.shape[1] + w_key.shape[1] + w_value.shape[1]
    return pl.pallas_call(
        base_kernel,
        out_shape=(jax.ShapeDtypeStruct(land.shape, dtype), jax.ShapeDtypeStruct((LANES, proj_dim), dtype), )+ PARTS * (jax.ShapeDtypeStruct((w_out.shape[1] // SLAB, w_out.shape[0] // PARTS, SLAB), dtype),),
        in_specs=[HBM, HBM, HBM, VMEM, VMEM, HBM, HBM, HBM, HBM, HBM],
        out_specs=(HBM, VMEM) + PARTS * (ANY,),
        scratch_shapes=[
            pltpu.VMEM((LANES, model_dim), dtype), pltpu.VMEM((LANES, proj_dim), jnp.float32), pltpu.VMEM((8, 512, 512), dtype), dma((8,)), dma((PARTS,)),
            dma((2, 3, 2, PIECES)), dma((2, 3, 2, PIECES)), dma((2, 3, 2, PIECES)), dma((2, 3, 2, PIECES)), dma((2,)), dma((2,)),
        ],
        input_output_aliases={9: 0},
        compiler_params=pltpu.CompilerParams(has_side_effects=True, vmem_limit_bytes=BASE_VMEM),
        name='base',
    )(packed, k_rows, v_rows, residual, gain, w_query, w_key, w_value, w_out, land)


def build_kernel(len_ref, proj_ref, freq_ref, res_ref, *rest, depth):
    w_refs, (k_ref, v_ref, land, kc_ref, vc_ref, xout_ref, ring, tail, wide, made, scores, probs, mixed, ovec, q_ref, knew_ref, vnew_ref, ring_sem, tail_sem, made_sem) = rest[:PARTS], rest[PARTS:]
    step = pl.program_id(0)
    steps = WINDOW // STEP
    me = lax.axis_index('sh')
    core, chip, n = me % 2, me // 2, len_ref[me]
    offset = core * span(len_ref[2 * chip])
    chips = [chip, chip + 1 - 2 * (chip % 2), (chip + 2) % 4, 3 - chip]
    extra = tail.shape[2]
    heads = tail.shape[1]
    head_dim = tail.shape[3]

    def copies(t, start, size, dst, sem):
        own = 2 * chip + core
        other = 2 * chip + 1 - core
        rows = pl.ds(start, size)
        yield pltpu.make_async_copy((k_ref, v_ref)[t].at[me, rows], dst.at[own], sem)
        yield pltpu.make_async_copy(land.at[t, 3, 1 - core, rows], dst.at[other], sem)
        far = pl.ds(pl.multiple_of(offset + start, ALIGN), size)
        for k in range(3):
            for q in range(2):
                yield pltpu.make_async_copy(land.at[t, k, q, far], dst.at[2 * chips[k + 1] + q], sem)

    def heads_of_row():
        q_width = ovec.shape[1]
        group = q_width // (heads * head_dim)

        def part(at):
            return proj_ref[:1, at:at + head_dim]

        angles = n.astype(jnp.float32) * freq_ref[...]
        lane = lax.broadcasted_iota(jnp.int32, angles.shape, 1)
        cos, sin = jnp.cos(angles), jnp.sin(angles)
        sin = jnp.where(lane < head_dim // 2, -sin, sin)

        def turned(at):
            vals = part(at).astype(jnp.float32)
            return (vals * cos + pltpu.roll(vals, head_dim // 2, 1) * sin).astype(q_ref.dtype)

        for pair in range(heads // 2):
            for half in range(2):
                h = 2 * pair + half
                rows = jnp.concatenate([turned((h * group + g) * head_dim) for g in range(group)] + [jnp.zeros((8 - group, head_dim), q_ref.dtype)], axis=0)
                none = jnp.zeros_like(rows)
                q_ref[pair, 8 * half:8 * half + 8, :] = jnp.concatenate([rows, none] if half == 0 else [none, rows], axis=1)
        knew_ref[...] = jnp.concatenate([turned(q_width + h * head_dim) for h in range(heads)], axis=0)
        vnew_ref[...] = jnp.concatenate([part(q_width + (heads + h) * head_dim) for h in range(heads)], axis=0)

    def chunk(s, then):
        for t in range(2):
            local = s - t * steps
            pl.when((local >= 0) & (local < steps) & (local * STEP < n))(functools.partial(then, t, local))

    def fetch(s):
        def then(t, local):
            for copy in copies(t, pl.multiple_of(local * STEP, STEP), STEP, ring.at[s % depth], ring_sem.at[s % depth]):
                copy.start()
        chunk(s, then)

    def arrived(s):
        def then(t, local):
            whole = ring.at[s % depth]
            pltpu.make_async_copy(whole, whole, ring_sem.at[s % depth]).wait()
        chunk(s, then)

    def fetch_tail(t):
        @pl.when(n > WINDOW)
        def _():
            for copy in copies(t, WINDOW, extra, tail.at[t], tail_sem.at[t]):
                copy.start()

    def save(b, out_ref, local):
        size = BLOCK * heads // SAVES
        for i in range(SAVES):
            at = b * BLOCK * heads + i * size
            here = pl.ds(pl.multiple_of(at, size), size)
            there = pl.ds(pl.multiple_of(local * STEP * heads + at, size), size)
            pltpu.make_async_copy(made.at[step % MADE, here], out_ref.at[there], made_sem.at[step % MADE]).start(priority=1)

    def saved(s):
        whole = made.at[s % MADE]
        pltpu.make_async_copy(whole, whole, made_sem.at[s % MADE]).wait()

    @pl.when(step == 0)
    def _():
        def ahead(s, carry):
            fetch(s)
            return carry
        fetch(jnp.int32(0))
        fetch_tail(0)
        lax.fori_loop(1, depth - 1, ahead, 0)
        fetch_tail(1)
        mixed[...] = jnp.zeros_like(mixed)
        heads_of_row()
    fetch(step + depth - 1)
    arrived(step)

    @pl.when(step >= MADE)
    def _():
        saved(step)

    def assemble(t, local, new_ref, out_ref, use):
        first = local * STEP
        newest = lax.rem(n, WINDOW)
        wraps = (local == 0) & (n > WINDOW)
        dead = first > n
        plain = (first + STEP <= n) & ~wraps & ((newest < first) | (newest >= first + STEP))
        slot = step % depth
        out = step % MADE

        @pl.when(wraps)
        def _():
            whole = tail.at[t]
            pltpu.make_async_copy(whole, whole, tail_sem.at[t]).wait()

        @pl.when(~plain & ~dead)
        def _():
            def patch(c, carry):
                low = first + c * extra
                rows = pl.ds(pl.multiple_of(c * extra, extra), extra)

                @pl.when((low < n - WINDOW) | (low + extra > n) | ((newest >= low) & (newest < low + extra)))
                def _():
                    pos = low + lax.broadcasted_iota(jnp.int32, (extra, head_dim), 0)
                    for h in range(heads):
                        vals = jnp.where(pos < n - WINDOW, tail[t, h], ring[slot, h, rows, :])
                        vals = jnp.where(pos < n, vals, jnp.zeros_like(vals))
                        ring[slot, h, rows, :] = jnp.where(pos == newest, jnp.broadcast_to(new_ref[h:h + 1, :], vals.shape), vals)
                return carry
            lax.fori_loop(0, STEP // extra, patch, 0)

        @pl.when(dead)
        def _():
            def clear(b, carry):
                made[out, pl.ds(pl.multiple_of(b * BLOCK * heads, BLOCK * heads), BLOCK * heads), :] = jnp.zeros((BLOCK * heads, head_dim), made.dtype)
                save(b, out_ref, local)
                return carry
            lax.fori_loop(0, STEP // BLOCK, clear, 0)
            use(None, None, None)

        @pl.when(~dead)
        def _():
            def mix(b, carry):
                for pair in range(heads // 2):
                    both = []
                    for h in (2 * pair, 2 * pair + 1):
                        vals = ring[slot, h, pl.ds(pl.multiple_of(b * BLOCK, BLOCK), BLOCK), :]
                        wide[pl.ds(h, BLOCK, stride=PITCH), :] = vals.astype(jnp.float32)
                        both.append(vals)
                    use(pair, b, jnp.concatenate(both, axis=1))
                rows = jnp.concatenate([wide[PITCH * p:PITCH * p + heads, :] for p in range(BLOCK)], axis=0)
                made[out, pl.ds(pl.multiple_of(b * BLOCK * heads, BLOCK * heads), BLOCK * heads), :] = rows.astype(made.dtype)
                save(b, out_ref, local)
                return carry
            lax.fori_loop(0, STEP // BLOCK, mix, 0)

    def slots_of(local, b, size):
        return pl.ds(pl.multiple_of(local * STEP + b * BLOCK, BLOCK), size)

    @pl.when(step < steps)
    def _():
        def use(pair, b, vals):
            if pair is None:
                scores[:, slots_of(step, 0, STEP)] = jnp.full((scores.shape[0], STEP), -jnp.inf)
                return
            slots = step * STEP + b * BLOCK + lax.broadcasted_iota(jnp.int32, (16, BLOCK), 1)
            live = (slots <= n) | (n >= WINDOW)
            s = lax.dot_general(q_ref[pair], vals, (((1,), (1,)), ((), ())), preferred_element_type=jnp.float32) / head_dim ** 0.5
            scores[pl.ds(16 * pair, 16), slots_of(step, b, BLOCK)] = jnp.where(live, s, -jnp.inf)
        assemble(0, step, knew_ref, kc_ref, use)

    @pl.when(step == steps)
    def _():
        for pair in range(heads // 2):
            s = scores[16 * pair:16 * pair + 16, :]
            e = jnp.exp(s - jnp.max(s, axis=-1, keepdims=True))
            probs[pair] = (e / jnp.sum(e, axis=-1, keepdims=True)).astype(probs.dtype)

    @pl.when(step >= steps)
    def _():
        local = step - steps

        def use(pair, b, vals):
            if pair is None:
                return
            mix = jnp.dot(probs[pair, :, slots_of(local, b, BLOCK)], vals, preferred_element_type=jnp.float32)
            mixed[2 * pair] += mix[:8, :head_dim]
            mixed[2 * pair + 1] += mix[8:, head_dim:]
        assemble(1, local, vnew_ref, vc_ref, use)

    @pl.when(step == 2 * steps - 1)
    def _():
        group = ovec.shape[1] // (heads * head_dim)
        for h in range(heads):
            o = mixed[h].astype(ovec.dtype)
            for g in range(group):
                cols = pl.ds((h * group + g) * head_dim, head_dim)
                ovec[:, cols] = jnp.broadcast_to(o[g:g + 1], (ovec.shape[0], head_dim))
        slabs, part, slab = w_refs[0].shape
        width = GROUP * slab

        def column(c, carry):
            acc = jnp.zeros((ovec.shape[0], width), jnp.float32)
            for i, w_ref in enumerate(w_refs):
                block = jnp.concatenate([w_ref[c * GROUP + j] for j in range(GROUP)], axis=1)
                acc += jnp.dot(ovec[:, i * part:(i + 1) * part], block, preferred_element_type=jnp.float32)
            cols = pl.ds(pl.multiple_of(c * width, width), width)
            xout_ref[:, cols] = (res_ref[:, cols].astype(jnp.float32) + acc[:1]).astype(xout_ref.dtype)
            return carry
        lax.fori_loop(0, slabs // GROUP, column, 0)
        for s in range(2 * steps - MADE, 2 * steps):
            saved(s)


def build(lengths, proj, freq, residual, w_out, k_rows, v_rows, land, heads):
    seq_len, head_dim = k_rows.shape[1:]
    steps = WINDOW // STEP
    depth = DEPTH
    dtype = k_rows.dtype
    cache = jax.ShapeDtypeStruct((WINDOW * heads, head_dim), dtype)
    dma = pltpu.SemaphoreType.DMA
    return pl.pallas_call(
        functools.partial(build_kernel, depth=depth),
        grid=(2 * steps,),
        out_shape=(cache, cache, jax.ShapeDtypeStruct(residual.shape, dtype)),
        in_specs=[SMEM, VMEM, VMEM, VMEM] + PARTS * [VMEM] + [HBM, HBM, HBM],
        out_specs=(HBM, HBM, VMEM),
        scratch_shapes=[
            pltpu.VMEM((depth, heads, STEP, head_dim), dtype),
            pltpu.VMEM((2, heads, seq_len - WINDOW, head_dim), dtype),
            pltpu.VMEM((BLOCK * PITCH, head_dim), jnp.float32),
            pltpu.VMEM((MADE, STEP * heads, head_dim), dtype),
            pltpu.VMEM((8 * heads, WINDOW), jnp.float32),
            pltpu.VMEM((heads // 2, 16, WINDOW), dtype),
            pltpu.VMEM((heads, 8, head_dim), jnp.float32),
            pltpu.VMEM((LANES, PARTS * w_out[0].shape[1]), dtype),
            pltpu.VMEM((heads // 2, 16, 2 * head_dim), dtype),
            pltpu.VMEM((heads, head_dim), dtype),
            pltpu.VMEM((heads, head_dim), dtype),
            dma((depth,)), dma((2,)), dma((MADE,)),
        ],
        compiler_params=pltpu.CompilerParams(vmem_limit_bytes=BUILD_VMEM),
        name='build',
    )(lengths, proj, freq, residual, *w_out, k_rows, v_rows, land)


def frequencies(head_dim):
    half = THETA ** (-2.0 * np.arange(head_dim // 2, dtype=np.float64) / head_dim)
    return np.concatenate([half, half])[None].astype(np.float32)


def solution(mesh):
    head_spec = P('dp', None, 'sh', None)
    row_spec = P(('dp', 'sh'))
    full_spec = P(None, None)

    def per_device(k_prefill, v_prefill, lengths, residual, norm_gain, w_query, w_key, w_value, w_out):
        num_rows, seq_len, _, head_dim = k_prefill.shape
        kv_heads = w_key.shape[1] // head_dim
        k_rows = k_prefill.reshape(num_rows, seq_len, head_dim)
        v_rows = v_prefill.reshape(num_rows, seq_len, head_dim)
        packed, size = pack(lengths, k_rows, v_rows)
        sizes = (list_length(seq_len) - BASE) // QUANTUM
        land = lax.switch(size[0], [functools.partial(more, extra=i * QUANTUM) for i in range(sizes + 1)], packed)
        land, proj, *held = base(packed, k_rows, v_rows, residual, norm_gain.reshape(-1, head_dim), w_query, w_key, w_value, w_out, land)
        k_cache, v_cache, resid_out = build(lengths, proj, jnp.asarray(frequencies(head_dim)), residual, held, k_rows, v_rows, land, kv_heads)
        shape = (1, WINDOW, kv_heads, head_dim)
        return resid_out, k_cache.reshape(shape), v_cache.reshape(shape)
    return jax.shard_map(per_device, mesh=mesh, in_specs=(head_spec, head_spec, P('dp'), P(('dp', 'sh'), None), P(None), full_spec, full_spec, full_spec, full_spec), out_specs=(P(('dp', 'sh'), None), row_spec, row_spec), check_vma=False)
```
